32 devices in a mesh: agent: 4 (over x, core), tile: 8 (over z, y).
Axes of the slice: x: 2, y: 2, z: 4, core: 2. Of those that a mesh axis runs over, the one named last changes fastest.
Arguments:
- states: float32 [4, 4, 512, 512], P('agent', None, 'tile'), may hold values from -6 to 6
- sinogram: float32 [256, 4, 128], P('tile'), may hold values from -6 to 6
- blocks: bfloat16 [2048, 128, 128], P('tile'), may hold values from -0.1875 to 0.1875
- block_angle: int32 [2048], P('tile'), may hold values from 0 to 63
- block_detector: int32 [2048], P('tile'), may hold values from 0 to 3
- block_tile: int32 [2048], P('tile'), may hold values from 0 to 255
- conv_first: bfloat16 [3, 3, 3, 32], replicated, may hold values from -3 to 3
- conv_hidden: bfloat16 [3, 2, 3, 3, 32, 32], replicated, may hold values from -0.5 to 0.5
- conv_last: bfloat16 [3, 3, 3, 32], replicated, may hold values from -0.375 to 0.375
Outputs:
- new_states: float32 [4, 4, 512, 512], P('agent', None, 'tile')
The draws below stay inside these ranges and needn't reach their ends.
Inputs may be any that keep to these rules, and one draw needn't show every extreme that they name: `block_angle`: each block's angle index. `block_detector`: each block's detector block. `block_tile`: tile index among the 256 pixel tiles of the block's device.
All inputs are finite; a program needn't handle non-finite values.
Results may differ from the reference program's by a relative error of at most 0.0051.
Values may be sent and summed in bfloat16 or wider, within the bound.
A program may use at most 256 MiB of HBM per device.

```python
import jax
import jax.numpy as jnp
from jax import lax

IMG = 512
SLICES = 4
ANGLES = 64
NB_DEV = 256
WIDTH = 32
MID_LAYERS = 2
DATA_STEPS = 2
TILES_DEV = 256
RAY_BLOCKS = 256
BLOCKS = 2048
BLOCKS_PER_RAY = 8


def with_ends(values, own_key, least, largest):
    place = [jax.random.randint(jax.random.fold_in(own_key, axis), (), 0, length) for axis, length in enumerate(values.shape)]
    main_axis = values.shape.index(max(values.shape))
    neighbour = place[:main_axis] + [(place[main_axis] + 1) % values.shape[main_axis]] + place[main_axis + 1:]
    return values.at[tuple(place)].set(least).at[tuple(neighbour)].set(largest)


def level_of(key, extent, shards, low, top_value):
    level, own = 1.0, jax.random.fold_in(key, 6)
    for dim, parts in shards:
        heights = jnp.exp(jax.random.uniform(jax.random.fold_in(own, dim), (parts,), jnp.float32, low / len(shards), top_value / len(shards)))
        level = level * jnp.repeat(heights, extent[dim] // parts).reshape([-1 if axis == dim else 1 for axis in range(len(extent))])
    return level


def noise(key, extent, scale, most, cuts=(), kind=jnp.bfloat16):
    drawn = jax.random.normal(key, extent, jnp.float32) * scale
    if len(cuts) > 0:
        drawn = level_of(key, extent, cuts, -0.22, 0.18) * drawn
    return jnp.clip(drawn, min=-most, max=most).astype(kind)


def setup_inputs(seed: int = 0) -> dict:
    keys = jax.random.split(jax.random.key(seed), 10)
    states = noise(keys[0], (4, SLICES, IMG, IMG), 1.0, 6.0, ((0, 4), (2, 8)), jnp.float32)
    sinogram = noise(keys[1], (RAY_BLOCKS, SLICES, 128), 1.0, 6.0, ((0, 8),), jnp.float32)
    blocks = noise(keys[2], (BLOCKS, 128, 128), (128 * BLOCKS_PER_RAY) ** -0.5, 0.1875, ((0, 8),))
    block_angle = with_ends(jax.random.randint(keys[3], (BLOCKS,), 0, ANGLES), jax.random.fold_in(keys[3], 1), 0, ANGLES - 1).astype(jnp.int32)
    block_detector = with_ends(jax.random.randint(keys[4], (BLOCKS,), 0, IMG // 128), jax.random.fold_in(keys[4], 1), 0, (IMG // 128) - 1).astype(jnp.int32)
    block_tile = with_ends(jax.random.randint(keys[5], (BLOCKS,), 0, TILES_DEV), jax.random.fold_in(keys[5], 1), 0, TILES_DEV - 1).astype(jnp.int32)
    conv_first = noise(keys[6], (3, 3, 3, WIDTH), 4 ** -0.5, 3.0)
    conv_hidden = noise(keys[7], (3, MID_LAYERS, 3, 3, WIDTH, WIDTH), (9 * WIDTH // 2) ** -0.5, 0.5)
    conv_last = noise(keys[8], (3, 3, 3, WIDTH), (9 * WIDTH) ** -0.5, 0.375)
    return {"states": states, "sinogram": sinogram, "blocks": blocks, "block_angle": block_angle, "block_detector": block_detector, "block_tile": block_tile, "conv_first": conv_first, "conv_hidden": conv_hidden, "conv_last": conv_last}


def conv_plane(feature, weight):
    padded = jnp.pad(feature.astype(jnp.float32), ((0, 0), (1, 1), (1, 1)))
    row_count = feature.shape[1]
    columns = feature.shape[2]
    weight_float = weight.astype(jnp.float32)
    summed = jnp.zeros((weight.shape[3], row_count, columns), jnp.float32)
    for offset_row in range(3):
        for offset_column in range(3):
            window = padded[:, offset_row:offset_row + row_count, offset_column:offset_column + columns]
            summed = summed + jnp.einsum("cd,cab->dab", weight_float[offset_row, offset_column], window, precision=lax.Precision.HIGHEST)
    return summed


def denoise_plane(single_plane, first, hidden, last):
    feature = single_plane[None]
    feature = jnp.maximum(conv_plane(feature, first[:, :, None, :]), 0.0).astype(jnp.bfloat16)
    for layer_index in range(hidden.shape[0]):
        feature = jnp.maximum(conv_plane(feature, hidden[layer_index]), 0.0).astype(jnp.bfloat16)
    return conv_plane(feature, last[:, :, :, None])[0]


def denoise_volume(volume, orient, conv_first, conv_hidden, conv_last):
    rounded = volume.astype(jnp.bfloat16)
    if orient == 0:
        planes = rounded
    elif orient == 1:
        planes = jnp.transpose(rounded, (2, 0, 1))
    else:
        planes = jnp.transpose(rounded, (1, 0, 2))
    result = lax.map(lambda single_plane: denoise_plane(single_plane, conv_first[orient], conv_hidden[orient], conv_last[orient]), planes)
    if orient == 0:
        return result
    if orient == 1:
        return jnp.transpose(result, (1, 2, 0))
    return jnp.transpose(result, (1, 0, 2))


def reference(states, sinogram, blocks, block_angle, block_detector, block_tile, conv_first, conv_hidden, conv_last):
    tiles_per_row = IMG // 128
    ray_index = (block_angle * tiles_per_row + block_detector).astype(jnp.int32)
    owner_device = (jnp.arange(BLOCKS, dtype=jnp.int32) // NB_DEV).astype(jnp.int32)
    pixel_index = (owner_device * TILES_DEV + block_tile).astype(jnp.int32)
    blocks_float = blocks.astype(jnp.float32)
    x_data = states[0]
    for step_index in range(DATA_STEPS):
        pixels = x_data.astype(jnp.bfloat16).reshape(SLICES, IMG * IMG // 128, 128)
        picked = jnp.take(pixels, pixel_index, axis=1).astype(jnp.float32)
        projected = jnp.einsum("zbp,bqp->bzq", picked, blocks_float, precision=lax.Precision.HIGHEST)
        ray_sums = jax.ops.segment_sum(projected, ray_index, num_segments=RAY_BLOCKS)
        residual = (ray_sums - sinogram).astype(jnp.bfloat16)
        spread = jnp.take(residual, ray_index, axis=0).astype(jnp.float32)
        contribution = jnp.einsum("bzq,bqp->bzp", spread, blocks_float, precision=lax.Precision.HIGHEST)
        summed = jax.ops.segment_sum(contribution, pixel_index, num_segments=IMG * IMG // 128)
        back_projected = jnp.transpose(summed, (1, 0, 2)).reshape(SLICES, IMG, IMG)
        x_data = x_data - 0.8 * back_projected
    fixed_points = [x_data]
    for orient in range(3):
        net_volume = denoise_volume(states[orient + 1], orient, conv_first, conv_hidden, conv_last)
        fixed_points.append(states[orient + 1] - net_volume)
    reflected = []
    for agent_index in range(4):
        reflected.append(2.0 * fixed_points[agent_index] - states[agent_index])
    average = (reflected[0] + reflected[1] + reflected[2] + reflected[3]) / 4.0
    results = []
    for agent_index in range(4):
        results.append(0.5 * states[agent_index] + 0.5 * (2.0 * average - reflected[agent_index]))
    return jnp.stack(results, axis=0)
```

```python
import functools

import jax
import jax.numpy as jnp
from jax import lax
from jax.experimental import pallas as pl
from jax.experimental.pallas import tpu as pltpu
from jax.sharding import PartitionSpec as P

DATA_STEPS = 2
MESH = pl.DeviceIdType.MESH
LANES = 128
STRIPS = 16
CHUNK = 32
UNROLL = 8
BF = jnp.bfloat16
F32 = jnp.float32
NATURAL = (0, 1, 2, 3)
EVEN_ORDER = (0, 1, 2, 3)
ODD_ORDER = (1, 0, 3, 2)


def main_cells(offset):
    order = EVEN_ORDER if offset % 2 else ODD_ORDER
    return [(offset, column) for column in order]

def edge_cells(offset):
    return [(offset + 1, 4), (offset, 4), (offset, -1), (offset + 1, -1)]

def window_cells(rows):
    tiles = [main_cells(a) for a in range(rows + 2)]
    return tiles + [edge_cells(a) for a in range(0, rows + 2, 2)]

def spread_lanes(w):
    return jnp.concatenate([w] * (LANES // w.shape[-1]), axis=-1)

def lane_iota(rows):
    return lax.broadcasted_iota(jnp.int32, (rows, LANES), 1)

def slot_mix(rows, taps, column_in, order, width):
    slot = lane_iota(rows) // width
    mixed = jnp.zeros((rows, LANES), F32)
    for place, column in enumerate(order):
        tap = column_in - column + 1
        if 0 <= tap < 3:
            mixed = jnp.where(slot == place, taps[tap], mixed)
    return mixed

def build_first(w_ref, o, w1):
    for k in range(6):
        for half in range(2):
            order = ODD_ORDER if half else EVEN_ORDER
            mixes = []
            for ti in range(3):
                taps = [jnp.broadcast_to(spread_lanes(w_ref[o, ti, tj:tj+1, :].astype(F32)), (16, LANES)) for tj in range(3)]
                mixes.append(slot_mix(16, taps, k - 1, order, 32))
            row = lax.broadcasted_iota(jnp.int32, (16, LANES), 0)
            for t in range(4):
                value = jnp.zeros((16, LANES), F32)
                for ti in range(3):
                    value = jnp.where(row == 2 * t + half + ti, mixes[ti], value)
                at = t * 2 * LANES + half * LANES
                w1[k * 16:(k + 1) * 16, at:at + LANES] = value.astype(BF)

def build_hidden(w_ref, o, layer, wh):
    wide = [[spread_lanes(w_ref[o, layer, ti, tj].astype(F32)) for tj in range(3)] for ti in range(3)]
    inner = wide[0][0].shape[0]
    for n, tile in enumerate(window_cells(2)):
        for slot, (a, column) in enumerate(tile):
            at = n * LANES + slot * inner
            for half in range(2):
                ti = a - (half + 1) + 1
                if 0 <= ti < 3:
                    value = slot_mix(inner, wide[ti], column, ODD_ORDER if half else EVEN_ORDER, inner)
                else:
                    value = jnp.zeros((inner, LANES), F32)
                wh[layer, at:at + inner, half * LANES:(half + 1) * LANES] = value.astype(BF)

def column_of(row):
    inner = row.shape[1]
    r = lax.broadcasted_iota(jnp.int32, (inner, inner), 0)
    c = lax.broadcasted_iota(jnp.int32, (inner, inner), 1)
    picked = jnp.where(r == c, jnp.broadcast_to(row, (inner, inner)), 0.0)
    return jnp.broadcast_to(jnp.sum(picked, axis=1, keepdims=True), (inner, LANES))

def build_last(w_ref, o, wl):
    taps = [[column_of(w_ref[o, ti, tj:tj+1, :].astype(F32)) for tj in range(3)] for ti in range(3)]
    inner = taps[0][0].shape[0]
    lane = lane_iota(inner)
    row8 = lane % 8
    zero = jnp.zeros((inner, LANES), F32)
    rows = []
    for a in range(10):
        line = []
        for tj in range(3):
            value = zero
            for ti in range(3):
                if 0 <= a - ti < 8:
                    value = jnp.where(row8 == a - ti, taps[ti][tj], value)
            line.append(value)
        rows.append(line)
    for n, tile in enumerate(window_cells(8)):
        for slot, (a, column) in enumerate(tile):
            at = n * LANES + slot * inner
            wl[at:at + inner, :] = slot_mix(inner, rows[a], column, EVEN_ORDER, LANES // 4).astype(BF)


def axial_kernel(plan, edges_ref, cur_ref, cf_ref, ch_ref, cl_ref, out_ref, main, edge, w1, wh, wl, raw, xs, place, back, gathered_out):
    halo, chunk = plan
    slices, local, columns = cur_ref.shape
    rows = local + 2 * halo
    stored = rows + 8
    groups = columns // 4
    per = groups // STRIPS
    span = slices * groups
    layers = ch_ref.shape[1]
    tile = lax.axis_index("tile")
    at_start = tile == 0
    at_end = tile == lax.axis_size("tile") - 1
    fill_rows(raw, edges_ref, cur_ref, stored, halo)

    build_first(cf_ref, 0, w1)
    for layer in range(layers):
        build_hidden(ch_ref, 0, layer, wh)
    build_last(cl_ref, 0, wl)

    col = lax.broadcasted_iota(jnp.int32, (columns, groups), 0)
    m = lax.broadcasted_iota(jnp.int32, (columns, groups), 1)
    first_col = 4 * ((m % STRIPS) * per + m // STRIPS)
    for k in range(6):
        place[:, k * groups:(k + 1) * groups] = jnp.where(col == first_col + (k - 1), 1.0, 0.0).astype(BF)
    m = lax.broadcasted_iota(jnp.int32, (groups, columns), 0)
    col = lax.broadcasted_iota(jnp.int32, (groups, columns), 1)
    first_col = 4 * ((m % STRIPS) * per + m // STRIPS)
    for k in range(4):
        back[k * groups:(k + 1) * groups, :] = jnp.where(col == first_col + k, 1.0, 0.0).astype(BF)
    xs[...] = jnp.dot(raw[...].astype(BF), place[...], preferred_element_type=F32)

    slot = lane_iota(STRIPS) // (LANES // 4)
    even_slots = (slot == 0) | (slot == 3)
    right_slots = slot < 2
    strip = lax.broadcasted_iota(jnp.int32, (STRIPS, LANES), 0)
    zero_tile = jnp.zeros((slices, per, STRIPS, LANES), BF)

    for side in range(2):
        for r in (0, 1, 2, rows - 1, rows, rows + 1):
            main[side, r] = zero_tile
        for e in (0, 1, rows // 2 - 1, rows // 2):
            edge[side, e] = zero_tile

    def put_edge(side, e, odd_row, even_row):
        v = jnp.where(even_slots, even_row, odd_row)
        for z in range(slices):
            for i in range(per):
                if i + 1 < per:
                    right = v[z, i + 1]
                else:
                    right = jnp.where(strip == STRIPS - 1, 0.0, pltpu.roll(v[z, 0], STRIPS - 1, 0))
                if i > 0:
                    left = v[z, i - 1]
                else:
                    left = jnp.where(strip == 0, 0.0, pltpu.roll(v[z, per - 1], 1, 0))
                edge[side, e, z, i] = jnp.where(right_slots, right, left).astype(BF)

    def put_pairs(side, pair, count, y):
        before = main[side, 2 * pair].astype(F32)
        for t in range(count):
            row = 2 * (pair + t)
            outside = (at_start & (row < halo)) | (at_end & (row >= rows - halo))
            v = jnp.maximum(y(t), 0.0) * jnp.where(outside, 0.0, 1.0)
            even_row = v[:, :LANES].reshape(slices, per, STRIPS, LANES)
            odd_row = v[:, LANES:].reshape(slices, per, STRIPS, LANES)
            main[side, row + 1] = even_row.astype(BF)
            main[side, row + 2] = odd_row.astype(BF)
            put_edge(side, pair + t, before, even_row)
            before = odd_row

    def first_step(c, carry):
        parts = []
        for z in range(slices):
            at = pl.ds(pl.multiple_of(z * stored + 8 * c, 8), 16)
            parts.append(jnp.concatenate([xs[at, k * groups:(k + 1) * groups] for k in range(6)], axis=0).astype(BF))
        x = jnp.concatenate(parts, axis=1)
        y = lax.dot_general(x, w1[...], (((0,), (0,)), ((), ())), preferred_element_type=F32)
        put_pairs(0, 4 * c, 4, lambda t: y[:, t * 2 * LANES:(t + 1) * 2 * LANES])
        return carry

    lax.fori_loop(0, rows // 8, first_step, 0)

    def window(side, pair, out_rows):
        parts = [main[side, 2 * pair + a].reshape(span, LANES) for a in range(out_rows + 2)]
        parts += [edge[side, pair + e].reshape(span, LANES) for e in range(out_rows // 2 + 1)]
        return jnp.concatenate(parts, axis=1)

    pairs = rows // 2 - 2
    for layer in range(layers):
        source, target = layer % 2, (layer + 1) % 2

        def hidden_step(c, carry):
            pair = 1 + c * chunk
            x = jnp.concatenate([window(source, pair + t, 2) for t in range(chunk)], axis=0)
            y = jnp.dot(x, wh[layer], preferred_element_type=F32)
            put_pairs(target, pair, chunk, lambda t: y[t * span:(t + 1) * span])
            return carry

        lax.fori_loop(0, pairs // chunk, hidden_step, 0)
        end = rows // 2 - 1
        put_edge(target, end, main[target, 2 * end].astype(F32), jnp.zeros((slices, per, STRIPS, LANES), F32))

    eighths = local // 8
    quad = (lane_iota(span) // 8) % 4

    def last_step(q, carry):
        x = window(layers % 2, halo // 2 + 4 * q, 8)
        y = jnp.dot(x, wl[...], preferred_element_type=F32)
        gathered_out[q // 4] = jnp.where(quad == q % 4, y, gathered_out[q // 4])
        return carry

    gathered_out[...] = jnp.zeros_like(gathered_out)
    lax.fori_loop(0, eighths, last_step, 0)

    for big in range(gathered_out.shape[0]):
        height = min(32, local - 32 * big)
        turned = [gathered_out[big, z * groups:(z + 1) * groups, :].T for z in range(slices)]
        lines = [jnp.concatenate([turned[z][k * 32:(k + 1) * 32] for k in range(4)], axis=1) for z in range(slices)]
        values = jnp.concatenate(lines, axis=0)
        high = values.astype(BF)
        low = (values - high.astype(F32)).astype(BF)
        net = jnp.dot(high, back[...], preferred_element_type=F32) + jnp.dot(low, back[...], preferred_element_type=F32)
        for z in range(slices):
            at = pl.ds(32 * big, height)
            out_ref[z, at, :] = cur_ref[z, at, :] - 2.0 * net[z * 32:z * 32 + height]

def axial_reflect(edges, current, cf, ch, cl, halo):
    slices, local, columns = current.shape
    rows = local + 2 * halo
    groups = columns // 4
    per = groups // STRIPS
    stored = rows + 8
    whole = pl.BlockSpec(memory_space=pltpu.VMEM)
    return pl.pallas_call(
        functools.partial(axial_kernel, (halo, 2)),
        out_shape=jax.ShapeDtypeStruct(current.shape, F32),
        in_specs=[whole] * 5,
        out_specs=whole,
        scratch_shapes=[
            pltpu.VMEM((2, rows + 2, slices, per, STRIPS, LANES), BF),
            pltpu.VMEM((2, rows // 2 + 1, slices, per, STRIPS, LANES), BF),
            pltpu.VMEM((96, 8 * LANES), BF),
            pltpu.VMEM((ch.shape[1], 6 * LANES, 2 * LANES), BF),
            pltpu.VMEM((15 * LANES, LANES), BF),
            pltpu.VMEM((slices * stored, columns), F32),
            pltpu.VMEM((slices * stored, 6 * groups), F32),
            pltpu.VMEM((columns, 6 * groups), BF),
            pltpu.VMEM((4 * groups, columns), BF),
            pltpu.VMEM((-(-local // 32), slices * groups, LANES), F32),
        ],
        compiler_params=pltpu.CompilerParams(vmem_limit_bytes=60 * 1024 * 1024),
        name="net_axial",
    )(edges, current, cf, ch, cl)


def fill_rows(raw, edges_ref, cur_ref, stored, halo):
    slices, local, columns = cur_ref.shape
    zero = jnp.zeros((1, columns), F32)
    tail = jnp.zeros((stored - 1 - local - 2 * halo, columns), F32)
    for z in range(slices):
        above = edges_ref[0, z * halo:(z + 1) * halo, :].astype(F32)
        below = edges_ref[1, z * halo:(z + 1) * halo, :].astype(F32)
        raw[z * stored:(z + 1) * stored, :] = jnp.concatenate([zero, above, cur_ref[z], below, tail], axis=0)


def build_first_plane(w_ref, o, w1):
    row = lax.broadcasted_iota(jnp.int32, (16, LANES), 0)
    for z in range(4):
        mixes = []
        for tj in range(3):
            taps = [jnp.broadcast_to(spread_lanes(w_ref[o, ti, tj:tj+1, :].astype(F32)), (16, LANES)) for ti in range(3)]
            mixes.append(slot_mix(16, taps, z, NATURAL, 32))
        for t in range(8):
            value = jnp.zeros((16, LANES), F32)
            for tj in range(3):
                value = jnp.where(row == t + tj, mixes[tj], value)
            w1[z * 16:(z + 1) * 16, t * LANES:(t + 1) * LANES] = value.astype(BF)

def build_hidden_plane(w_ref, o, layer, wh):
    wide = [[spread_lanes(w_ref[o, layer, ti, tj].astype(F32)) for ti in range(3)] for tj in range(3)]
    inner = wide[0][0].shape[0]
    for a in range(4):
        for z in range(4):
            at = a * LANES + z * inner
            for half in range(2):
                if 0 <= a - half < 3:
                    value = slot_mix(inner, wide[a - half], z, NATURAL, inner)
                else:
                    value = jnp.zeros((inner, LANES), F32)
                wh[layer, at:at + inner, half * LANES:(half + 1) * LANES] = value.astype(BF)

def build_last_plane(w_ref, o, wl):
    taps = [[column_of(w_ref[o, ti, tj:tj+1, :].astype(F32)) for ti in range(3)] for tj in range(3)]
    inner = taps[0][0].shape[0]
    row8 = lane_iota(inner) % 8
    zero = jnp.zeros((inner, LANES), F32)
    for a in range(10):
        line = []
        for ti in range(3):
            value = zero
            for tj in range(3):
                if 0 <= a - tj < 8:
                    value = jnp.where(row8 == a - tj, taps[tj][ti], value)
            line.append(value)
        for z in range(4):
            at = a * LANES + z * inner
            wl[at:at + inner, :] = slot_mix(inner, line, z, NATURAL, LANES // 4).astype(BF)


def plane_kernel(plan, x_ref, cur_ref, cf_ref, ch_ref, cl_ref, out_ref, main, w1, wh, wl, xs, gathered_out):
    o, halo, chunk, strips = plan
    slices, local, span = out_ref.shape
    rows = local + 2 * halo
    stored = rows + 8
    layers = ch_ref.shape[1]
    if halo:
        tile = lax.axis_index("tile")
        at_start = tile == 0
        at_end = tile == lax.axis_size("tile") - 1

    build_first_plane(cf_ref, o, w1)
    for layer in range(layers):
        build_hidden_plane(ch_ref, o, layer, wh)
    build_last_plane(cl_ref, o, wl)
    if halo:
        fill_rows(xs, x_ref, cur_ref, stored, halo)
    else:
        xs[...] = x_ref[...].astype(F32)
    for side in range(2):
        for r in (0, rows + 1):
            main[side, r] = jnp.zeros((span, LANES), BF)

    def put_pairs(side, pair, count, y):
        for t in range(count):
            row = 2 * (pair + t)
            v = jnp.maximum(y(t), 0.0)
            if halo:
                outside = (at_start & (row < halo)) | (at_end & (row >= rows - halo))
                v = v * jnp.where(outside, 0.0, 1.0)
            main[side, row + 1] = v[:, :LANES].astype(BF)
            main[side, row + 2] = v[:, LANES:].astype(BF)

    def ends(side):
        if strips > 1:
            step = span // strips
            main[side, 0, step:span] = main[side, rows, 0:span - step]
            main[side, rows + 1, 0:span - step] = main[side, 1, step:span]

    def first_step(c, carry):
        parts = [xs[pl.ds(pl.multiple_of(z * stored + 8 * c, 8), 16)] for z in range(slices)]
        x = jnp.concatenate(parts, axis=0).astype(BF)
        y = lax.dot_general(x, w1[...], (((0,), (0,)), ((), ())), preferred_element_type=F32)
        put_pairs(0, 4 * c, 4, lambda t: y[:, t * 2 * LANES:(t + 1) * 2 * LANES])
        return carry

    lax.fori_loop(0, rows // 8, first_step, 0)
    ends(0)

    for layer in range(layers):
        source, target = layer % 2, (layer + 1) % 2

        def hidden_step(c, carry):
            pair = c * chunk
            tiles = [main[source, 2 * pair + a] for a in range(2 * chunk + 2)]
            x = jnp.concatenate([jnp.concatenate(tiles[2 * t:2 * t + 4], axis=1) for t in range(chunk)], axis=0)
            y = jnp.dot(x, wh[layer], preferred_element_type=F32)
            put_pairs(target, pair, chunk, lambda t: y[t * span:(t + 1) * span])
            return carry

        lax.fori_loop(0, rows // 2 // chunk, hidden_step, 0)
        ends(target)

    quad = (lane_iota(span) // 8) % 4

    def last_step(q, carry):
        x = jnp.concatenate([main[layers % 2, halo + 8 * q + a] for a in range(10)], axis=1)
        y = jnp.dot(x, wl[...], preferred_element_type=F32)
        gathered_out[q // 4] = jnp.where(quad == q % 4, y, gathered_out[q // 4])
        return carry

    gathered_out[...] = jnp.zeros_like(gathered_out)
    lax.fori_loop(0, local // 8, last_step, 0)
    for big in range(gathered_out.shape[0]):
        height = min(32, local - 32 * big)
        net = gathered_out[big].T
        for z in range(slices):
            at = pl.ds(32 * big, height)
            out_ref[z, at, :] = cur_ref[z, at, :] - 2.0 * net[z * 32:z * 32 + height]

def plane_call(o, x, current, cf, ch, cl, halo, strips):
    slices, local, span = current.shape
    rows = local + 2 * halo
    whole = pl.BlockSpec(memory_space=pltpu.VMEM)
    return pl.pallas_call(
        functools.partial(plane_kernel, (o, halo, 4, strips)),
        out_shape=jax.ShapeDtypeStruct(current.shape, F32),
        in_specs=[whole] * 5, out_specs=whole,
        scratch_shapes=[
            pltpu.VMEM((2, rows + 2, span, LANES), BF),
            pltpu.VMEM((64, 8 * LANES), BF),
            pltpu.VMEM((ch.shape[1], 4 * LANES, 2 * LANES), BF),
            pltpu.VMEM((10 * LANES, LANES), BF),
            pltpu.VMEM((slices * (rows + 8), span), F32),
            pltpu.VMEM((-(-local // 32), span, LANES), F32),
        ],
        compiler_params=pltpu.CompilerParams(vmem_limit_bytes=60 * 1024 * 1024),
        name="net_sagittal" if halo else "net_coronal",
    )(x, current, cf, ch, cl)

def coronal_reflect(current, cf, ch, cl):
    slices, local, columns = current.shape
    strips = columns // local
    turned = jnp.transpose(current.reshape(slices, local, strips, local), (0, 3, 2, 1))
    t = turned.astype(BF)
    none = jnp.zeros((slices, 1, 1, local), BF)
    before = jnp.concatenate([none, t[:, -1:, :-1]], axis=2)
    after = jnp.concatenate([t[:, :1, 1:], none], axis=2)
    rest = jnp.zeros((slices, 6, strips, local), BF)
    x = jnp.concatenate([before, t, after, rest], axis=1)
    x = x.reshape(-1, columns)
    out = plane_call(2, x, turned.reshape(slices, local, columns), cf, ch, cl, 0, strips)
    return jnp.transpose(out.reshape(slices, local, strips, local), (0, 3, 2, 1)).reshape(current.shape)

def swap_halves(v):
    return pltpu.roll(v, 4, 0)

def block_pass(index_from, index_to, blocks, source, total, transposed, unroll=2):
    count = blocks.shape[0]
    low = lax.broadcasted_iota(jnp.int32, (8, LANES), 0) < 4
    zero = jnp.zeros((8, LANES), jnp.float32)

    def step(s, carry):
        b = s * 4
        picked = [source[index_from[b + j]] for j in range(4)]
        first = jnp.where(low, picked[0], picked[1])
        second = jnp.where(low, picked[2], picked[3])
        lhs = jnp.concatenate(
            [jnp.concatenate([first, zero], axis=0), jnp.concatenate([zero, second], axis=0)], axis=1
        ).astype(jnp.bfloat16)
        m = [blocks[b + j] for j in range(4)]
        if transposed:
            rhs = jnp.concatenate([jnp.concatenate([m[0], m[2]], axis=1), jnp.concatenate([m[1], m[3]], axis=1)], axis=0)
            y = lax.dot_general(lhs, rhs, (((1,), (1,)), ((), ())), preferred_element_type=jnp.float32)
        else:
            rhs = jnp.concatenate([jnp.concatenate([m[0], m[1]], axis=1), jnp.concatenate([m[2], m[3]], axis=1)], axis=0)
            y = jnp.dot(lhs, rhs, preferred_element_type=jnp.float32)
        parts = [
            jnp.where(low, y[:8, :LANES], 0.0),
            jnp.where(low, 0.0, y[:8, LANES:]),
            jnp.where(low, y[8:, :LANES], 0.0),
            jnp.where(low, 0.0, y[8:, LANES:]),
        ]
        for j in range(4):
            at = index_to[b + j]
            total[at] = total[at] + parts[j]
        return carry
    return step

def start_blocks(blocks_hbm, held, sems):
    n = blocks_hbm.shape[0] // CHUNK
    for i in range(n):
        pltpu.make_async_copy(blocks_hbm.at[pl.ds(i*CHUNK, CHUNK)], held.at[pl.ds(i*CHUNK, CHUNK)], sems.at[i]).start()

def wait_blocks(blocks_hbm, held, sems, i):
    pltpu.make_async_copy(blocks_hbm.at[pl.ds(i*CHUNK, CHUNK)], held.at[pl.ds(i*CHUNK, CHUNK)], sems.at[i]).wait()

def sweep(step, blocks_hbm, held, sems, waiting, unroll):
    n = held.shape[0] // CHUNK
    per = CHUNK // 4
    def chunk(i, c):
        if waiting:
            wait_blocks(blocks_hbm, held, sems, i)
        return lax.fori_loop(0, per // unroll, lambda s, c: functools.reduce(lambda c, u: step(i*per + s*unroll + u, c), range(unroll), c), c)
    lax.fori_loop(0, n, chunk, 0)

def compact(total, part_ref):
    low = lax.broadcasted_iota(jnp.int32, (8, LANES), 0) < 4
    pairs = total.shape[0] // 4
    def step(k, c):
        out = []
        for j in range(2):
            a = total[4*k + 2*j]; b = total[4*k + 2*j + 1]
            out.append(jnp.where(low, a + swap_halves(a), b + swap_halves(b)))
        part_ref[pl.ds(pl.multiple_of(16*k,16), 16)] = jnp.concatenate(out, axis=0).astype(jnp.bfloat16)
        return c
    lax.fori_loop(0, pairs, step, 0, unroll=4)

def expand(res_ref, spread):
    low = lax.broadcasted_iota(jnp.int32, (8, LANES), 0) < 4
    n = res_ref.shape[0] // 16
    def step(k, c):
        v = res_ref[pl.ds(pl.multiple_of(16*k,16), 16)].astype(jnp.float32)
        for j in range(2):
            u = v[8*j:8*j+8]
            w = swap_halves(u)
            spread[4*k + 2*j] = jnp.where(low, u, w)
            spread[4*k + 2*j + 1] = jnp.where(low, w, u)
        return c
    lax.fori_loop(0, n, step, 0, unroll=4)

def clear(ref, unroll=8):
    z = jnp.zeros((8,) + ref.shape[1:], ref.dtype)
    def step(i, c):
        ref[pl.ds(i*8, 8)] = z
        return c
    lax.fori_loop(0, ref.shape[0]//8, step, 0)

def project_kernel(rays, tiles, blocks_hbm, pixels, part_ref, held, total, sems):
    start_blocks(blocks_hbm, held, sems)
    clear(total)
    step = block_pass(tiles, rays, held, pixels, total, True)
    sweep(step, blocks_hbm, held, sems, True, UNROLL)
    compact(total, part_ref)

def back_update(rays, tiles, blocks_hbm, res_ref, pixels, moved_ref, held, spread, sems):
    start_blocks(blocks_hbm, held, sems)
    expand(res_ref, spread)
    clear(moved_ref)
    sweep(block_pass(rays, tiles, held, spread, moved_ref, False), blocks_hbm, held, sems, True, UNROLL)


def advance_kernel(rays, tiles, blocks_hbm, res_ref, pixels, part_ref, moved_ref, held, spread, total, sems):
    back_update(rays, tiles, blocks_hbm, res_ref, pixels, moved_ref, held, spread, sems)
    clear(total)

    def update(i, carry):
        at = pl.ds(i * 8, 8)
        a = moved_ref[at]
        moved_ref[at] = pixels[at] - 0.8 * (a + pltpu.roll(a, 4, 1))
        return carry

    lax.fori_loop(0, moved_ref.shape[0] // 8, update, 0)
    sweep(block_pass(tiles, rays, held, moved_ref, total, True), blocks_hbm, held, sems, False, UNROLL)
    compact(total, part_ref)


def settle_kernel(rays, tiles, blocks_hbm, res_ref, pixels, first_ref, out_ref, held, spread, sems):
    back_update(rays, tiles, blocks_hbm, res_ref, pixels, out_ref, held, spread, sems)

    def update(i, carry):
        at = pl.ds(i * 8, 8)
        a = out_ref[at]
        moved = pixels[at] - 0.8 * (a + pltpu.roll(a, 4, 1))
        out_ref[at] = 2.0 * moved - first_ref[at]
        return carry

    lax.fori_loop(0, out_ref.shape[0] // 8, update, 0)


def data_call(kernel, name, ins, outs, blocks, scratch):
    vmem = pl.BlockSpec(memory_space=pltpu.VMEM)
    smem = pl.BlockSpec(memory_space=pltpu.SMEM)
    anywhere = pl.BlockSpec(memory_space=pl.ANY)
    return pl.pallas_call(
        kernel,
        out_shape=outs,
        in_specs=[smem, smem, anywhere] + [vmem] * (len(ins) - 3),
        out_specs=jax.tree.map(lambda _: vmem, outs),
        scratch_shapes=[pltpu.VMEM(blocks.shape, BF)]
        + [pltpu.VMEM(s, F32) for s in scratch]
        + [pltpu.SemaphoreType.DMA((blocks.shape[0] // CHUNK,))],
        compiler_params=pltpu.CompilerParams(vmem_limit_bytes=40 * 1024 * 1024),
        name=name,
    )(*ins)


def halo_kernel(halo, cur_hbm, out_ref, edge, sent, load, send, recv):
    agent = lax.axis_index("agent")
    tile = lax.axis_index("tile")
    last = lax.axis_size("tile") - 1
    slices, local, columns = cur_hbm.shape
    rows = edge.shape[2]
    active = (agent == 1) | (agent == 2)

    def copy(side, peer):
        return pltpu.make_async_remote_copy(
            src_ref=sent.at[side],
            dst_ref=out_ref.at[1 - side],
            send_sem=send.at[side],
            recv_sem=recv.at[1 - side],
            device_id=(agent, peer),
            device_id_type=MESH,
        )

    @pl.when(active)
    def _():
        barrier = pltpu.get_barrier_semaphore()

        @pl.when(tile > 0)
        def _():
            pl.semaphore_signal(barrier, inc=1, device_id=(agent, tile - 1), device_id_type=MESH)

        @pl.when(tile < last)
        def _():
            pl.semaphore_signal(barrier, inc=1, device_id=(agent, tile + 1), device_id_type=MESH)

        loads = [
            pltpu.make_async_copy(cur_hbm.at[:, pl.ds(0, rows)], edge.at[0], load.at[0]),
            pltpu.make_async_copy(cur_hbm.at[:, pl.ds(local - rows, rows)], edge.at[1], load.at[1]),
        ]
        for item in loads:
            item.start()
        for item in loads:
            item.wait()
        for side in range(2):
            first = 0 if side == 0 else rows - halo
            parts = [edge[side, z, first:first + halo, :] for z in range(slices)]
            sent[side] = jnp.concatenate(parts, axis=0).astype(BF)

        pl.semaphore_wait(barrier, jnp.where(tile > 0, 1, 0) + jnp.where(tile < last, 1, 0))

        @pl.when(tile > 0)
        def _():
            copy(0, tile - 1).start()

        @pl.when(tile < last)
        def _():
            copy(1, tile + 1).start()

        @pl.when(tile == 0)
        def _():
            out_ref[0] = jnp.zeros(out_ref.shape[1:], BF)

        @pl.when(tile == last)
        def _():
            out_ref[1] = jnp.zeros(out_ref.shape[1:], BF)

        @pl.when(tile > 0)
        def _():
            copy(1, tile - 1).wait_recv()

        @pl.when(tile < last)
        def _():
            copy(0, tile + 1).wait_recv()

        @pl.when(tile > 0)
        def _():
            copy(0, tile - 1).wait_send()

        @pl.when(tile < last)
        def _():
            copy(1, tile + 1).wait_send()


def halo_exchange(current, halo):
    slices, local, columns = current.shape
    return pl.pallas_call(
        functools.partial(halo_kernel, halo),
        out_shape=jax.ShapeDtypeStruct((2, slices * halo, columns), BF),
        in_specs=[pl.BlockSpec(memory_space=pl.ANY)],
        out_specs=pl.BlockSpec(memory_space=pltpu.VMEM),
        scratch_shapes=[
            pltpu.VMEM((2, slices, 8, columns), F32),
            pltpu.VMEM((2, slices * halo, columns), BF),
            pltpu.SemaphoreType.DMA((2,)),
            pltpu.SemaphoreType.DMA((2,)),
            pltpu.SemaphoreType.DMA((2,)),
        ],
        compiler_params=pltpu.CompilerParams(collective_id=2, has_side_effects=True),
        name="halo_exchange",
    )(current)


def ray_kernel(count, part_ref, sino_ref, out_ref, got, fresh, send1, recv1, send2, recv2):
    rows = sino_ref.shape[0]
    agent = lax.axis_index("agent")

    @pl.when(agent == 0)
    def _():
        me = lax.axis_index("tile")
        barrier = pltpu.get_barrier_semaphore()
        for d in range(1, count):
            pl.semaphore_signal(barrier, inc=1, device_id=(agent, lax.rem(me + d, count)), device_id_type=MESH)
        pl.semaphore_wait(barrier, count - 1)

        def part_copy(d):
            peer = lax.rem(me + d, count)
            return pltpu.make_async_remote_copy(
                src_ref=part_ref.at[peer],
                dst_ref=got.at[d],
                send_sem=send1.at[d],
                recv_sem=recv1.at[d],
                device_id=(agent, peer),
                device_id_type=MESH,
            )

        for d in range(1, count):
            part_copy(d).start()
        total = part_ref[me].astype(jnp.float32) - sino_ref[...]
        for d in range(1, count):
            part_copy(d).wait_recv()
            total = total + got[d].astype(jnp.float32)
        fresh[...] = total.astype(jnp.bfloat16)

        def rest_copy(d):
            return pltpu.make_async_remote_copy(
                src_ref=fresh,
                dst_ref=got2_slot(me),
                send_sem=send2.at[d],
                recv_sem=recv2.at[d],
                device_id=(agent, lax.rem(me + d, count)),
                device_id_type=MESH,
            )

        def got2_slot(slot):
            return out_ref.at[slot]

        for d in range(1, count):
            rest_copy(d).start()
        out_ref[me] = fresh[...]
        for d in range(1, count):
            rest_copy(d).wait_recv()
        for d in range(1, count):
            part_copy(d).wait_send()
            rest_copy(d).wait_send()


def ray_exchange(part, sinogram, count):
    rows = sinogram.shape[0]
    whole = pl.BlockSpec(memory_space=pltpu.VMEM)
    return pl.pallas_call(
        functools.partial(ray_kernel, count),
        out_shape=jax.ShapeDtypeStruct((count, rows, LANES), jnp.bfloat16),
        in_specs=[whole] * 2,
        out_specs=whole,
        scratch_shapes=[
            pltpu.VMEM((count, rows, LANES), jnp.bfloat16),
            pltpu.VMEM((rows, LANES), jnp.bfloat16),
            pltpu.SemaphoreType.DMA((count,)),
            pltpu.SemaphoreType.DMA((count,)),
            pltpu.SemaphoreType.DMA((count,)),
            pltpu.SemaphoreType.DMA((count,)),
        ],
        compiler_params=pltpu.CompilerParams(collective_id=0, has_side_effects=True),
        name="ray_exchange",
    )(part, sinogram)


def agent_kernel(own_ref, out_ref, near, pair, far, send, recv):
    me = lax.axis_index("agent")
    tile = lax.axis_index("tile")
    partner = me + 1 - 2 * (me % 2)
    across = (me + 2) % 4
    barrier = pltpu.get_barrier_semaphore()
    for peer in (partner, across):
        pl.semaphore_signal(barrier, inc=1, device_id=(peer, tile), device_id_type=MESH)
    pl.semaphore_wait(barrier, 2)

    first = pltpu.make_async_remote_copy(
        src_ref=own_ref,
        dst_ref=near,
        send_sem=send.at[0],
        recv_sem=recv.at[0],
        device_id=(partner, tile),
        device_id_type=MESH,
    )
    first.start()
    first.wait()
    pair[...] = (own_ref[...].astype(jnp.float32) + near[...].astype(jnp.float32)).astype(jnp.bfloat16)
    second = pltpu.make_async_remote_copy(
        src_ref=pair,
        dst_ref=far,
        send_sem=send.at[1],
        recv_sem=recv.at[1],
        device_id=(across, tile),
        device_id_type=MESH,
    )
    second.start()
    second.wait()
    out_ref[...] = near[...].astype(jnp.float32) + far[...].astype(jnp.float32)


def agent_sum(own):
    whole = pl.BlockSpec(memory_space=pltpu.VMEM)
    return pl.pallas_call(
        agent_kernel,
        out_shape=jax.ShapeDtypeStruct(own.shape, jnp.float32),
        in_specs=[whole],
        out_specs=whole,
        scratch_shapes=[
            pltpu.VMEM(own.shape, jnp.bfloat16),
            pltpu.VMEM(own.shape, jnp.bfloat16),
            pltpu.VMEM(own.shape, jnp.bfloat16),
            pltpu.SemaphoreType.DMA((2,)),
            pltpu.SemaphoreType.DMA((2,)),
        ],
        compiler_params=pltpu.CompilerParams(collective_id=1, has_side_effects=True),
        name="agent_sum",
    )(own)


def per_device(
    states,
    sinogram,
    blocks,
    block_angle,
    block_detector,
    block_tile,
    conv_first,
    conv_hidden,
    conv_last,
):
    current = states[0]
    slices, local_rows, image_columns = current.shape
    tile_count = lax.axis_size("tile")
    agent_place = lax.axis_index("agent")
    is_data = agent_place == 0
    tiles_here = local_rows * image_columns // LANES
    rays_here = sinogram.shape[0]
    ray_total = rays_here * tile_count
    part_shape = (tile_count, rays_here * slices, LANES)
    halo = conv_hidden.shape[1] + 2
    filters = (conv_first, conv_hidden, conv_last)
    rays = block_angle * (image_columns // LANES) + block_detector
    pixel_shape = jax.ShapeDtypeStruct((tiles_here, 2 * slices, LANES), F32)
    part_type = jax.ShapeDtypeStruct((ray_total * slices, LANES), BF)
    ray_shape = (ray_total, 2 * slices, LANES)

    def tiled():
        pixels = jnp.transpose(current.reshape(slices, tiles_here, LANES), (1, 0, 2))
        return jnp.concatenate([pixels, pixels], axis=1)

    edges = halo_exchange(current, halo)
    no_part = jnp.zeros(part_shape, BF)
    no_pixels = jnp.zeros(pixel_shape.shape, F32)

    def data_start():
        pixels = tiled()
        part = data_call(project_kernel, "project", (rays, block_tile, blocks, pixels), part_type, blocks, [ray_shape])
        return part.reshape(part_shape), pixels, current

    def axial_only():
        return no_part, no_pixels, axial_reflect(edges, current, *filters, halo)

    def sagittal_only():
        return no_part, no_pixels, plane_call(1, edges, current, *filters, halo, 1)

    def coronal_only():
        return no_part, no_pixels, coronal_reflect(current, *filters)

    part, pixels, reflect = lax.switch(agent_place, [data_start, axial_only, sagittal_only, coronal_only])
    own_sinogram = sinogram.reshape(rays_here * slices, LANES)
    first = pixels

    for step in range(DATA_STEPS):
        residual = ray_exchange(part, own_sinogram, tile_count)
        if step < DATA_STEPS - 1:

            def advance(pixels, residual):
                ins = (rays, block_tile, blocks, residual.reshape(part_type.shape), pixels)
                part, moved = data_call(
                    advance_kernel, "advance", ins, (part_type, pixel_shape), blocks, [ray_shape, ray_shape]
                )
                return part.reshape(part_shape), moved

            part, pixels = lax.cond(is_data, advance, lambda p, r: (no_part, p), pixels, residual)
        else:

            def settle(pixels, first, reflect, residual):
                ins = (rays, block_tile, blocks, residual.reshape(part_type.shape), pixels, first)
                out = data_call(settle_kernel, "settle", ins, pixel_shape, blocks, [ray_shape])
                return jnp.transpose(out[:, :slices], (1, 0, 2)).reshape(reflect.shape)

            reflect = lax.cond(is_data, settle, lambda p, f, s, r: s, pixels, first, reflect, residual)

    sent = reflect.astype(BF).reshape(slices * local_rows, image_columns)
    others = agent_sum(sent).reshape(reflect.shape)
    new_states = 0.5 * current + 0.25 * others - 0.25 * reflect
    return new_states[None]


def solution(mesh):
    placed = (
        P("agent", None, "tile", None),
        P("tile", None, None),
        P("tile", None, None),
        P("tile"),
        P("tile"),
        P("tile"),
        P(),
        P(),
        P(),
    )
    return jax.shard_map(
        per_device,
        mesh=mesh,
        in_specs=placed,
        out_specs=P("agent", None, "tile", None),
        check_vma=False,
    )
```

```python
import functools

import jax
import jax.numpy as jnp
from jax import lax
from jax.experimental import pallas as pl
from jax.experimental.pallas import tpu as pltpu
from jax.sharding import PartitionSpec as P

DATA_STEPS = 2
MESH = pl.DeviceIdType.MESH
LANES = 128
STRIPS = 16
CHUNK = 32
BF = jnp.bfloat16
F32 = jnp.float32
NATURAL = (0, 1, 2, 3)
EVEN_ORDER = (0, 1, 2, 3)
ODD_ORDER = (1, 0, 3, 2)


def main_cells(offset):
    order = EVEN_ORDER if offset % 2 else ODD_ORDER
    return [(offset, column) for column in order]

def edge_cells(offset):
    return [(offset + 1, 4), (offset, 4), (offset, -1), (offset + 1, -1)]

def window_cells(rows):
    tiles = [main_cells(a) for a in range(rows + 2)]
    return tiles + [edge_cells(a) for a in range(0, rows + 2, 2)]

def spread_lanes(w):
    return jnp.concatenate([w] * (LANES // w.shape[-1]), axis=-1)

def lane_iota(rows):
    return lax.broadcasted_iota(jnp.int32, (rows, LANES), 1)

def slot_mix(rows, taps, column_in, order, width):
    slot = lane_iota(rows) // width
    mixed = jnp.zeros((rows, LANES), F32)
    for place, column in enumerate(order):
        tap = column_in - column + 1
        if 0 <= tap < 3:
            mixed = jnp.where(slot == place, taps[tap], mixed)
    return mixed

def build_first(w_ref, o, w1):
    for k in range(6):
        for half in range(2):
            order = ODD_ORDER if half else EVEN_ORDER
            mixes = []
            for ti in range(3):
                taps = [jnp.broadcast_to(spread_lanes(w_ref[o, ti, tj:tj+1, :].astype(F32)), (16, LANES)) for tj in range(3)]
                mixes.append(slot_mix(16, taps, k - 1, order, 32))
            row = lax.broadcasted_iota(jnp.int32, (16, LANES), 0)
            for t in range(4):
                value = jnp.zeros((16, LANES), F32)
                for ti in range(3):
                    value = jnp.where(row == 2 * t + half + ti, mixes[ti], value)
                at = t * 2 * LANES + half * LANES
                w1[k * 16:(k + 1) * 16, at:at + LANES] = value.astype(BF)

def build_hidden(w_ref, o, layer, wh):
    wide = [[spread_lanes(w_ref[o, layer, ti, tj].astype(F32)) for tj in range(3)] for ti in range(3)]
    inner = wide[0][0].shape[0]
    for n, tile in enumerate(window_cells(2)):
        for slot, (a, column) in enumerate(tile):
            at = n * LANES + slot * inner
            for half in range(2):
                ti = a - (half + 1) + 1
                if 0 <= ti < 3:
                    value = slot_mix(inner, wide[ti], column, ODD_ORDER if half else EVEN_ORDER, inner)
                else:
                    value = jnp.zeros((inner, LANES), F32)
                wh[layer, at:at + inner, half * LANES:(half + 1) * LANES] = value.astype(BF)

def column_of(row):
    inner = row.shape[1]
    r = lax.broadcasted_iota(jnp.int32, (inner, inner), 0)
    c = lax.broadcasted_iota(jnp.int32, (inner, inner), 1)
    picked = jnp.where(r == c, jnp.broadcast_to(row, (inner, inner)), 0.0)
    return jnp.broadcast_to(jnp.sum(picked, axis=1, keepdims=True), (inner, LANES))

def build_last(w_ref, o, wl):
    taps = [[column_of(w_ref[o, ti, tj:tj+1, :].astype(F32)) for tj in range(3)] for ti in range(3)]
    inner = taps[0][0].shape[0]
    lane = lane_iota(inner)
    row8 = lane % 8
    zero = jnp.zeros((inner, LANES), F32)
    rows = []
    for a in range(10):
        line = []
        for tj in range(3):
            value = zero
            for ti in range(3):
                if 0 <= a - ti < 8:
                    value = jnp.where(row8 == a - ti, taps[ti][tj], value)
            line.append(value)
        rows.append(line)
    for n, tile in enumerate(window_cells(8)):
        for slot, (a, column) in enumerate(tile):
            at = n * LANES + slot * inner
            wl[at:at + inner, :] = slot_mix(inner, rows[a], column, EVEN_ORDER, LANES // 4).astype(BF)


def axial_kernel(plan, edges_ref, cur_ref, cf_ref, ch_ref, cl_ref, out_ref, main, edge, w1, wh, wl, raw, xs, place, back, gathered_out):
    halo, chunk = plan
    slices, local, columns = cur_ref.shape
    rows = local + 2 * halo
    stored = rows + 8
    groups = columns // 4
    per = groups // STRIPS
    span = slices * groups
    layers = ch_ref.shape[1]
    tile = lax.axis_index("tile")
    at_start = tile == 0
    at_end = tile == lax.axis_size("tile") - 1
    fill_rows(raw, edges_ref, cur_ref, stored, halo)

    build_first(cf_ref, 0, w1)
    for layer in range(layers):
        build_hidden(ch_ref, 0, layer, wh)
    build_last(cl_ref, 0, wl)

    col = lax.broadcasted_iota(jnp.int32, (columns, groups), 0)
    m = lax.broadcasted_iota(jnp.int32, (columns, groups), 1)
    first_col = 4 * ((m % STRIPS) * per + m // STRIPS)
    for k in range(6):
        place[:, k * groups:(k + 1) * groups] = jnp.where(col == first_col + (k - 1), 1.0, 0.0).astype(BF)
    m = lax.broadcasted_iota(jnp.int32, (groups, columns), 0)
    col = lax.broadcasted_iota(jnp.int32, (groups, columns), 1)
    first_col = 4 * ((m % STRIPS) * per + m // STRIPS)
    for k in range(4):
        back[k * groups:(k + 1) * groups, :] = jnp.where(col == first_col + k, 1.0, 0.0).astype(BF)
    xs[...] = jnp.dot(raw[...].astype(BF), place[...], preferred_element_type=F32)

    slot = lane_iota(STRIPS) // (LANES // 4)
    even_slots = (slot == 0) | (slot == 3)
    right_slots = slot < 2
    strip = lax.broadcasted_iota(jnp.int32, (STRIPS, LANES), 0)
    zero_tile = jnp.zeros((slices, per, STRIPS, LANES), BF)

    for side in range(2):
        for r in (0, 1, 2, rows - 1, rows, rows + 1):
            main[side, r] = zero_tile
        for e in (0, 1, rows // 2 - 1, rows // 2):
            edge[side, e] = zero_tile

    def put_edge(side, e, odd_row, even_row):
        v = jnp.where(even_slots, even_row, odd_row)
        for z in range(slices):
            for i in range(per):
                if i + 1 < per:
                    right = v[z, i + 1]
                else:
                    right = jnp.where(strip == STRIPS - 1, 0.0, pltpu.roll(v[z, 0], STRIPS - 1, 0))
                if i > 0:
                    left = v[z, i - 1]
                else:
                    left = jnp.where(strip == 0, 0.0, pltpu.roll(v[z, per - 1], 1, 0))
                edge[side, e, z, i] = jnp.where(right_slots, right, left).astype(BF)

    def put_pairs(side, pair, count, y):
        before = main[side, 2 * pair].astype(F32)
        for t in range(count):
            row = 2 * (pair + t)
            outside = (at_start & (row < halo)) | (at_end & (row >= rows - halo))
            v = jnp.maximum(y(t), 0.0) * jnp.where(outside, 0.0, 1.0)
            even_row = v[:, :LANES].reshape(slices, per, STRIPS, LANES)
            odd_row = v[:, LANES:].reshape(slices, per, STRIPS, LANES)
            main[side, row + 1] = even_row.astype(BF)
            main[side, row + 2] = odd_row.astype(BF)
            put_edge(side, pair + t, before, even_row)
            before = odd_row

    def first_step(c, carry):
        parts = []
        for z in range(slices):
            at = pl.ds(pl.multiple_of(z * stored + 8 * c, 8), 16)
            parts.append(jnp.concatenate([xs[at, k * groups:(k + 1) * groups] for k in range(6)], axis=0).astype(BF))
        x = jnp.concatenate(parts, axis=1)
        y = lax.dot_general(x, w1[...], (((0,), (0,)), ((), ())), preferred_element_type=F32)
        put_pairs(0, 4 * c, 4, lambda t: y[:, t * 2 * LANES:(t + 1) * 2 * LANES])
        return carry

    lax.fori_loop(0, rows // 8, first_step, 0)

    def window(side, pair, out_rows):
        parts = [main[side, 2 * pair + a].reshape(span, LANES) for a in range(out_rows + 2)]
        parts += [edge[side, pair + e].reshape(span, LANES) for e in range(out_rows // 2 + 1)]
        return jnp.concatenate(parts, axis=1)

    pairs = rows // 2 - 2
    for layer in range(layers):
        source, target = layer % 2, (layer + 1) % 2

        def hidden_step(c, carry):
            pair = 1 + c * chunk
            x = jnp.concatenate([window(source, pair + t, 2) for t in range(chunk)], axis=0)
            y = jnp.dot(x, wh[layer], preferred_element_type=F32)
            put_pairs(target, pair, chunk, lambda t: y[t * span:(t + 1) * span])
            return carry

        lax.fori_loop(0, pairs // chunk, hidden_step, 0)
        end = rows // 2 - 1
        put_edge(target, end, main[target, 2 * end].astype(F32), jnp.zeros((slices, per, STRIPS, LANES), F32))

    eighths = local // 8
    quad = (lane_iota(span) // 8) % 4

    def last_step(q, carry):
        x = window(layers % 2, halo // 2 + 4 * q, 8)
        y = jnp.dot(x, wl[...], preferred_element_type=F32)
        gathered_out[q // 4] = jnp.where(quad == q % 4, y, gathered_out[q // 4])
        return carry

    gathered_out[...] = jnp.zeros_like(gathered_out)
    lax.fori_loop(0, eighths, last_step, 0)

    for big in range(gathered_out.shape[0]):
        height = min(32, local - 32 * big)
        turned = [gathered_out[big, z * groups:(z + 1) * groups, :].T for z in range(slices)]
        lines = [jnp.concatenate([turned[z][k * 32:(k + 1) * 32] for k in range(4)], axis=1) for z in range(slices)]
        values = jnp.concatenate(lines, axis=0)
        high = values.astype(BF)
        low = (values - high.astype(F32)).astype(BF)
        net = jnp.dot(high, back[...], preferred_element_type=F32) + jnp.dot(low, back[...], preferred_element_type=F32)
        for z in range(slices):
            at = pl.ds(32 * big, height)
            out_ref[z, at, :] = cur_ref[z, at, :] - 2.0 * net[z * 32:z * 32 + height]

def axial_reflect(edges, current, cf, ch, cl, halo):
    slices, local, columns = current.shape
    rows = local + 2 * halo
    groups = columns // 4
    per = groups // STRIPS
    stored = rows + 8
    whole = pl.BlockSpec(memory_space=pltpu.VMEM)
    return pl.pallas_call(
        functools.partial(axial_kernel, (halo, 2)),
        out_shape=jax.ShapeDtypeStruct(current.shape, F32),
        in_specs=[whole] * 5,
        out_specs=whole,
        scratch_shapes=[
            pltpu.VMEM((2, rows + 2, slices, per, STRIPS, LANES), BF),
            pltpu.VMEM((2, rows // 2 + 1, slices, per, STRIPS, LANES), BF),
            pltpu.VMEM((96, 8 * LANES), BF),
            pltpu.VMEM((ch.shape[1], 6 * LANES, 2 * LANES), BF),
            pltpu.VMEM((15 * LANES, LANES), BF),
            pltpu.VMEM((slices * stored, columns), F32),
            pltpu.VMEM((slices * stored, 6 * groups), F32),
            pltpu.VMEM((columns, 6 * groups), BF),
            pltpu.VMEM((4 * groups, columns), BF),
            pltpu.VMEM((-(-local // 32), slices * groups, LANES), F32),
        ],
        compiler_params=pltpu.CompilerParams(vmem_limit_bytes=60 * 1024 * 1024),
        name="net_axial",
    )(edges, current, cf, ch, cl)


def fill_rows(raw, edges_ref, cur_ref, stored, halo):
    slices, local, columns = cur_ref.shape
    zero = jnp.zeros((1, columns), F32)
    tail = jnp.zeros((stored - 1 - local - 2 * halo, columns), F32)
    for z in range(slices):
        above = edges_ref[0, z * halo:(z + 1) * halo, :].astype(F32)
        below = edges_ref[1, z * halo:(z + 1) * halo, :].astype(F32)
        raw[z * stored:(z + 1) * stored, :] = jnp.concatenate([zero, above, cur_ref[z], below, tail], axis=0)


def build_first_plane(w_ref, o, w1):
    row = lax.broadcasted_iota(jnp.int32, (16, LANES), 0)
    for z in range(4):
        mixes = []
        for tj in range(3):
            taps = [jnp.broadcast_to(spread_lanes(w_ref[o, ti, tj:tj+1, :].astype(F32)), (16, LANES)) for ti in range(3)]
            mixes.append(slot_mix(16, taps, z, NATURAL, 32))
        for t in range(8):
            value = jnp.zeros((16, LANES), F32)
            for tj in range(3):
                value = jnp.where(row == t + tj, mixes[tj], value)
            w1[z * 16:(z + 1) * 16, t * LANES:(t + 1) * LANES] = value.astype(BF)

def build_hidden_plane(w_ref, o, layer, wh):
    wide = [[spread_lanes(w_ref[o, layer, ti, tj].astype(F32)) for ti in range(3)] for tj in range(3)]
    inner = wide[0][0].shape[0]
    for a in range(4):
        for z in range(4):
            at = a * LANES + z * inner
            for half in range(2):
                if 0 <= a - half < 3:
                    value = slot_mix(inner, wide[a - half], z, NATURAL, inner)
                else:
                    value = jnp.zeros((inner, LANES), F32)
                wh[layer, at:at + inner, half * LANES:(half + 1) * LANES] = value.astype(BF)

def build_last_plane(w_ref, o, wl):
    taps = [[column_of(w_ref[o, ti, tj:tj+1, :].astype(F32)) for ti in range(3)] for tj in range(3)]
    inner = taps[0][0].shape[0]
    row8 = lane_iota(inner) % 8
    zero = jnp.zeros((inner, LANES), F32)
    for a in range(10):
        line = []
        for ti in range(3):
            value = zero
            for tj in range(3):
                if 0 <= a - tj < 8:
                    value = jnp.where(row8 == a - tj, taps[tj][ti], value)
            line.append(value)
        for z in range(4):
            at = a * LANES + z * inner
            wl[at:at + inner, :] = slot_mix(inner, line, z, NATURAL, LANES // 4).astype(BF)


def plane_kernel(plan, x_ref, cur_ref, cf_ref, ch_ref, cl_ref, out_ref, main, w1, wh, wl, xs, gathered_out):
    o, halo, chunk, strips = plan
    slices, local, span = out_ref.shape
    rows = local + 2 * halo
    stored = rows + 8
    layers = ch_ref.shape[1]
    if halo:
        tile = lax.axis_index("tile")
        at_start = tile == 0
        at_end = tile == lax.axis_size("tile") - 1

    build_first_plane(cf_ref, o, w1)
    for layer in range(layers):
        build_hidden_plane(ch_ref, o, layer, wh)
    build_last_plane(cl_ref, o, wl)
    if halo:
        fill_rows(xs, x_ref, cur_ref, stored, halo)
    else:
        xs[...] = x_ref[...].astype(F32)
    for side in range(2):
        for r in (0, rows + 1):
            main[side, r] = jnp.zeros((span, LANES), BF)

    def put_pairs(side, pair, count, y):
        for t in range(count):
            row = 2 * (pair + t)
            v = jnp.maximum(y(t), 0.0)
            if halo:
                outside = (at_start & (row < halo)) | (at_end & (row >= rows - halo))
                v = v * jnp.where(outside, 0.0, 1.0)
            main[side, row + 1] = v[:, :LANES].astype(BF)
            main[side, row + 2] = v[:, LANES:].astype(BF)

    def ends(side):
        if strips > 1:
            step = span // strips
            main[side, 0, step:span] = main[side, rows, 0:span - step]
            main[side, rows + 1, 0:span - step] = main[side, 1, step:span]

    def first_step(c, carry):
        parts = [xs[pl.ds(pl.multiple_of(z * stored + 8 * c, 8), 16)] for z in range(slices)]
        x = jnp.concatenate(parts, axis=0).astype(BF)
        y = lax.dot_general(x, w1[...], (((0,), (0,)), ((), ())), preferred_element_type=F32)
        put_pairs(0, 4 * c, 4, lambda t: y[:, t * 2 * LANES:(t + 1) * 2 * LANES])
        return carry

    lax.fori_loop(0, rows // 8, first_step, 0)
    ends(0)

    for layer in range(layers):
        source, target = layer % 2, (layer + 1) % 2

        def hidden_step(c, carry):
            pair = c * chunk
            tiles = [main[source, 2 * pair + a] for a in range(2 * chunk + 2)]
            x = jnp.concatenate([jnp.concatenate(tiles[2 * t:2 * t + 4], axis=1) for t in range(chunk)], axis=0)
            y = jnp.dot(x, wh[layer], preferred_element_type=F32)
            put_pairs(target, pair, chunk, lambda t: y[t * span:(t + 1) * span])
            return carry

        lax.fori_loop(0, rows // 2 // chunk, hidden_step, 0)
        ends(target)

    quad = (lane_iota(span) // 8) % 4

    def last_step(q, carry):
        x = jnp.concatenate([main[layers % 2, halo + 8 * q + a] for a in range(10)], axis=1)
        y = jnp.dot(x, wl[...], preferred_element_type=F32)
        gathered_out[q // 4] = jnp.where(quad == q % 4, y, gathered_out[q // 4])
        return carry

    gathered_out[...] = jnp.zeros_like(gathered_out)
    lax.fori_loop(0, local // 8, last_step, 0)
    for big in range(gathered_out.shape[0]):
        height = min(32, local - 32 * big)
        net = gathered_out[big].T
        for z in range(slices):
            at = pl.ds(32 * big, height)
            out_ref[z, at, :] = cur_ref[z, at, :] - 2.0 * net[z * 32:z * 32 + height]

def plane_call(o, x, current, cf, ch, cl, halo, strips):
    slices, local, span = current.shape
    rows = local + 2 * halo
    whole = pl.BlockSpec(memory_space=pltpu.VMEM)
    return pl.pallas_call(
        functools.partial(plane_kernel, (o, halo, 4, strips)),
        out_shape=jax.ShapeDtypeStruct(current.shape, F32),
        in_specs=[whole] * 5, out_specs=whole,
        scratch_shapes=[
            pltpu.VMEM((2, rows + 2, span, LANES), BF),
            pltpu.VMEM((64, 8 * LANES), BF),
            pltpu.VMEM((ch.shape[1], 4 * LANES, 2 * LANES), BF),
            pltpu.VMEM((10 * LANES, LANES), BF),
            pltpu.VMEM((slices * (rows + 8), span), F32),
            pltpu.VMEM((-(-local // 32), span, LANES), F32),
        ],
        compiler_params=pltpu.CompilerParams(vmem_limit_bytes=60 * 1024 * 1024),
        name="net_sagittal" if halo else "net_coronal",
    )(x, current, cf, ch, cl)

def coronal_reflect(current, cf, ch, cl):
    slices, local, columns = current.shape
    strips = columns // local
    turned = jnp.transpose(current.reshape(slices, local, strips, local), (0, 3, 2, 1))
    t = turned.astype(BF)
    none = jnp.zeros((slices, 1, 1, local), BF)
    before = jnp.concatenate([none, t[:, -1:, :-1]], axis=2)
    after = jnp.concatenate([t[:, :1, 1:], none], axis=2)
    rest = jnp.zeros((slices, 6, strips, local), BF)
    x = jnp.concatenate([before, t, after, rest], axis=1)
    x = x.reshape(-1, columns)
    out = plane_call(2, x, turned.reshape(slices, local, columns), cf, ch, cl, 0, strips)
    return jnp.transpose(out.reshape(slices, local, strips, local), (0, 3, 2, 1)).reshape(current.shape)

def halo_kernel(halo, cur_hbm, out_ref, edge, sent, load, send, recv):
    agent = lax.axis_index("agent")
    tile = lax.axis_index("tile")
    last = lax.axis_size("tile") - 1
    slices, local, columns = cur_hbm.shape
    rows = edge.shape[2]
    active = (agent == 1) | (agent == 2)

    def copy(side, peer):
        return pltpu.make_async_remote_copy(
            src_ref=sent.at[side],
            dst_ref=out_ref.at[1 - side],
            send_sem=send.at[side],
            recv_sem=recv.at[1 - side],
            device_id=(agent, peer),
            device_id_type=MESH,
        )

    @pl.when(active)
    def _():
        barrier = pltpu.get_barrier_semaphore()

        @pl.when(tile > 0)
        def _():
            pl.semaphore_signal(barrier, inc=1, device_id=(agent, tile - 1), device_id_type=MESH)

        @pl.when(tile < last)
        def _():
            pl.semaphore_signal(barrier, inc=1, device_id=(agent, tile + 1), device_id_type=MESH)

        loads = [
            pltpu.make_async_copy(cur_hbm.at[:, pl.ds(0, rows)], edge.at[0], load.at[0]),
            pltpu.make_async_copy(cur_hbm.at[:, pl.ds(local - rows, rows)], edge.at[1], load.at[1]),
        ]
        for item in loads:
            item.start()
        for item in loads:
            item.wait()
        for side in range(2):
            first = 0 if side == 0 else rows - halo
            parts = [edge[side, z, first:first + halo, :] for z in range(slices)]
            sent[side] = jnp.concatenate(parts, axis=0).astype(BF)

        pl.semaphore_wait(barrier, jnp.where(tile > 0, 1, 0) + jnp.where(tile < last, 1, 0))

        @pl.when(tile > 0)
        def _():
            copy(0, tile - 1).start()

        @pl.when(tile < last)
        def _():
            copy(1, tile + 1).start()

        @pl.when(tile == 0)
        def _():
            out_ref[0] = jnp.zeros(out_ref.shape[1:], BF)

        @pl.when(tile == last)
        def _():
            out_ref[1] = jnp.zeros(out_ref.shape[1:], BF)

        @pl.when(tile > 0)
        def _():
            copy(1, tile - 1).wait_recv()

        @pl.when(tile < last)
        def _():
            copy(0, tile + 1).wait_recv()

        @pl.when(tile > 0)
        def _():
            copy(0, tile - 1).wait_send()

        @pl.when(tile < last)
        def _():
            copy(1, tile + 1).wait_send()


def halo_exchange(current, halo):
    slices, local, columns = current.shape
    return pl.pallas_call(
        functools.partial(halo_kernel, halo),
        out_shape=jax.ShapeDtypeStruct((2, slices * halo, columns), BF),
        in_specs=[pl.BlockSpec(memory_space=pl.ANY)],
        out_specs=pl.BlockSpec(memory_space=pltpu.VMEM),
        scratch_shapes=[
            pltpu.VMEM((2, slices, 8, columns), F32),
            pltpu.VMEM((2, slices * halo, columns), BF),
            pltpu.SemaphoreType.DMA((2,)),
            pltpu.SemaphoreType.DMA((2,)),
            pltpu.SemaphoreType.DMA((2,)),
        ],
        compiler_params=pltpu.CompilerParams(collective_id=2, has_side_effects=True),
        name="halo_exchange",
    )(current)


def swap_bits(me, d):
    peer, bit = me, 1
    while bit <= d:
        if d & bit:
            peer = peer + bit * (1 - 2 * ((me // bit) % 2))
        bit *= 2
    return peer


def block_copy(blocks_hbm, held, sems, i):
    at = pl.ds(i * CHUNK, CHUNK)
    return pltpu.make_async_copy(blocks_hbm.at[at], held.at[at], sems.at[i])


def block_step(held, picked, y, slices, transposed, u):
    row = lax.broadcasted_iota(jnp.int32, (8, LANES), 0)
    at = pl.ds(pl.multiple_of(8 * u, 8), 8)
    p = [picked[at, z * LANES:(z + 1) * LANES] for z in range(slices)]
    halves = []
    for t in range(2):
        sides = []
        for side in range(2):
            mask = row // 2 == 2 * t + side
            sides.append(jnp.concatenate([jnp.where(mask, v, 0.0) for v in p], axis=0))
        lhs = jnp.concatenate(sides, axis=1).astype(BF)
        m = [held[8 * u + 4 * t + j] for j in range(4)]
        if transposed:
            top, bottom = jnp.concatenate([m[0], m[2]], axis=1), jnp.concatenate([m[1], m[3]], axis=1)
            dims = (((1,), (1,)), ((), ()))
        else:
            top, bottom = jnp.concatenate([m[0], m[1]], axis=1), jnp.concatenate([m[2], m[3]], axis=1)
            dims = (((1,), (0,)), ((), ()))
        rhs = jnp.concatenate([top, bottom], axis=0)
        halves.append(lax.dot_general(lhs, rhs, dims, preferred_element_type=F32))
    for z in range(slices):
        a, b = (h[8 * z:8 * z + 8] for h in halves)
        low = jnp.where(row < 4, a[:, :LANES], b[:, :LANES])
        high = jnp.where(row < 4, a[:, LANES:], b[:, LANES:])
        y[at, z * LANES:(z + 1) * LANES] = jnp.where(row % 2 == 0, low, high)


def block_sweep(blocks_hbm, held, sems, picked, y, slices, transposed, waiting):
    def chunk(i, carry):
        if waiting:
            block_copy(blocks_hbm, held, sems, i).wait()
        for j in range(CHUNK // 8):
            block_step(held, picked, y, slices, transposed, i * (CHUNK // 8) + j)
        return carry

    lax.fori_loop(0, held.shape[0] // CHUNK, chunk, 0)


def gather_rows(hot, source):
    return jnp.dot(hot, source, preferred_element_type=F32)


def scatter_rows(hot, y):
    high = y.astype(BF)
    low = (y - high.astype(F32)).astype(BF)
    return jnp.dot(
        jnp.concatenate([hot, hot], axis=1), jnp.concatenate([high, low], axis=0), preferred_element_type=F32
    )


def data_kernel(
    count, angle_ref, detector_ref, tile_ref, sino_ref, cur_hbm, blocks_hbm, out_ref,
    held, cur, ray_hot, ray_turned, tile_hot, tile_turned, x, y, picked, total, part, got, fresh, full,
    load, sems, send1, recv1, send2, recv2,
):
    agent = lax.axis_index("agent")
    me = lax.axis_index("tile")
    slices, local, columns = out_ref.shape
    detectors = columns // LANES
    rays_here = fresh.shape[1]
    ray_total = count * rays_here
    tiles_here = detectors * local
    blocks_here = held.shape[0]
    order = list(range(count - 1, 0, -1))

    def part_copy(step, d):
        return pltpu.make_async_remote_copy(
            src_ref=part.at[step, swap_bits(me, d)],
            dst_ref=got.at[step, d],
            send_sem=send1.at[step, d],
            recv_sem=recv1.at[step, d],
            device_id=(agent, swap_bits(me, d)),
            device_id_type=MESH,
        )

    def rest_copy(step, d):
        return pltpu.make_async_remote_copy(
            src_ref=fresh.at[step],
            dst_ref=full.at[step, me],
            send_sem=send2.at[step, d],
            recv_sem=recv2.at[step, d],
            device_id=(agent, swap_bits(me, d)),
            device_id_type=MESH,
        )

    def exchange(step):
        for slot in range(count):
            part[step, slot] = total[slot * rays_here:(slot + 1) * rays_here, :].astype(BF)
        for d in order:
            part_copy(step, d).start()
        own = total[pl.ds(pl.multiple_of(me * rays_here, 8), rays_here), :]
        measured = [sino_ref[pl.ds(z, rays_here, stride=slices), :] for z in range(slices)]
        value = own - jnp.concatenate(measured, axis=1)
        for d in reversed(order):
            part_copy(step, d).wait_recv()
            value = value + got[step, d].astype(F32)
        fresh[step] = value.astype(BF)
        for d in order:
            rest_copy(step, d).start()
        full[step, me] = fresh[step]
        for d in order:
            rest_copy(step, d).wait_recv()
        for d in order:
            part_copy(step, d).wait_send()
            rest_copy(step, d).wait_send()
        return full[step].reshape(ray_total, slices * LANES)

    @pl.when(agent == 0)
    def _():
        barrier = pltpu.get_barrier_semaphore()
        for d in order:
            pl.semaphore_signal(barrier, inc=1, device_id=(agent, swap_bits(me, d)), device_id_type=MESH)
        first = pltpu.make_async_copy(cur_hbm, cur, load.at[0])
        first.start()
        for i in range(blocks_here // CHUNK):
            block_copy(blocks_hbm, held, sems, i).start()

        hot_rows = lax.broadcasted_iota(jnp.int32, (ray_total, blocks_here), 0)
        ray = angle_ref[...] * detectors + detector_ref[...]
        hot = jnp.where(hot_rows == jnp.broadcast_to(ray, hot_rows.shape), 1.0, 0.0)
        ray_hot[...] = hot.astype(BF)
        ray_turned[...] = hot.T.astype(BF)
        hot_rows = lax.broadcasted_iota(jnp.int32, (tiles_here, blocks_here), 0)
        place = tile_ref[...]
        place = (place % detectors) * local + place // detectors
        hot = jnp.where(hot_rows == jnp.broadcast_to(place, hot_rows.shape), 1.0, 0.0)
        tile_hot[...] = hot.astype(BF)
        tile_turned[...] = hot.T.astype(BF)

        first.wait()
        for z in range(slices):
            for t in range(detectors):
                x[t * local:(t + 1) * local, z * LANES:(z + 1) * LANES] = cur[z, :, t * LANES:(t + 1) * LANES]

        for step in range(DATA_STEPS):
            picked[...] = gather_rows(tile_turned[...], x[...].astype(BF))
            block_sweep(blocks_hbm, held, sems, picked, y, slices, True, step == 0)
            total[...] = scatter_rows(ray_hot[...], y[...])
            if step == 0:
                pl.semaphore_wait(barrier, count - 1)
            picked[...] = gather_rows(ray_turned[...], exchange(step))
            block_sweep(blocks_hbm, held, sems, picked, y, slices, False, False)
            x[...] = x[...] - 0.8 * scatter_rows(tile_hot[...], y[...])

        for z in range(slices):
            for t in range(detectors):
                moved = x[t * local:(t + 1) * local, z * LANES:(z + 1) * LANES]
                at = slice(t * LANES, (t + 1) * LANES)
                out_ref[z, :, at] = 2.0 * moved - cur[z, :, at]


def data_reflect(angle, detector, tile, sinogram, current, blocks, count):
    slices, local, columns = current.shape
    rays_here = sinogram.shape[0]
    ray_total = rays_here * count
    tiles_here = columns // LANES * local
    blocks_here = blocks.shape[0]
    width = slices * LANES
    vmem = pl.BlockSpec(memory_space=pltpu.VMEM)
    anywhere = pl.BlockSpec(memory_space=pl.ANY)
    return pl.pallas_call(
        functools.partial(data_kernel, count),
        out_shape=jax.ShapeDtypeStruct(current.shape, F32),
        in_specs=[vmem] * 4 + [anywhere] * 2,
        out_specs=vmem,
        scratch_shapes=[
            pltpu.VMEM(blocks.shape, BF),
            pltpu.VMEM(current.shape, F32),
            pltpu.VMEM((ray_total, blocks_here), BF),
            pltpu.VMEM((blocks_here, ray_total), BF),
            pltpu.VMEM((tiles_here, blocks_here), BF),
            pltpu.VMEM((blocks_here, tiles_here), BF),
            pltpu.VMEM((tiles_here, width), F32),
            pltpu.VMEM((blocks_here, width), F32),
            pltpu.VMEM((blocks_here, width), F32),
            pltpu.VMEM((ray_total, width), F32),
            pltpu.VMEM((DATA_STEPS, count, rays_here, width), BF),
            pltpu.VMEM((DATA_STEPS, count, rays_here, width), BF),
            pltpu.VMEM((DATA_STEPS, rays_here, width), BF),
            pltpu.VMEM((DATA_STEPS, count, rays_here, width), BF),
            pltpu.SemaphoreType.DMA((1,)),
            pltpu.SemaphoreType.DMA((blocks_here // CHUNK,)),
            pltpu.SemaphoreType.DMA((DATA_STEPS, count)),
            pltpu.SemaphoreType.DMA((DATA_STEPS, count)),
            pltpu.SemaphoreType.DMA((DATA_STEPS, count)),
            pltpu.SemaphoreType.DMA((DATA_STEPS, count)),
        ],
        compiler_params=pltpu.CompilerParams(
            collective_id=0, has_side_effects=True, vmem_limit_bytes=40 * 1024 * 1024
        ),
        name="data_agent",
    )(
        angle.reshape(1, -1), detector.reshape(1, -1), tile.reshape(1, -1),
        sinogram.reshape(rays_here * slices, LANES), current, blocks,
    )


def agent_kernel(own_ref, out_ref, own, near, pair, far, s1, r1, s2, r2, s3, r3, s4, r4):
    me = lax.axis_index("agent")
    tile = lax.axis_index("tile")
    core = me % 2
    other = 1 - core
    partner = me + 1 - 2 * core
    across = (me + 2) % 4
    chunks = pair.shape[0]
    barrier = pltpu.get_barrier_semaphore()
    for peer in (partner, across):
        pl.semaphore_signal(barrier, inc=1, device_id=(peer, tile), device_id_type=MESH)
    own[...] = own_ref[...].astype(BF)
    pl.semaphore_wait(barrier, 2)

    def send(source, target, s, r, to):
        return pltpu.make_async_remote_copy(
            src_ref=source, dst_ref=target, send_sem=s, recv_sem=r, device_id=(to, tile), device_id_type=MESH
        )

    def first(k, half):
        return send(own.at[half, k], near.at[half, k], s1.at[k], r1.at[k], partner)

    def rest(half):
        return send(own.at[half], near.at[half], s2.at[0], r2.at[0], partner)

    def cross(k):
        return send(pair.at[k], far.at[core, k], s3.at[k], r3.at[k], across)

    def onward(k, half):
        return send(far.at[half, k], far.at[half, k], s4.at[k], r4.at[k], partner)

    def result(half, k):
        out_ref[half, k] = near[half, k].astype(F32) + far[half, k].astype(F32) - own_ref[half, k]

    for k in range(chunks):
        first(k, other).start()
    rest(core).start()
    for k in range(chunks):
        first(k, core).wait_recv()
        pair[k] = (own[core, k].astype(F32) + near[core, k].astype(F32)).astype(BF)
        cross(k).start()
    for k in range(chunks):
        cross(k).wait_recv()
        onward(k, core).start()
        result(core, k)
    rest(other).wait_recv()
    for k in range(chunks):
        onward(k, other).wait_recv()
        result(other, k)
    for k in range(chunks):
        first(k, other).wait_send()
        cross(k).wait_send()
        onward(k, core).wait_send()
    rest(core).wait_send()


def agent_sum(reflect):
    slices, local, columns = reflect.shape
    half = slices * local // 2
    chunks = max(1, half // 32)
    shape = (2, chunks, half // chunks, columns)
    whole = pl.BlockSpec(memory_space=pltpu.VMEM)
    out = pl.pallas_call(
        agent_kernel,
        out_shape=jax.ShapeDtypeStruct(shape, F32),
        in_specs=[whole],
        out_specs=whole,
        scratch_shapes=[
            pltpu.VMEM(shape, BF),
            pltpu.VMEM(shape, BF),
            pltpu.VMEM(shape[1:], BF),
            pltpu.VMEM(shape, BF),
            pltpu.SemaphoreType.DMA((chunks,)),
            pltpu.SemaphoreType.DMA((chunks,)),
            pltpu.SemaphoreType.DMA((1,)),
            pltpu.SemaphoreType.DMA((1,)),
            pltpu.SemaphoreType.DMA((chunks,)),
            pltpu.SemaphoreType.DMA((chunks,)),
            pltpu.SemaphoreType.DMA((chunks,)),
            pltpu.SemaphoreType.DMA((chunks,)),
        ],
        compiler_params=pltpu.CompilerParams(collective_id=1, has_side_effects=True),
        name="agent_sum",
    )(reflect.reshape(shape))
    return out.reshape(reflect.shape)


def per_device(
    states,
    sinogram,
    blocks,
    block_angle,
    block_detector,
    block_tile,
    conv_first,
    conv_hidden,
    conv_last,
):
    current = states[0]
    agent_place = lax.axis_index("agent")
    halo = conv_hidden.shape[1] + 2
    filters = (conv_first, conv_hidden, conv_last)
    edges = halo_exchange(current, halo)
    data = data_reflect(
        block_angle, block_detector, block_tile, sinogram, current, blocks, lax.axis_size("tile")
    )

    def data_only():
        return data

    def axial_only():
        return axial_reflect(edges, current, *filters, halo)

    def sagittal_only():
        return plane_call(1, edges, current, *filters, halo, 1)

    def coronal_only():
        return coronal_reflect(current, *filters)

    reflect = lax.switch(agent_place, [data_only, axial_only, sagittal_only, coronal_only])
    return (0.5 * current + 0.25 * agent_sum(reflect))[None]


def solution(mesh):
    placed = (
        P("agent", None, "tile", None),
        P("tile", None, None),
        P("tile", None, None),
        P("tile"),
        P("tile"),
        P("tile"),
        P(),
        P(),
        P(),
    )
    return jax.shard_map(
        per_device,
        mesh=mesh,
        in_specs=placed,
        out_specs=P("agent", None, "tile", None),
        check_vma=False,
    )
```

```python
import functools

import jax
import jax.numpy as jnp
from jax import lax
from jax.experimental import pallas as pl
from jax.experimental.pallas import tpu as pltpu
from jax.sharding import PartitionSpec as P

DATA_STEPS = 2
MESH = pl.DeviceIdType.MESH
LANES = 128
STRIPS = 16
CHUNK = 32
BF = jnp.bfloat16
F32 = jnp.float32
NATURAL = (0, 1, 2, 3)
EVEN_ORDER = (0, 1, 2, 3)
ODD_ORDER = (1, 0, 3, 2)


def main_cells(offset):
    order = EVEN_ORDER if offset % 2 else ODD_ORDER
    return [(offset, column) for column in order]

def edge_cells(offset):
    return [(offset + 1, 4), (offset, 4), (offset, -1), (offset + 1, -1)]

def window_cells(rows):
    tiles = [main_cells(a) for a in range(rows + 2)]
    return tiles + [edge_cells(a) for a in range(0, rows + 2, 2)]

def spread_lanes(w):
    return jnp.concatenate([w] * (LANES // w.shape[-1]), axis=-1)

def lane_iota(rows):
    return lax.broadcasted_iota(jnp.int32, (rows, LANES), 1)

def slot_mix(rows, taps, column_in, order, width):
    slot = lane_iota(rows) // width
    mixed = jnp.zeros((rows, LANES), F32)
    for place, column in enumerate(order):
        tap = column_in - column + 1
        if 0 <= tap < 3:
            mixed = jnp.where(slot == place, taps[tap], mixed)
    return mixed

def build_first(w_ref, o, w1):
    for k in range(6):
        for half in range(2):
            order = ODD_ORDER if half else EVEN_ORDER
            mixes = []
            for ti in range(3):
                taps = [jnp.broadcast_to(spread_lanes(w_ref[o, ti, tj:tj+1, :].astype(F32)), (16, LANES)) for tj in range(3)]
                mixes.append(slot_mix(16, taps, k - 1, order, 32))
            row = lax.broadcasted_iota(jnp.int32, (16, LANES), 0)
            for t in range(4):
                value = jnp.zeros((16, LANES), F32)
                for ti in range(3):
                    value = jnp.where(row == 2 * t + half + ti, mixes[ti], value)
                at = t * 2 * LANES + half * LANES
                w1[k * 16:(k + 1) * 16, at:at + LANES] = value.astype(BF)

def build_hidden(w_ref, o, layer, wh):
    wide = [[spread_lanes(w_ref[o, layer, ti, tj].astype(F32)) for tj in range(3)] for ti in range(3)]
    inner = wide[0][0].shape[0]
    for n, tile in enumerate(window_cells(2)):
        for slot, (a, column) in enumerate(tile):
            at = n * LANES + slot * inner
            for half in range(2):
                ti = a - (half + 1) + 1
                if 0 <= ti < 3:
                    value = slot_mix(inner, wide[ti], column, ODD_ORDER if half else EVEN_ORDER, inner)
                else:
                    value = jnp.zeros((inner, LANES), F32)
                wh[layer, at:at + inner, half * LANES:(half + 1) * LANES] = value.astype(BF)

def column_of(row):
    inner = row.shape[1]
    r = lax.broadcasted_iota(jnp.int32, (inner, inner), 0)
    c = lax.broadcasted_iota(jnp.int32, (inner, inner), 1)
    picked = jnp.where(r == c, jnp.broadcast_to(row, (inner, inner)), 0.0)
    return jnp.broadcast_to(jnp.sum(picked, axis=1, keepdims=True), (inner, LANES))

def build_last(w_ref, o, wl):
    taps = [[column_of(w_ref[o, ti, tj:tj+1, :].astype(F32)) for tj in range(3)] for ti in range(3)]
    inner = taps[0][0].shape[0]
    lane = lane_iota(inner)
    row8 = lane % 8
    zero = jnp.zeros((inner, LANES), F32)
    rows = []
    for a in range(10):
        line = []
        for tj in range(3):
            value = zero
            for ti in range(3):
                if 0 <= a - ti < 8:
                    value = jnp.where(row8 == a - ti, taps[ti][tj], value)
            line.append(value)
        rows.append(line)
    for n, tile in enumerate(window_cells(8)):
        for slot, (a, column) in enumerate(tile):
            at = n * LANES + slot * inner
            wl[at:at + inner, :] = slot_mix(inner, rows[a], column, EVEN_ORDER, LANES // 4).astype(BF)


def axial_kernel(plan, edges_ref, cur_ref, cf_ref, ch_ref, cl_ref, out_ref, main, edge, w1, wh, wl, raw, xs, place, back, gathered_out):
    halo, chunk = plan
    slices, local, columns = cur_ref.shape
    rows = local + 2 * halo
    stored = rows + 8
    groups = columns // 4
    per = groups // STRIPS
    span = slices * groups
    layers = ch_ref.shape[1]
    tile = lax.axis_index("tile")
    at_start = tile == 0
    at_end = tile == lax.axis_size("tile") - 1
    fill_rows(raw, edges_ref, cur_ref, stored, halo)

    build_first(cf_ref, 0, w1)
    for layer in range(layers):
        build_hidden(ch_ref, 0, layer, wh)
    build_last(cl_ref, 0, wl)

    col = lax.broadcasted_iota(jnp.int32, (columns, groups), 0)
    m = lax.broadcasted_iota(jnp.int32, (columns, groups), 1)
    first_col = 4 * ((m % STRIPS) * per + m // STRIPS)
    for k in range(6):
        place[:, k * groups:(k + 1) * groups] = jnp.where(col == first_col + (k - 1), 1.0, 0.0).astype(BF)
    m = lax.broadcasted_iota(jnp.int32, (groups, columns), 0)
    col = lax.broadcasted_iota(jnp.int32, (groups, columns), 1)
    first_col = 4 * ((m % STRIPS) * per + m // STRIPS)
    for k in range(4):
        back[k * groups:(k + 1) * groups, :] = jnp.where(col == first_col + k, 1.0, 0.0).astype(BF)
    xs[...] = jnp.dot(raw[...].astype(BF), place[...], preferred_element_type=F32)

    slot = lane_iota(STRIPS) // (LANES // 4)
    even_slots = (slot == 0) | (slot == 3)
    right_slots = slot < 2
    strip = lax.broadcasted_iota(jnp.int32, (STRIPS, LANES), 0)
    zero_tile = jnp.zeros((slices, per, STRIPS, LANES), BF)

    for side in range(2):
        for r in (0, 1, 2, rows - 1, rows, rows + 1):
            main[side, r] = zero_tile
        for e in (0, 1, rows // 2 - 1, rows // 2):
            edge[side, e] = zero_tile

    def put_edge(side, e, odd_row, even_row):
        v = jnp.where(even_slots, even_row, odd_row)
        for z in range(slices):
            for i in range(per):
                if i + 1 < per:
                    right = v[z, i + 1]
                else:
                    right = jnp.where(strip == STRIPS - 1, 0.0, pltpu.roll(v[z, 0], STRIPS - 1, 0))
                if i > 0:
                    left = v[z, i - 1]
                else:
                    left = jnp.where(strip == 0, 0.0, pltpu.roll(v[z, per - 1], 1, 0))
                edge[side, e, z, i] = jnp.where(right_slots, right, left).astype(BF)

    def put_pairs(side, pair, count, y):
        before = main[side, 2 * pair].astype(F32)
        for t in range(count):
            row = 2 * (pair + t)
            outside = (at_start & (row < halo)) | (at_end & (row >= rows - halo))
            v = jnp.maximum(y(t), 0.0) * jnp.where(outside, 0.0, 1.0)
            even_row = v[:, :LANES].reshape(slices, per, STRIPS, LANES)
            odd_row = v[:, LANES:].reshape(slices, per, STRIPS, LANES)
            main[side, row + 1] = even_row.astype(BF)
            main[side, row + 2] = odd_row.astype(BF)
            put_edge(side, pair + t, before, even_row)
            before = odd_row

    def first_step(c, carry):
        parts = []
        for z in range(slices):
            at = pl.ds(pl.multiple_of(z * stored + 8 * c, 8), 16)
            parts.append(jnp.concatenate([xs[at, k * groups:(k + 1) * groups] for k in range(6)], axis=0).astype(BF))
        x = jnp.concatenate(parts, axis=1)
        y = lax.dot_general(x, w1[...], (((0,), (0,)), ((), ())), preferred_element_type=F32)
        put_pairs(0, 4 * c, 4, lambda t: y[:, t * 2 * LANES:(t + 1) * 2 * LANES])
        return carry

    lax.fori_loop(0, rows // 8, first_step, 0)

    def window(side, pair, out_rows):
        parts = [main[side, 2 * pair + a].reshape(span, LANES) for a in range(out_rows + 2)]
        parts += [edge[side, pair + e].reshape(span, LANES) for e in range(out_rows // 2 + 1)]
        return jnp.concatenate(parts, axis=1)

    pairs = rows // 2 - 2
    for layer in range(layers):
        source, target = layer % 2, (layer + 1) % 2

        def hidden_step(c, carry):
            pair = 1 + c * chunk
            x = jnp.concatenate([window(source, pair + t, 2) for t in range(chunk)], axis=0)
            y = jnp.dot(x, wh[layer], preferred_element_type=F32)
            put_pairs(target, pair, chunk, lambda t: y[t * span:(t + 1) * span])
            return carry

        lax.fori_loop(0, pairs // chunk, hidden_step, 0)
        end = rows // 2 - 1
        put_edge(target, end, main[target, 2 * end].astype(F32), jnp.zeros((slices, per, STRIPS, LANES), F32))

    eighths = local // 8
    quad = (lane_iota(span) // 8) % 4

    def last_step(q, carry):
        x = window(layers % 2, halo // 2 + 4 * q, 8)
        y = jnp.dot(x, wl[...], preferred_element_type=F32)
        gathered_out[q // 4] = jnp.where(quad == q % 4, y, gathered_out[q // 4])
        return carry

    gathered_out[...] = jnp.zeros_like(gathered_out)
    lax.fori_loop(0, eighths, last_step, 0)

    for big in range(gathered_out.shape[0]):
        height = min(32, local - 32 * big)
        turned = [gathered_out[big, z * groups:(z + 1) * groups, :].T for z in range(slices)]
        lines = [jnp.concatenate([turned[z][k * 32:(k + 1) * 32] for k in range(4)], axis=1) for z in range(slices)]
        values = jnp.concatenate(lines, axis=0)
        high = values.astype(BF)
        low = (values - high.astype(F32)).astype(BF)
        net = jnp.dot(high, back[...], preferred_element_type=F32) + jnp.dot(low, back[...], preferred_element_type=F32)
        for z in range(slices):
            at = pl.ds(32 * big, height)
            out_ref[z, at, :] = cur_ref[z, at, :] - 2.0 * net[z * 32:z * 32 + height]

def axial_reflect(edges, current, cf, ch, cl, halo):
    slices, local, columns = current.shape
    rows = local + 2 * halo
    groups = columns // 4
    per = groups // STRIPS
    stored = rows + 8
    whole = pl.BlockSpec(memory_space=pltpu.VMEM)
    return pl.pallas_call(
        functools.partial(axial_kernel, (halo, 2)),
        out_shape=jax.ShapeDtypeStruct(current.shape, F32),
        in_specs=[whole] * 5,
        out_specs=whole,
        scratch_shapes=[
            pltpu.VMEM((2, rows + 2, slices, per, STRIPS, LANES), BF),
            pltpu.VMEM((2, rows // 2 + 1, slices, per, STRIPS, LANES), BF),
            pltpu.VMEM((96, 8 * LANES), BF),
            pltpu.VMEM((ch.shape[1], 6 * LANES, 2 * LANES), BF),
            pltpu.VMEM((15 * LANES, LANES), BF),
            pltpu.VMEM((slices * stored, columns), F32),
            pltpu.VMEM((slices * stored, 6 * groups), F32),
            pltpu.VMEM((columns, 6 * groups), BF),
            pltpu.VMEM((4 * groups, columns), BF),
            pltpu.VMEM((-(-local // 32), slices * groups, LANES), F32),
        ],
        compiler_params=pltpu.CompilerParams(vmem_limit_bytes=60 * 1024 * 1024),
        name="net_axial",
    )(edges, current, cf, ch, cl)


def fill_rows(raw, edges_ref, cur_ref, stored, halo):
    slices, local, columns = cur_ref.shape
    zero = jnp.zeros((1, columns), F32)
    tail = jnp.zeros((stored - 1 - local - 2 * halo, columns), F32)
    for z in range(slices):
        above = edges_ref[0, z * halo:(z + 1) * halo, :].astype(F32)
        below = edges_ref[1, z * halo:(z + 1) * halo, :].astype(F32)
        raw[z * stored:(z + 1) * stored, :] = jnp.concatenate([zero, above, cur_ref[z], below, tail], axis=0)


def build_first_plane(w_ref, o, w1):
    row = lax.broadcasted_iota(jnp.int32, (16, LANES), 0)
    for z in range(4):
        mixes = []
        for tj in range(3):
            taps = [jnp.broadcast_to(spread_lanes(w_ref[o, ti, tj:tj+1, :].astype(F32)), (16, LANES)) for ti in range(3)]
            mixes.append(slot_mix(16, taps, z, NATURAL, 32))
        for t in range(8):
            value = jnp.zeros((16, LANES), F32)
            for tj in range(3):
                value = jnp.where(row == t + tj, mixes[tj], value)
            w1[z * 16:(z + 1) * 16, t * LANES:(t + 1) * LANES] = value.astype(BF)

def build_hidden_plane(w_ref, o, layer, wh):
    wide = [[spread_lanes(w_ref[o, layer, ti, tj].astype(F32)) for ti in range(3)] for tj in range(3)]
    inner = wide[0][0].shape[0]
    for a in range(4):
        for z in range(4):
            at = a * LANES + z * inner
            for half in range(2):
                if 0 <= a - half < 3:
                    value = slot_mix(inner, wide[a - half], z, NATURAL, inner)
                else:
                    value = jnp.zeros((inner, LANES), F32)
                wh[layer, at:at + inner, half * LANES:(half + 1) * LANES] = value.astype(BF)

def build_last_plane(w_ref, o, wl):
    taps = [[column_of(w_ref[o, ti, tj:tj+1, :].astype(F32)) for ti in range(3)] for tj in range(3)]
    inner = taps[0][0].shape[0]
    row8 = lane_iota(inner) % 8
    zero = jnp.zeros((inner, LANES), F32)
    for a in range(10):
        line = []
        for ti in range(3):
            value = zero
            for tj in range(3):
                if 0 <= a - tj < 8:
                    value = jnp.where(row8 == a - tj, taps[tj][ti], value)
            line.append(value)
        for z in range(4):
            at = a * LANES + z * inner
            wl[at:at + inner, :] = slot_mix(inner, line, z, NATURAL, LANES // 4).astype(BF)


def plane_kernel(plan, x_ref, cur_ref, cf_ref, ch_ref, cl_ref, out_ref, main, w1, wh, wl, xs, gathered_out):
    o, halo, chunk, strips = plan
    slices, local, span = out_ref.shape
    rows = local + 2 * halo
    stored = rows + 8
    layers = ch_ref.shape[1]
    if halo:
        tile = lax.axis_index("tile")
        at_start = tile == 0
        at_end = tile == lax.axis_size("tile") - 1

    build_first_plane(cf_ref, o, w1)
    for layer in range(layers):
        build_hidden_plane(ch_ref, o, layer, wh)
    build_last_plane(cl_ref, o, wl)
    if halo:
        fill_rows(xs, x_ref, cur_ref, stored, halo)
    else:
        xs[...] = x_ref[...].astype(F32)
    for side in range(2):
        for r in (0, rows + 1):
            main[side, r] = jnp.zeros((span, LANES), BF)

    def put_pairs(side, pair, count, y):
        for t in range(count):
            row = 2 * (pair + t)
            v = jnp.maximum(y(t), 0.0)
            if halo:
                outside = (at_start & (row < halo)) | (at_end & (row >= rows - halo))
                v = v * jnp.where(outside, 0.0, 1.0)
            main[side, row + 1] = v[:, :LANES].astype(BF)
            main[side, row + 2] = v[:, LANES:].astype(BF)

    def ends(side):
        if strips > 1:
            step = span // strips
            main[side, 0, step:span] = main[side, rows, 0:span - step]
            main[side, rows + 1, 0:span - step] = main[side, 1, step:span]

    def first_step(c, carry):
        parts = [xs[pl.ds(pl.multiple_of(z * stored + 8 * c, 8), 16)] for z in range(slices)]
        x = jnp.concatenate(parts, axis=0).astype(BF)
        y = lax.dot_general(x, w1[...], (((0,), (0,)), ((), ())), preferred_element_type=F32)
        put_pairs(0, 4 * c, 4, lambda t: y[:, t * 2 * LANES:(t + 1) * 2 * LANES])
        return carry

    lax.fori_loop(0, rows // 8, first_step, 0)
    ends(0)

    for layer in range(layers):
        source, target = layer % 2, (layer + 1) % 2

        def hidden_step(c, carry):
            pair = c * chunk
            tiles = [main[source, 2 * pair + a] for a in range(2 * chunk + 2)]
            x = jnp.concatenate([jnp.concatenate(tiles[2 * t:2 * t + 4], axis=1) for t in range(chunk)], axis=0)
            y = jnp.dot(x, wh[layer], preferred_element_type=F32)
            put_pairs(target, pair, chunk, lambda t: y[t * span:(t + 1) * span])
            return carry

        lax.fori_loop(0, rows // 2 // chunk, hidden_step, 0)
        ends(target)

    quad = (lane_iota(span) // 8) % 4

    def last_step(q, carry):
        x = jnp.concatenate([main[layers % 2, halo + 8 * q + a] for a in range(10)], axis=1)
        y = jnp.dot(x, wl[...], preferred_element_type=F32)
        gathered_out[q // 4] = jnp.where(quad == q % 4, y, gathered_out[q // 4])
        return carry

    gathered_out[...] = jnp.zeros_like(gathered_out)
    lax.fori_loop(0, local // 8, last_step, 0)
    for big in range(gathered_out.shape[0]):
        height = min(32, local - 32 * big)
        net = gathered_out[big].T
        for z in range(slices):
            at = pl.ds(32 * big, height)
            out_ref[z, at, :] = cur_ref[z, at, :] - 2.0 * net[z * 32:z * 32 + height]

def plane_call(o, x, current, cf, ch, cl, halo, strips):
    slices, local, span = current.shape
    rows = local + 2 * halo
    whole = pl.BlockSpec(memory_space=pltpu.VMEM)
    return pl.pallas_call(
        functools.partial(plane_kernel, (o, halo, 4, strips)),
        out_shape=jax.ShapeDtypeStruct(current.shape, F32),
        in_specs=[whole] * 5, out_specs=whole,
        scratch_shapes=[
            pltpu.VMEM((2, rows + 2, span, LANES), BF),
            pltpu.VMEM((64, 8 * LANES), BF),
            pltpu.VMEM((ch.shape[1], 4 * LANES, 2 * LANES), BF),
            pltpu.VMEM((10 * LANES, LANES), BF),
            pltpu.VMEM((slices * (rows + 8), span), F32),
            pltpu.VMEM((-(-local // 32), span, LANES), F32),
        ],
        compiler_params=pltpu.CompilerParams(vmem_limit_bytes=60 * 1024 * 1024),
        name="net_sagittal" if halo else "net_coronal",
    )(x, current, cf, ch, cl)

def coronal_reflect(current, cf, ch, cl):
    slices, local, columns = current.shape
    strips = columns // local
    turned = jnp.transpose(current.reshape(slices, local, strips, local), (0, 3, 2, 1))
    t = turned.astype(BF)
    none = jnp.zeros((slices, 1, 1, local), BF)
    before = jnp.concatenate([none, t[:, -1:, :-1]], axis=2)
    after = jnp.concatenate([t[:, :1, 1:], none], axis=2)
    rest = jnp.zeros((slices, 6, strips, local), BF)
    x = jnp.concatenate([before, t, after, rest], axis=1)
    x = x.reshape(-1, columns)
    out = plane_call(2, x, turned.reshape(slices, local, columns), cf, ch, cl, 0, strips)
    return jnp.transpose(out.reshape(slices, local, strips, local), (0, 3, 2, 1)).reshape(current.shape)

def halo_kernel(halo, cur_hbm, out_ref, edge, sent, load, send, recv):
    agent = lax.axis_index("agent")
    tile = lax.axis_index("tile")
    last = lax.axis_size("tile") - 1
    slices, local, columns = cur_hbm.shape
    rows = edge.shape[2]
    active = (agent == 1) | (agent == 2)

    def copy(side, peer):
        return pltpu.make_async_remote_copy(
            src_ref=sent.at[side],
            dst_ref=out_ref.at[1 - side],
            send_sem=send.at[side],
            recv_sem=recv.at[1 - side],
            device_id=(agent, peer),
            device_id_type=MESH,
        )

    @pl.when(active)
    def _():
        barrier = pltpu.get_barrier_semaphore()

        @pl.when(tile > 0)
        def _():
            pl.semaphore_signal(barrier, inc=1, device_id=(agent, tile - 1), device_id_type=MESH)

        @pl.when(tile < last)
        def _():
            pl.semaphore_signal(barrier, inc=1, device_id=(agent, tile + 1), device_id_type=MESH)

        loads = [
            pltpu.make_async_copy(cur_hbm.at[:, pl.ds(0, rows)], edge.at[0], load.at[0]),
            pltpu.make_async_copy(cur_hbm.at[:, pl.ds(local - rows, rows)], edge.at[1], load.at[1]),
        ]
        for item in loads:
            item.start()
        for item in loads:
            item.wait()
        for side in range(2):
            first = 0 if side == 0 else rows - halo
            parts = [edge[side, z, first:first + halo, :] for z in range(slices)]
            sent[side] = jnp.concatenate(parts, axis=0).astype(BF)

        pl.semaphore_wait(barrier, jnp.where(tile > 0, 1, 0) + jnp.where(tile < last, 1, 0))

        @pl.when(tile > 0)
        def _():
            copy(0, tile - 1).start()

        @pl.when(tile < last)
        def _():
            copy(1, tile + 1).start()

        @pl.when(tile == 0)
        def _():
            out_ref[0] = jnp.zeros(out_ref.shape[1:], BF)

        @pl.when(tile == last)
        def _():
            out_ref[1] = jnp.zeros(out_ref.shape[1:], BF)

        @pl.when(tile > 0)
        def _():
            copy(1, tile - 1).wait_recv()

        @pl.when(tile < last)
        def _():
            copy(0, tile + 1).wait_recv()

        @pl.when(tile > 0)
        def _():
            copy(0, tile - 1).wait_send()

        @pl.when(tile < last)
        def _():
            copy(1, tile + 1).wait_send()


def halo_exchange(current, halo):
    slices, local, columns = current.shape
    return pl.pallas_call(
        functools.partial(halo_kernel, halo),
        out_shape=jax.ShapeDtypeStruct((2, slices * halo, columns), BF),
        in_specs=[pl.BlockSpec(memory_space=pl.ANY)],
        out_specs=pl.BlockSpec(memory_space=pltpu.VMEM),
        scratch_shapes=[
            pltpu.VMEM((2, slices, 8, columns), F32),
            pltpu.VMEM((2, slices * halo, columns), BF),
            pltpu.SemaphoreType.DMA((2,)),
            pltpu.SemaphoreType.DMA((2,)),
            pltpu.SemaphoreType.DMA((2,)),
        ],
        compiler_params=pltpu.CompilerParams(collective_id=2, has_side_effects=True),
        name="halo_exchange",
    )(current)


def swap_bits(me, d):
    peer, bit = me, 1
    while bit <= d:
        if d & bit:
            peer = peer + bit * (1 - 2 * ((me // bit) % 2))
        bit *= 2
    return peer


def block_copy(blocks_hbm, held, sems, i):
    at = pl.ds(i * CHUNK, CHUNK)
    return pltpu.make_async_copy(blocks_hbm.at[at], held.at[at], sems.at[i])


def block_step(held, picked, y, slices, transposed, u):
    row = lax.broadcasted_iota(jnp.int32, (8, LANES), 0)
    at = pl.ds(pl.multiple_of(8 * u, 8), 8)
    p = [picked[at, z * LANES:(z + 1) * LANES] for z in range(slices)]
    halves = []
    for t in range(2):
        sides = []
        for side in range(2):
            mask = row // 2 == 2 * t + side
            sides.append(jnp.concatenate([jnp.where(mask, v, 0.0) for v in p], axis=0))
        lhs = jnp.concatenate(sides, axis=1).astype(BF)
        m = [held[8 * u + 4 * t + j] for j in range(4)]
        if transposed:
            top, bottom = jnp.concatenate([m[0], m[2]], axis=1), jnp.concatenate([m[1], m[3]], axis=1)
            dims = (((1,), (1,)), ((), ()))
        else:
            top, bottom = jnp.concatenate([m[0], m[1]], axis=1), jnp.concatenate([m[2], m[3]], axis=1)
            dims = (((1,), (0,)), ((), ()))
        rhs = jnp.concatenate([top, bottom], axis=0)
        halves.append(lax.dot_general(lhs, rhs, dims, preferred_element_type=F32))
    for z in range(slices):
        a, b = (h[8 * z:8 * z + 8] for h in halves)
        low = jnp.where(row < 4, a[:, :LANES], b[:, :LANES])
        high = jnp.where(row < 4, a[:, LANES:], b[:, LANES:])
        y[at, z * LANES:(z + 1) * LANES] = jnp.where(row % 2 == 0, low, high)


def block_sweep(blocks_hbm, held, sems, picked, y, slices, transposed, waiting):
    def chunk(i, carry):
        if waiting:
            block_copy(blocks_hbm, held, sems, i).wait()
        for j in range(CHUNK // 8):
            block_step(held, picked, y, slices, transposed, i * (CHUNK // 8) + j)
        return carry

    lax.fori_loop(0, held.shape[0] // CHUNK, chunk, 0)


def gather_rows(hot, source):
    return jnp.dot(hot, source, preferred_element_type=F32)


def scatter_rows(hot, y):
    high = y.astype(BF)
    low = (y - high.astype(F32)).astype(BF)
    return jnp.dot(
        jnp.concatenate([hot, hot], axis=1), jnp.concatenate([high, low], axis=0), preferred_element_type=F32
    )


def data_kernel(
    count, angle_ref, detector_ref, tile_ref, sino_ref, cur_hbm, blocks_hbm, out_ref,
    held, cur, ray_hot, ray_turned, tile_hot, tile_turned, x, y, picked, total, part, got, fresh, full,
    load, sems, send1, recv1, send2, recv2,
):
    agent = lax.axis_index("agent")
    me = lax.axis_index("tile")
    slices, local, columns = out_ref.shape
    detectors = columns // LANES
    rays_here = fresh.shape[1]
    ray_total = count * rays_here
    tiles_here = detectors * local
    blocks_here = held.shape[0]
    order = list(range(count - 1, 0, -1))

    def part_copy(step, d):
        return pltpu.make_async_remote_copy(
            src_ref=part.at[step, swap_bits(me, d)],
            dst_ref=got.at[step, d],
            send_sem=send1.at[step, d],
            recv_sem=recv1.at[step, d],
            device_id=(agent, swap_bits(me, d)),
            device_id_type=MESH,
        )

    def rest_copy(step, d):
        return pltpu.make_async_remote_copy(
            src_ref=fresh.at[step],
            dst_ref=full.at[step, me],
            send_sem=send2.at[step, d],
            recv_sem=recv2.at[step, d],
            device_id=(agent, swap_bits(me, d)),
            device_id_type=MESH,
        )

    def exchange(step):
        for slot in range(count):
            part[step, slot] = total[slot * rays_here:(slot + 1) * rays_here, :].astype(BF)
        for d in order:
            part_copy(step, d).start()
        own = total[pl.ds(pl.multiple_of(me * rays_here, 8), rays_here), :]
        measured = [sino_ref[pl.ds(z, rays_here, stride=slices), :] for z in range(slices)]
        value = own - jnp.concatenate(measured, axis=1)
        for d in reversed(order):
            part_copy(step, d).wait_recv()
            value = value + got[step, d].astype(F32)
        fresh[step] = value.astype(BF)
        for d in order:
            rest_copy(step, d).start()
        full[step, me] = fresh[step]
        for d in order:
            rest_copy(step, d).wait_recv()
        for d in order:
            part_copy(step, d).wait_send()
            rest_copy(step, d).wait_send()
        return full[step].reshape(ray_total, slices * LANES)

    @pl.when(agent == 0)
    def _():
        barrier = pltpu.get_barrier_semaphore()
        for d in order:
            pl.semaphore_signal(barrier, inc=1, device_id=(agent, swap_bits(me, d)), device_id_type=MESH)
        first = pltpu.make_async_copy(cur_hbm, cur, load.at[0])
        first.start()
        for i in range(blocks_here // CHUNK):
            block_copy(blocks_hbm, held, sems, i).start()

        hot_rows = lax.broadcasted_iota(jnp.int32, (ray_total, blocks_here), 0)
        ray = angle_ref[...] * detectors + detector_ref[...]
        hot = jnp.where(hot_rows == jnp.broadcast_to(ray, hot_rows.shape), 1.0, 0.0)
        ray_hot[...] = hot.astype(BF)
        ray_turned[...] = hot.T.astype(BF)
        hot_rows = lax.broadcasted_iota(jnp.int32, (tiles_here, blocks_here), 0)
        place = tile_ref[...]
        place = (place % detectors) * local + place // detectors
        hot = jnp.where(hot_rows == jnp.broadcast_to(place, hot_rows.shape), 1.0, 0.0)
        tile_hot[...] = hot.astype(BF)
        tile_turned[...] = hot.T.astype(BF)

        first.wait()
        for z in range(slices):
            for t in range(detectors):
                x[t * local:(t + 1) * local, z * LANES:(z + 1) * LANES] = cur[z, :, t * LANES:(t + 1) * LANES]

        for step in range(DATA_STEPS):
            picked[...] = gather_rows(tile_turned[...], x[...].astype(BF))
            block_sweep(blocks_hbm, held, sems, picked, y, slices, True, step == 0)
            total[...] = scatter_rows(ray_hot[...], y[...])
            if step == 0:
                pl.semaphore_wait(barrier, count - 1)
            picked[...] = gather_rows(ray_turned[...], exchange(step))
            block_sweep(blocks_hbm, held, sems, picked, y, slices, False, False)
            x[...] = x[...] - 0.8 * scatter_rows(tile_hot[...], y[...])

        for z in range(slices):
            for t in range(detectors):
                moved = x[t * local:(t + 1) * local, z * LANES:(z + 1) * LANES]
                at = slice(t * LANES, (t + 1) * LANES)
                out_ref[z, :, at] = 2.0 * moved - cur[z, :, at]


def data_reflect(angle, detector, tile, sinogram, current, blocks, count):
    slices, local, columns = current.shape
    rays_here = sinogram.shape[0]
    ray_total = rays_here * count
    tiles_here = columns // LANES * local
    blocks_here = blocks.shape[0]
    width = slices * LANES
    vmem = pl.BlockSpec(memory_space=pltpu.VMEM)
    anywhere = pl.BlockSpec(memory_space=pl.ANY)
    return pl.pallas_call(
        functools.partial(data_kernel, count),
        out_shape=jax.ShapeDtypeStruct(current.shape, F32),
        in_specs=[vmem] * 4 + [anywhere] * 2,
        out_specs=vmem,
        scratch_shapes=[
            pltpu.VMEM(blocks.shape, BF),
            pltpu.VMEM(current.shape, F32),
            pltpu.VMEM((ray_total, blocks_here), BF),
            pltpu.VMEM((blocks_here, ray_total), BF),
            pltpu.VMEM((tiles_here, blocks_here), BF),
            pltpu.VMEM((blocks_here, tiles_here), BF),
            pltpu.VMEM((tiles_here, width), F32),
            pltpu.VMEM((blocks_here, width), F32),
            pltpu.VMEM((blocks_here, width), F32),
            pltpu.VMEM((ray_total, width), F32),
            pltpu.VMEM((DATA_STEPS, count, rays_here, width), BF),
            pltpu.VMEM((DATA_STEPS, count, rays_here, width), BF),
            pltpu.VMEM((DATA_STEPS, rays_here, width), BF),
            pltpu.VMEM((DATA_STEPS, count, rays_here, width), BF),
            pltpu.SemaphoreType.DMA((1,)),
            pltpu.SemaphoreType.DMA((blocks_here // CHUNK,)),
            pltpu.SemaphoreType.DMA((DATA_STEPS, count)),
            pltpu.SemaphoreType.DMA((DATA_STEPS, count)),
            pltpu.SemaphoreType.DMA((DATA_STEPS, count)),
            pltpu.SemaphoreType.DMA((DATA_STEPS, count)),
        ],
        compiler_params=pltpu.CompilerParams(
            collective_id=0, has_side_effects=True, vmem_limit_bytes=62 * 1024 * 1024
        ),
        name="data_agent",
    )(
        angle.reshape(1, -1), detector.reshape(1, -1), tile.reshape(1, -1),
        sinogram.reshape(rays_here * slices, LANES), current, blocks,
    )


def agent_kernel(own_ref, cur_hbm, out_ref, cur, own, near, pair, far, load, s1, r1, s2, r2, s3, r3, s4, r4):
    me = lax.axis_index("agent")
    tile = lax.axis_index("tile")
    core = me % 2
    other = 1 - core
    partner = me + 1 - 2 * core
    across = (me + 2) % 4
    chunks = pair.shape[0]
    barrier = pltpu.get_barrier_semaphore()
    for peer in (partner, across):
        pl.semaphore_signal(barrier, inc=1, device_id=(peer, tile), device_id_type=MESH)
    state = pltpu.make_async_copy(cur_hbm, cur, load.at[0])
    state.start()
    own[...] = own_ref[...].astype(BF)
    pl.semaphore_wait(barrier, 2)

    def send(source, target, s, r, to):
        return pltpu.make_async_remote_copy(
            src_ref=source, dst_ref=target, send_sem=s, recv_sem=r, device_id=(to, tile), device_id_type=MESH
        )

    def first(k, half):
        return send(own.at[half, k], near.at[half, k], s1.at[k], r1.at[k], partner)

    def rest(half):
        return send(own.at[half], near.at[half], s2.at[0], r2.at[0], partner)

    def cross(k):
        return send(pair.at[k], far.at[core, k], s3.at[k], r3.at[k], across)

    def onward(k, half):
        return send(far.at[half, k], far.at[half, k], s4.at[k], r4.at[k], partner)

    def result(half, k):
        others = near[half, k].astype(F32) + far[half, k].astype(F32)
        out_ref[half, k] = 2.0 * cur[half, k] + others - own_ref[half, k]

    for k in range(chunks):
        first(k, other).start()
    rest(core).start()
    for k in range(chunks):
        first(k, core).wait_recv()
        pair[k] = (own[core, k].astype(F32) + near[core, k].astype(F32)).astype(BF)
        cross(k).start()
    state.wait()
    for k in range(chunks):
        cross(k).wait_recv()
        onward(k, core).start()
        result(core, k)
    rest(other).wait_recv()
    for k in range(chunks):
        onward(k, other).wait_recv()
        result(other, k)
    for k in range(chunks):
        first(k, other).wait_send()
        cross(k).wait_send()
        onward(k, core).wait_send()
    rest(core).wait_send()


def agent_sum(reflect, current):
    slices, local, columns = reflect.shape
    half = slices * local // 2
    chunks = max(1, half // 32)
    shape = (2, chunks, half // chunks, columns)
    whole = pl.BlockSpec(memory_space=pltpu.VMEM)
    out = pl.pallas_call(
        agent_kernel,
        out_shape=jax.ShapeDtypeStruct(shape, F32),
        in_specs=[whole, pl.BlockSpec(memory_space=pl.ANY)],
        out_specs=whole,
        scratch_shapes=[
            pltpu.VMEM(shape, F32),
            pltpu.VMEM(shape, BF),
            pltpu.VMEM(shape, BF),
            pltpu.VMEM(shape[1:], BF),
            pltpu.VMEM(shape, BF),
            pltpu.SemaphoreType.DMA((1,)),
            pltpu.SemaphoreType.DMA((chunks,)),
            pltpu.SemaphoreType.DMA((chunks,)),
            pltpu.SemaphoreType.DMA((1,)),
            pltpu.SemaphoreType.DMA((1,)),
            pltpu.SemaphoreType.DMA((chunks,)),
            pltpu.SemaphoreType.DMA((chunks,)),
            pltpu.SemaphoreType.DMA((chunks,)),
            pltpu.SemaphoreType.DMA((chunks,)),
        ],
        compiler_params=pltpu.CompilerParams(collective_id=1, has_side_effects=True),
        name="agent_sum",
    )(reflect.reshape(shape), current.reshape(shape))
    return out.reshape(reflect.shape)


def per_device(
    states,
    sinogram,
    blocks,
    block_angle,
    block_detector,
    block_tile,
    conv_first,
    conv_hidden,
    conv_last,
):
    current = states[0]
    agent_place = lax.axis_index("agent")
    halo = conv_hidden.shape[1] + 2
    filters = (conv_first, conv_hidden, conv_last)
    edges = halo_exchange(current, halo)
    data = data_reflect(
        block_angle, block_detector, block_tile, sinogram, current, blocks, lax.axis_size("tile")
    )

    def data_only():
        return data

    def axial_only():
        return axial_reflect(edges, current, *filters, halo)

    def sagittal_only():
        return plane_call(1, edges, current, *filters, halo, 1)

    def coronal_only():
        return coronal_reflect(current, *filters)

    reflect = lax.switch(agent_place, [data_only, axial_only, sagittal_only, coronal_only])
    return (0.25 * agent_sum(reflect, current))[None]


def solution(mesh):
    placed = (
        P("agent", None, "tile", None),
        P("tile", None, None),
        P("tile", None, None),
        P("tile"),
        P("tile"),
        P("tile"),
        P(),
        P(),
        P(),
    )
    return jax.shard_map(
        per_device,
        mesh=mesh,
        in_specs=placed,
        out_specs=P("agent", None, "tile", None),
        check_vma=False,
    )
```

```python
import functools

import jax
import jax.numpy as jnp
from jax import lax
from jax.experimental import pallas as pl
from jax.experimental.pallas import tpu as pltpu
from jax.sharding import PartitionSpec as P

DATA_STEPS = 2
MESH = pl.DeviceIdType.MESH
LANES = 128
STRIPS = 16
CHUNK = 32
BF = jnp.bfloat16
F32 = jnp.float32
NATURAL = (0, 1, 2, 3)
EVEN_ORDER = (0, 1, 2, 3)
ODD_ORDER = (1, 0, 3, 2)


def main_cells(offset):
    order = EVEN_ORDER if offset % 2 else ODD_ORDER
    return [(offset, column) for column in order]

def edge_cells(offset):
    return [(offset + 1, 4), (offset, 4), (offset, -1), (offset + 1, -1)]

def window_cells(rows):
    tiles = [main_cells(a) for a in range(rows + 2)]
    return tiles + [edge_cells(a) for a in range(0, rows + 2, 2)]

def spread_lanes(w):
    return jnp.concatenate([w] * (LANES // w.shape[-1]), axis=-1)

def lane_iota(rows):
    return lax.broadcasted_iota(jnp.int32, (rows, LANES), 1)

def slot_mix(rows, taps, column_in, order, width):
    slot = lane_iota(rows) // width
    mixed = jnp.zeros((rows, LANES), F32)
    for place, column in enumerate(order):
        tap = column_in - column + 1
        if 0 <= tap < 3:
            mixed = jnp.where(slot == place, taps[tap], mixed)
    return mixed

def build_first(w_ref, o, w1):
    for k in range(6):
        for half in range(2):
            order = ODD_ORDER if half else EVEN_ORDER
            mixes = []
            for ti in range(3):
                taps = [jnp.broadcast_to(spread_lanes(w_ref[o, ti, tj:tj+1, :].astype(F32)), (16, LANES)) for tj in range(3)]
                mixes.append(slot_mix(16, taps, k - 1, order, 32))
            row = lax.broadcasted_iota(jnp.int32, (16, LANES), 0)
            for t in range(4):
                value = jnp.zeros((16, LANES), F32)
                for ti in range(3):
                    value = jnp.where(row == 2 * t + half + ti, mixes[ti], value)
                at = t * 2 * LANES + half * LANES
                w1[k * 16:(k + 1) * 16, at:at + LANES] = value.astype(BF)

def build_hidden(w_ref, o, layer, wh):
    wide = [[spread_lanes(w_ref[o, layer, ti, tj].astype(F32)) for tj in range(3)] for ti in range(3)]
    inner = wide[0][0].shape[0]
    for n, tile in enumerate(window_cells(2)):
        for slot, (a, column) in enumerate(tile):
            at = n * LANES + slot * inner
            for half in range(2):
                ti = a - (half + 1) + 1
                if 0 <= ti < 3:
                    value = slot_mix(inner, wide[ti], column, ODD_ORDER if half else EVEN_ORDER, inner)
                else:
                    value = jnp.zeros((inner, LANES), F32)
                wh[layer, at:at + inner, half * LANES:(half + 1) * LANES] = value.astype(BF)

def column_of(row):
    inner = row.shape[1]
    r = lax.broadcasted_iota(jnp.int32, (inner, inner), 0)
    c = lax.broadcasted_iota(jnp.int32, (inner, inner), 1)
    picked = jnp.where(r == c, jnp.broadcast_to(row, (inner, inner)), 0.0)
    return jnp.broadcast_to(jnp.sum(picked, axis=1, keepdims=True), (inner, LANES))

def build_last(w_ref, o, wl):
    taps = [[column_of(w_ref[o, ti, tj:tj+1, :].astype(F32)) for tj in range(3)] for ti in range(3)]
    inner = taps[0][0].shape[0]
    lane = lane_iota(inner)
    row8 = lane % 8
    zero = jnp.zeros((inner, LANES), F32)
    rows = []
    for a in range(10):
        line = []
        for tj in range(3):
            value = zero
            for ti in range(3):
                if 0 <= a - ti < 8:
                    value = jnp.where(row8 == a - ti, taps[ti][tj], value)
            line.append(value)
        rows.append(line)
    for n, tile in enumerate(window_cells(8)):
        for slot, (a, column) in enumerate(tile):
            at = n * LANES + slot * inner
            wl[at:at + inner, :] = slot_mix(inner, rows[a], column, EVEN_ORDER, LANES // 4).astype(BF)


def axial_kernel(plan, edges_ref, cur_ref, cf_ref, ch_ref, cl_ref, out_ref, main, edge, w1, wh, wl, raw, xs, place, back, gathered_out):
    halo, chunk = plan
    slices, local, columns = cur_ref.shape
    rows = local + 2 * halo
    stored = rows + 8
    groups = columns // 4
    per = groups // STRIPS
    span = slices * groups
    layers = ch_ref.shape[1]
    tile = lax.axis_index("tile")
    at_start = tile == 0
    at_end = tile == lax.axis_size("tile") - 1
    fill_rows(raw, edges_ref, cur_ref, stored, halo)

    build_first(cf_ref, 0, w1)
    for layer in range(layers):
        build_hidden(ch_ref, 0, layer, wh)
    build_last(cl_ref, 0, wl)

    col = lax.broadcasted_iota(jnp.int32, (columns, groups), 0)
    m = lax.broadcasted_iota(jnp.int32, (columns, groups), 1)
    first_col = 4 * ((m % STRIPS) * per + m // STRIPS)
    for k in range(6):
        place[:, k * groups:(k + 1) * groups] = jnp.where(col == first_col + (k - 1), 1.0, 0.0).astype(BF)
    m = lax.broadcasted_iota(jnp.int32, (groups, columns), 0)
    col = lax.broadcasted_iota(jnp.int32, (groups, columns), 1)
    first_col = 4 * ((m % STRIPS) * per + m // STRIPS)
    for k in range(4):
        back[k * groups:(k + 1) * groups, :] = jnp.where(col == first_col + k, 1.0, 0.0).astype(BF)
    xs[...] = jnp.dot(raw[...].astype(BF), place[...], preferred_element_type=F32)

    slot = lane_iota(STRIPS) // (LANES // 4)
    even_slots = (slot == 0) | (slot == 3)
    right_slots = slot < 2
    strip = lax.broadcasted_iota(jnp.int32, (STRIPS, LANES), 0)
    zero_tile = jnp.zeros((slices, per, STRIPS, LANES), BF)

    for side in range(2):
        for r in (0, 1, 2, rows - 1, rows, rows + 1):
            main[side, r] = zero_tile
        for e in (0, 1, rows // 2 - 1, rows // 2):
            edge[side, e] = zero_tile

    def put_edge(side, e, odd_row, even_row):
        v = jnp.where(even_slots, even_row, odd_row)
        for z in range(slices):
            for i in range(per):
                if i + 1 < per:
                    right = v[z, i + 1]
                else:
                    right = jnp.where(strip == STRIPS - 1, 0.0, pltpu.roll(v[z, 0], STRIPS - 1, 0))
                if i > 0:
                    left = v[z, i - 1]
                else:
                    left = jnp.where(strip == 0, 0.0, pltpu.roll(v[z, per - 1], 1, 0))
                edge[side, e, z, i] = jnp.where(right_slots, right, left).astype(BF)

    def put_pairs(side, pair, count, y):
        before = main[side, 2 * pair].astype(F32)
        for t in range(count):
            row = 2 * (pair + t)
            outside = (at_start & (row < halo)) | (at_end & (row >= rows - halo))
            v = jnp.maximum(y(t), 0.0) * jnp.where(outside, 0.0, 1.0)
            even_row = v[:, :LANES].reshape(slices, per, STRIPS, LANES)
            odd_row = v[:, LANES:].reshape(slices, per, STRIPS, LANES)
            main[side, row + 1] = even_row.astype(BF)
            main[side, row + 2] = odd_row.astype(BF)
            put_edge(side, pair + t, before, even_row)
            before = odd_row

    def first_step(c, carry):
        parts = []
        for z in range(slices):
            at = pl.ds(pl.multiple_of(z * stored + 8 * c, 8), 16)
            parts.append(jnp.concatenate([xs[at, k * groups:(k + 1) * groups] for k in range(6)], axis=0).astype(BF))
        x = jnp.concatenate(parts, axis=1)
        y = lax.dot_general(x, w1[...], (((0,), (0,)), ((), ())), preferred_element_type=F32)
        put_pairs(0, 4 * c, 4, lambda t: y[:, t * 2 * LANES:(t + 1) * 2 * LANES])
        return carry

    lax.fori_loop(0, rows // 8, first_step, 0)

    def window(side, pair, out_rows):
        parts = [main[side, 2 * pair + a].reshape(span, LANES) for a in range(out_rows + 2)]
        parts += [edge[side, pair + e].reshape(span, LANES) for e in range(out_rows // 2 + 1)]
        return jnp.concatenate(parts, axis=1)

    pairs = rows // 2 - 2
    for layer in range(layers):
        source, target = layer % 2, (layer + 1) % 2

        def hidden_step(c, carry):
            pair = 1 + c * chunk
            x = jnp.concatenate([window(source, pair + t, 2) for t in range(chunk)], axis=0)
            y = jnp.dot(x, wh[layer], preferred_element_type=F32)
            put_pairs(target, pair, chunk, lambda t: y[t * span:(t + 1) * span])
            return carry

        lax.fori_loop(0, pairs // chunk, hidden_step, 0)
        end = rows // 2 - 1
        put_edge(target, end, main[target, 2 * end].astype(F32), jnp.zeros((slices, per, STRIPS, LANES), F32))

    eighths = local // 8
    quad = (lane_iota(span) // 8) % 4

    def last_step(q, carry):
        x = window(layers % 2, halo // 2 + 4 * q, 8)
        y = jnp.dot(x, wl[...], preferred_element_type=F32)
        gathered_out[q // 4] = jnp.where(quad == q % 4, y, gathered_out[q // 4])
        return carry

    gathered_out[...] = jnp.zeros_like(gathered_out)
    lax.fori_loop(0, eighths, last_step, 0)

    for big in range(gathered_out.shape[0]):
        height = min(32, local - 32 * big)
        turned = [gathered_out[big, z * groups:(z + 1) * groups, :].T for z in range(slices)]
        lines = [jnp.concatenate([turned[z][k * 32:(k + 1) * 32] for k in range(4)], axis=1) for z in range(slices)]
        values = jnp.concatenate(lines, axis=0)
        high = values.astype(BF)
        low = (values - high.astype(F32)).astype(BF)
        net = jnp.dot(high, back[...], preferred_element_type=F32) + jnp.dot(low, back[...], preferred_element_type=F32)
        for z in range(slices):
            at = pl.ds(32 * big, height)
            out_ref[z, at, :] = cur_ref[z, at, :] - 2.0 * net[z * 32:z * 32 + height]

def axial_reflect(edges, current, cf, ch, cl, halo):
    slices, local, columns = current.shape
    rows = local + 2 * halo
    groups = columns // 4
    per = groups // STRIPS
    stored = rows + 8
    whole = pl.BlockSpec(memory_space=pltpu.VMEM)
    return pl.pallas_call(
        functools.partial(axial_kernel, (halo, 2)),
        out_shape=jax.ShapeDtypeStruct(current.shape, F32),
        in_specs=[whole] * 5,
        out_specs=whole,
        scratch_shapes=[
            pltpu.VMEM((2, rows + 2, slices, per, STRIPS, LANES), BF),
            pltpu.VMEM((2, rows // 2 + 1, slices, per, STRIPS, LANES), BF),
            pltpu.VMEM((96, 8 * LANES), BF),
            pltpu.VMEM((ch.shape[1], 6 * LANES, 2 * LANES), BF),
            pltpu.VMEM((15 * LANES, LANES), BF),
            pltpu.VMEM((slices * stored, columns), F32),
            pltpu.VMEM((slices * stored, 6 * groups), F32),
            pltpu.VMEM((columns, 6 * groups), BF),
            pltpu.VMEM((4 * groups, columns), BF),
            pltpu.VMEM((-(-local // 32), slices * groups, LANES), F32),
        ],
        compiler_params=pltpu.CompilerParams(vmem_limit_bytes=60 * 1024 * 1024),
        name="net_axial",
    )(edges, current, cf, ch, cl)


def fill_rows(raw, edges_ref, cur_ref, stored, halo):
    slices, local, columns = cur_ref.shape
    zero = jnp.zeros((1, columns), F32)
    tail = jnp.zeros((stored - 1 - local - 2 * halo, columns), F32)
    for z in range(slices):
        above = edges_ref[0, z * halo:(z + 1) * halo, :].astype(F32)
        below = edges_ref[1, z * halo:(z + 1) * halo, :].astype(F32)
        raw[z * stored:(z + 1) * stored, :] = jnp.concatenate([zero, above, cur_ref[z], below, tail], axis=0)


def build_first_plane(w_ref, o, w1):
    row = lax.broadcasted_iota(jnp.int32, (16, LANES), 0)
    for z in range(4):
        mixes = []
        for tj in range(3):
            taps = [jnp.broadcast_to(spread_lanes(w_ref[o, ti, tj:tj+1, :].astype(F32)), (16, LANES)) for ti in range(3)]
            mixes.append(slot_mix(16, taps, z, NATURAL, 32))
        for t in range(8):
            value = jnp.zeros((16, LANES), F32)
            for tj in range(3):
                value = jnp.where(row == t + tj, mixes[tj], value)
            w1[z * 16:(z + 1) * 16, t * LANES:(t + 1) * LANES] = value.astype(BF)

def build_hidden_plane(w_ref, o, layer, wh):
    wide = [[spread_lanes(w_ref[o, layer, ti, tj].astype(F32)) for ti in range(3)] for tj in range(3)]
    inner = wide[0][0].shape[0]
    for a in range(4):
        for z in range(4):
            at = a * LANES + z * inner
            for half in range(2):
                if 0 <= a - half < 3:
                    value = slot_mix(inner, wide[a - half], z, NATURAL, inner)
                else:
                    value = jnp.zeros((inner, LANES), F32)
                wh[layer, at:at + inner, half * LANES:(half + 1) * LANES] = value.astype(BF)

def build_last_plane(w_ref, o, wl):
    taps = [[column_of(w_ref[o, ti, tj:tj+1, :].astype(F32)) for ti in range(3)] for tj in range(3)]
    inner = taps[0][0].shape[0]
    row8 = lane_iota(inner) % 8
    zero = jnp.zeros((inner, LANES), F32)
    for a in range(10):
        line = []
        for ti in range(3):
            value = zero
            for tj in range(3):
                if 0 <= a - tj < 8:
                    value = jnp.where(row8 == a - tj, taps[tj][ti], value)
            line.append(value)
        for z in range(4):
            at = a * LANES + z * inner
            wl[at:at + inner, :] = slot_mix(inner, line, z, NATURAL, LANES // 4).astype(BF)


def plane_kernel(plan, x_ref, cur_ref, cf_ref, ch_ref, cl_ref, out_ref, main, w1, wh, wl, xs, gathered_out):
    o, halo, chunk, strips = plan
    slices, local, span = out_ref.shape
    rows = local + 2 * halo
    stored = rows + 8
    layers = ch_ref.shape[1]
    if halo:
        tile = lax.axis_index("tile")
        at_start = tile == 0
        at_end = tile == lax.axis_size("tile") - 1

    build_first_plane(cf_ref, o, w1)
    for layer in range(layers):
        build_hidden_plane(ch_ref, o, layer, wh)
    build_last_plane(cl_ref, o, wl)
    if halo:
        fill_rows(xs, x_ref, cur_ref, stored, halo)
    else:
        xs[...] = x_ref[...].astype(F32)
    for side in range(2):
        for r in (0, rows + 1):
            main[side, r] = jnp.zeros((span, LANES), BF)

    def put_pairs(side, pair, count, y):
        for t in range(count):
            row = 2 * (pair + t)
            v = jnp.maximum(y(t), 0.0)
            if halo:
                outside = (at_start & (row < halo)) | (at_end & (row >= rows - halo))
                v = v * jnp.where(outside, 0.0, 1.0)
            main[side, row + 1] = v[:, :LANES].astype(BF)
            main[side, row + 2] = v[:, LANES:].astype(BF)

    def ends(side):
        if strips > 1:
            step = span // strips
            main[side, 0, step:span] = main[side, rows, 0:span - step]
            main[side, rows + 1, 0:span - step] = main[side, 1, step:span]

    def first_step(c, carry):
        parts = [xs[pl.ds(pl.multiple_of(z * stored + 8 * c, 8), 16)] for z in range(slices)]
        x = jnp.concatenate(parts, axis=0).astype(BF)
        y = lax.dot_general(x, w1[...], (((0,), (0,)), ((), ())), preferred_element_type=F32)
        put_pairs(0, 4 * c, 4, lambda t: y[:, t * 2 * LANES:(t + 1) * 2 * LANES])
        return carry

    lax.fori_loop(0, rows // 8, first_step, 0)
    ends(0)

    for layer in range(layers):
        source, target = layer % 2, (layer + 1) % 2

        def hidden_step(c, carry):
            pair = c * chunk
            tiles = [main[source, 2 * pair + a] for a in range(2 * chunk + 2)]
            x = jnp.concatenate([jnp.concatenate(tiles[2 * t:2 * t + 4], axis=1) for t in range(chunk)], axis=0)
            y = jnp.dot(x, wh[layer], preferred_element_type=F32)
            put_pairs(target, pair, chunk, lambda t: y[t * span:(t + 1) * span])
            return carry

        lax.fori_loop(0, rows // 2 // chunk, hidden_step, 0)
        ends(target)

    quad = (lane_iota(span) // 8) % 4

    def last_step(q, carry):
        x = jnp.concatenate([main[layers % 2, halo + 8 * q + a] for a in range(10)], axis=1)
        y = jnp.dot(x, wl[...], preferred_element_type=F32)
        gathered_out[q // 4] = jnp.where(quad == q % 4, y, gathered_out[q // 4])
        return carry

    gathered_out[...] = jnp.zeros_like(gathered_out)
    lax.fori_loop(0, local // 8, last_step, 0)
    for big in range(gathered_out.shape[0]):
        height = min(32, local - 32 * big)
        net = gathered_out[big].T
        for z in range(slices):
            at = pl.ds(32 * big, height)
            out_ref[z, at, :] = cur_ref[z, at, :] - 2.0 * net[z * 32:z * 32 + height]

def plane_call(o, x, current, cf, ch, cl, halo, strips):
    slices, local, span = current.shape
    rows = local + 2 * halo
    whole = pl.BlockSpec(memory_space=pltpu.VMEM)
    return pl.pallas_call(
        functools.partial(plane_kernel, (o, halo, 4, strips)),
        out_shape=jax.ShapeDtypeStruct(current.shape, F32),
        in_specs=[whole] * 5, out_specs=whole,
        scratch_shapes=[
            pltpu.VMEM((2, rows + 2, span, LANES), BF),
            pltpu.VMEM((64, 8 * LANES), BF),
            pltpu.VMEM((ch.shape[1], 4 * LANES, 2 * LANES), BF),
            pltpu.VMEM((10 * LANES, LANES), BF),
            pltpu.VMEM((slices * (rows + 8), span), F32),
            pltpu.VMEM((-(-local // 32), span, LANES), F32),
        ],
        compiler_params=pltpu.CompilerParams(vmem_limit_bytes=60 * 1024 * 1024),
        name="net_sagittal" if halo else "net_coronal",
    )(x, current, cf, ch, cl)

def coronal_reflect(current, cf, ch, cl):
    slices, local, columns = current.shape
    strips = columns // local
    turned = jnp.transpose(current.reshape(slices, local, strips, local), (0, 3, 2, 1))
    t = turned.astype(BF)
    none = jnp.zeros((slices, 1, 1, local), BF)
    before = jnp.concatenate([none, t[:, -1:, :-1]], axis=2)
    after = jnp.concatenate([t[:, :1, 1:], none], axis=2)
    rest = jnp.zeros((slices, 6, strips, local), BF)
    x = jnp.concatenate([before, t, after, rest], axis=1)
    x = x.reshape(-1, columns)
    out = plane_call(2, x, turned.reshape(slices, local, columns), cf, ch, cl, 0, strips)
    return jnp.transpose(out.reshape(slices, local, strips, local), (0, 3, 2, 1)).reshape(current.shape)

def halo_kernel(halo, cur_hbm, out_ref, edge, sent, load, send, recv):
    agent = lax.axis_index("agent")
    tile = lax.axis_index("tile")
    last = lax.axis_size("tile") - 1
    slices, local, columns = cur_hbm.shape
    rows = edge.shape[2]
    active = (agent == 1) | (agent == 2)

    def copy(side, peer):
        return pltpu.make_async_remote_copy(
            src_ref=sent.at[side],
            dst_ref=out_ref.at[1 - side],
            send_sem=send.at[side],
            recv_sem=recv.at[1 - side],
            device_id=(agent, peer),
            device_id_type=MESH,
        )

    @pl.when(active)
    def _():
        barrier = pltpu.get_barrier_semaphore()

        @pl.when(tile > 0)
        def _():
            pl.semaphore_signal(barrier, inc=1, device_id=(agent, tile - 1), device_id_type=MESH)

        @pl.when(tile < last)
        def _():
            pl.semaphore_signal(barrier, inc=1, device_id=(agent, tile + 1), device_id_type=MESH)

        loads = [
            pltpu.make_async_copy(cur_hbm.at[:, pl.ds(0, rows)], edge.at[0], load.at[0]),
            pltpu.make_async_copy(cur_hbm.at[:, pl.ds(local - rows, rows)], edge.at[1], load.at[1]),
        ]
        for item in loads:
            item.start()
        for item in loads:
            item.wait()
        for side in range(2):
            first = 0 if side == 0 else rows - halo
            parts = [edge[side, z, first:first + halo, :] for z in range(slices)]
            sent[side] = jnp.concatenate(parts, axis=0).astype(BF)

        pl.semaphore_wait(barrier, jnp.where(tile > 0, 1, 0) + jnp.where(tile < last, 1, 0))

        @pl.when(tile > 0)
        def _():
            copy(0, tile - 1).start()

        @pl.when(tile < last)
        def _():
            copy(1, tile + 1).start()

        @pl.when(tile == 0)
        def _():
            out_ref[0] = jnp.zeros(out_ref.shape[1:], BF)

        @pl.when(tile == last)
        def _():
            out_ref[1] = jnp.zeros(out_ref.shape[1:], BF)

        @pl.when(tile > 0)
        def _():
            copy(1, tile - 1).wait_recv()

        @pl.when(tile < last)
        def _():
            copy(0, tile + 1).wait_recv()

        @pl.when(tile > 0)
        def _():
            copy(0, tile - 1).wait_send()

        @pl.when(tile < last)
        def _():
            copy(1, tile + 1).wait_send()


def halo_exchange(current, halo):
    slices, local, columns = current.shape
    return pl.pallas_call(
        functools.partial(halo_kernel, halo),
        out_shape=jax.ShapeDtypeStruct((2, slices * halo, columns), BF),
        in_specs=[pl.BlockSpec(memory_space=pl.ANY)],
        out_specs=pl.BlockSpec(memory_space=pltpu.VMEM),
        scratch_shapes=[
            pltpu.VMEM((2, slices, 8, columns), F32),
            pltpu.VMEM((2, slices * halo, columns), BF),
            pltpu.SemaphoreType.DMA((2,)),
            pltpu.SemaphoreType.DMA((2,)),
            pltpu.SemaphoreType.DMA((2,)),
        ],
        compiler_params=pltpu.CompilerParams(collective_id=2, has_side_effects=True),
        name="halo_exchange",
    )(current)


def swap_bits(me, d):
    peer, bit = me, 1
    while bit <= d:
        if d & bit:
            peer = peer + bit * (1 - 2 * ((me // bit) % 2))
        bit *= 2
    return peer


def block_copy(blocks_hbm, held, sems, i):
    at = pl.ds(i * CHUNK, CHUNK)
    return pltpu.make_async_copy(blocks_hbm.at[at], held.at[at], sems.at[i])


def block_step(held, picked, y, slices, transposed, u):
    row = lax.broadcasted_iota(jnp.int32, (8, LANES), 0)
    at = pl.ds(pl.multiple_of(8 * u, 8), 8)
    p = [picked[at, z * LANES:(z + 1) * LANES] for z in range(slices)]
    halves = []
    for t in range(2):
        sides = []
        for side in range(2):
            mask = row // 2 == 2 * t + side
            sides.append(jnp.concatenate([jnp.where(mask, v, 0.0) for v in p], axis=0))
        lhs = jnp.concatenate(sides, axis=1).astype(BF)
        m = [held[8 * u + 4 * t + j] for j in range(4)]
        if transposed:
            top, bottom = jnp.concatenate([m[0], m[2]], axis=1), jnp.concatenate([m[1], m[3]], axis=1)
            dims = (((1,), (1,)), ((), ()))
        else:
            top, bottom = jnp.concatenate([m[0], m[1]], axis=1), jnp.concatenate([m[2], m[3]], axis=1)
            dims = (((1,), (0,)), ((), ()))
        rhs = jnp.concatenate([top, bottom], axis=0)
        halves.append(lax.dot_general(lhs, rhs, dims, preferred_element_type=F32))
    for z in range(slices):
        a, b = (h[8 * z:8 * z + 8] for h in halves)
        low = jnp.where(row < 4, a[:, :LANES], b[:, :LANES])
        high = jnp.where(row < 4, a[:, LANES:], b[:, LANES:])
        y[at, z * LANES:(z + 1) * LANES] = jnp.where(row % 2 == 0, low, high)


def block_sweep(blocks_hbm, held, sems, picked, y, slices, transposed, waiting):
    def chunk(i, carry):
        if waiting:
            block_copy(blocks_hbm, held, sems, i).wait()
        for j in range(CHUNK // 8):
            block_step(held, picked, y, slices, transposed, i * (CHUNK // 8) + j)
        return carry

    lax.fori_loop(0, held.shape[0] // CHUNK, chunk, 0)


def gather_rows(hot, source):
    return jnp.dot(hot, source, preferred_element_type=F32)


def scatter_rows(hot, y):
    high = y.astype(BF)
    low = (y - high.astype(F32)).astype(BF)
    return jnp.dot(
        jnp.concatenate([hot, hot], axis=1), jnp.concatenate([high, low], axis=0), preferred_element_type=F32
    )


def join_kernel(
    plan, angle_ref, detector_ref, tile_ref, sino_ref, reflect_ref, cur_hbm, blocks_hbm, out_ref,
    held, cur, ray_hot, ray_turned, tile_hot, tile_turned, x, y, picked, total, part, got, fresh, full,
    own, pair, beside, across, onward,
    load, sems, send1, recv1, send2, recv2, ready,
    send_beside, recv_beside, send_across, recv_across, send_onward, recv_onward,
):
    agent = lax.axis_index("agent")
    me = lax.axis_index("tile")
    count, slices = plan
    chunks, height, columns = own.shape
    local = chunks * height // slices
    detectors = columns // LANES
    rays_here = fresh.shape[1]
    ray_total = count * rays_here
    tiles_here = detectors * local
    blocks_here = held.shape[0]
    order = list(range(count - 1, 0, -1))
    core = agent % 2
    neighbour = agent + 1 - 2 * core
    opposite = (agent + 2) % 4
    state = pltpu.make_async_copy(cur_hbm, cur, load.at[0])
    state.start()

    def send(source, target, s, r, k, to):
        return pltpu.make_async_remote_copy(
            src_ref=source.at[k], dst_ref=target.at[k], send_sem=s.at[k], recv_sem=r.at[k],
            device_id=(to, me), device_id_type=MESH,
        )

    def to_beside(k):
        return send(own, beside, send_beside, recv_beside, k, neighbour)

    def to_across(source, k):
        return send(source, across, send_across, recv_across, k, opposite)

    def to_onward(k):
        return send(across, onward, send_onward, recv_onward, k, neighbour)

    def rows_of(k):
        return slice(k * height, (k + 1) * height)

    def part_copy(step, d):
        return pltpu.make_async_remote_copy(
            src_ref=part.at[step, swap_bits(me, d)],
            dst_ref=got.at[step, d],
            send_sem=send1.at[step, d],
            recv_sem=recv1.at[step, d],
            device_id=(agent, swap_bits(me, d)),
            device_id_type=MESH,
        )

    def rest_copy(step, d):
        return pltpu.make_async_remote_copy(
            src_ref=fresh.at[step],
            dst_ref=full.at[step, me],
            send_sem=send2.at[step, d],
            recv_sem=recv2.at[step, d],
            device_id=(agent, swap_bits(me, d)),
            device_id_type=MESH,
        )

    def exchange(step):
        for slot in range(count):
            part[step, slot] = total[slot * rays_here:(slot + 1) * rays_here, :].astype(BF)
        for d in order:
            part_copy(step, d).start()
        own = total[pl.ds(pl.multiple_of(me * rays_here, 8), rays_here), :]
        measured = [sino_ref[pl.ds(z, rays_here, stride=slices), :] for z in range(slices)]
        value = own - jnp.concatenate(measured, axis=1)
        for d in reversed(order):
            part_copy(step, d).wait_recv()
            value = value + got[step, d].astype(F32)
        fresh[step] = value.astype(BF)
        for d in order:
            rest_copy(step, d).start()
        full[step, me] = fresh[step]
        for d in order:
            rest_copy(step, d).wait_recv()
        for d in order:
            part_copy(step, d).wait_send()
            rest_copy(step, d).wait_send()
        return full[step].reshape(ray_total, slices * LANES)

    @pl.when(agent == 0)
    def _():
        barrier = pltpu.get_barrier_semaphore()
        for d in order:
            pl.semaphore_signal(barrier, inc=1, device_id=(agent, swap_bits(me, d)), device_id_type=MESH)
        for peer in (neighbour, opposite):
            pl.semaphore_signal(barrier, inc=1, device_id=(peer, me), device_id_type=MESH)
        for i in range(blocks_here // CHUNK):
            block_copy(blocks_hbm, held, sems, i).start()

        hot_rows = lax.broadcasted_iota(jnp.int32, (ray_total, blocks_here), 0)
        ray = angle_ref[...] * detectors + detector_ref[...]
        hot = jnp.where(hot_rows == jnp.broadcast_to(ray, hot_rows.shape), 1.0, 0.0)
        ray_hot[...] = hot.astype(BF)
        ray_turned[...] = hot.T.astype(BF)
        hot_rows = lax.broadcasted_iota(jnp.int32, (tiles_here, blocks_here), 0)
        place = tile_ref[...]
        place = (place % detectors) * local + place // detectors
        hot = jnp.where(hot_rows == jnp.broadcast_to(place, hot_rows.shape), 1.0, 0.0)
        tile_hot[...] = hot.astype(BF)
        tile_turned[...] = hot.T.astype(BF)

        state.wait()
        for z in range(slices):
            for t in range(detectors):
                x[t * local:(t + 1) * local, z * LANES:(z + 1) * LANES] = cur[z * local:(z + 1) * local, t * LANES:(t + 1) * LANES]

        for step in range(DATA_STEPS):
            picked[...] = gather_rows(tile_turned[...], x[...].astype(BF))
            block_sweep(blocks_hbm, held, sems, picked, y, slices, True, step == 0)
            total[...] = scatter_rows(ray_hot[...], y[...])
            if step == 0:
                pl.semaphore_wait(barrier, count - 1)
            picked[...] = gather_rows(ray_turned[...], exchange(step))
            block_sweep(blocks_hbm, held, sems, picked, y, slices, False, False)
            x[...] = x[...] - 0.8 * scatter_rows(tile_hot[...], y[...])

        for z in range(slices):
            for t in range(detectors):
                moved = x[t * local:(t + 1) * local, z * LANES:(z + 1) * LANES]
                at = (slice(z * local, (z + 1) * local), slice(t * LANES, (t + 1) * LANES))
                out_ref[at] = 2.0 * moved - cur[at]
        for k in range(chunks):
            own[k] = out_ref[rows_of(k), :].astype(BF)
        out_ref[...] = 2.0 * cur[...] - out_ref[...]
        pl.semaphore_wait(ready.at[0], 2)

    @pl.when(agent != 0)
    def _():
        barrier = pltpu.get_barrier_semaphore()

        @pl.when(agent != 1)
        def _():
            pl.semaphore_signal(barrier, inc=1, device_id=(neighbour, me), device_id_type=MESH)

        @pl.when(agent != 2)
        def _():
            pl.semaphore_signal(barrier, inc=1, device_id=(opposite, me), device_id_type=MESH)

        for k in range(chunks):
            own[k] = reflect_ref[rows_of(k), :].astype(BF)
        state.wait()
        out_ref[...] = 2.0 * cur[...] - reflect_ref[...]
        pl.semaphore_wait(barrier, 2)

        @pl.when(agent != 3)
        def _():
            pl.semaphore_signal(ready.at[0], inc=1, device_id=(0, me), device_id_type=MESH)

    def add(k, others):
        out_ref[rows_of(k), :] = out_ref[rows_of(k), :] + others

    @pl.when(agent < 2)
    def _():
        for k in range(chunks):
            to_across(own, k).start()
            to_beside(k).start()
        for k in range(chunks):
            to_beside(k).wait_recv()
            to_across(own, k).wait_recv()
            add(k, beside[k].astype(F32) + across[k].astype(F32))
        for k in range(chunks):
            to_across(own, k).wait_send()
            to_beside(k).wait_send()

    @pl.when(agent >= 2)
    def _():
        for k in range(chunks):
            to_beside(k).start()
        for k in range(chunks):
            to_beside(k).wait_recv()
            pair[k] = (own[k].astype(F32) + beside[k].astype(F32)).astype(BF)
            to_across(pair, k).start()
        for k in range(chunks):
            to_across(pair, k).wait_recv()
            to_onward(k).start()
            add(k, beside[k].astype(F32) + across[k].astype(F32))
        for k in range(chunks):
            to_onward(k).wait_recv()
            add(k, onward[k].astype(F32))
        for k in range(chunks):
            to_beside(k).wait_send()
            to_across(pair, k).wait_send()
            to_onward(k).wait_send()


def idle_kernel(out_ref):
    pass


def join(angle, detector, tile, sinogram, reflect, current, blocks, count):
    slices, local, columns = current.shape
    rays_here = sinogram.shape[0]
    ray_total = rays_here * count
    tiles_here = columns // LANES * local
    blocks_here = blocks.shape[0]
    width = slices * LANES
    rows = slices * local
    chunks = max(1, rows // 32)
    chunk = (chunks, rows // chunks, columns)
    vmem = pl.BlockSpec(memory_space=pltpu.VMEM)
    anywhere = pl.BlockSpec(memory_space=pl.ANY)
    out = pl.pallas_call(
        functools.partial(join_kernel, (count, slices)),
        out_shape=jax.ShapeDtypeStruct((rows, columns), F32),
        in_specs=[vmem] * 5 + [anywhere] * 2,
        out_specs=vmem,
        scratch_shapes=[
            pltpu.VMEM(blocks.shape, BF),
            pltpu.VMEM((rows, columns), F32),
            pltpu.VMEM((ray_total, blocks_here), BF),
            pltpu.VMEM((blocks_here, ray_total), BF),
            pltpu.VMEM((tiles_here, blocks_here), BF),
            pltpu.VMEM((blocks_here, tiles_here), BF),
            pltpu.VMEM((tiles_here, width), F32),
            pltpu.VMEM((blocks_here, width), F32),
            pltpu.VMEM((blocks_here, width), F32),
            pltpu.VMEM((ray_total, width), F32),
            pltpu.VMEM((DATA_STEPS, count, rays_here, width), BF),
            pltpu.VMEM((DATA_STEPS, count, rays_here, width), BF),
            pltpu.VMEM((DATA_STEPS, rays_here, width), BF),
            pltpu.VMEM((DATA_STEPS, count, rays_here, width), BF),
        ]
        + [pltpu.VMEM(chunk, BF)] * 5
        + [pltpu.SemaphoreType.DMA((1,)), pltpu.SemaphoreType.DMA((blocks_here // CHUNK,))]
        + [pltpu.SemaphoreType.DMA((DATA_STEPS, count))] * 4
        + [pltpu.SemaphoreType.REGULAR((1,))]
        + [pltpu.SemaphoreType.DMA((chunks,))] * 6,
        compiler_params=pltpu.CompilerParams(
            collective_id=0, has_side_effects=True, vmem_limit_bytes=58 * 1024 * 1024
        ),
        name="join_agents",
    )(
        angle.reshape(1, -1), detector.reshape(1, -1), tile.reshape(1, -1),
        sinogram.reshape(rays_here * slices, LANES), reflect.reshape(rows, columns),
        current.reshape(rows, columns), blocks,
    )
    return out.reshape(current.shape)


def per_device(
    states,
    sinogram,
    blocks,
    block_angle,
    block_detector,
    block_tile,
    conv_first,
    conv_hidden,
    conv_last,
):
    current = states[0]
    agent_place = lax.axis_index("agent")
    halo = conv_hidden.shape[1] + 2
    filters = (conv_first, conv_hidden, conv_last)
    edges = halo_exchange(current, halo)

    def data_only():
        return pl.pallas_call(
            idle_kernel,
            out_shape=jax.ShapeDtypeStruct(current.shape, F32),
            out_specs=pl.BlockSpec(memory_space=pl.ANY),
            name="idle",
        )()

    def axial_only():
        return axial_reflect(edges, current, *filters, halo)

    def sagittal_only():
        return plane_call(1, edges, current, *filters, halo, 1)

    def coronal_only():
        return coronal_reflect(current, *filters)

    reflect = lax.switch(agent_place, [data_only, axial_only, sagittal_only, coronal_only])
    joined = join(
        block_angle, block_detector, block_tile, sinogram, reflect, current, blocks, lax.axis_size("tile")
    )
    return (0.25 * joined)[None]


def solution(mesh):
    placed = (
        P("agent", None, "tile", None),
        P("tile", None, None),
        P("tile", None, None),
        P("tile"),
        P("tile"),
        P("tile"),
        P(),
        P(),
        P(),
    )
    return jax.shard_map(
        per_device,
        mesh=mesh,
        in_specs=placed,
        out_specs=P("agent", None, "tile", None),
        check_vma=False,
    )
```

```python
import functools

import jax
import jax.numpy as jnp
from jax import lax
from jax.experimental import pallas as pl
from jax.experimental.pallas import tpu as pltpu
from jax.sharding import PartitionSpec as P

DATA_STEPS = 2
MESH = pl.DeviceIdType.MESH
LANES = 128
STRIPS = 16
CHUNK = 64
SPAN = 256
BF = jnp.bfloat16
F32 = jnp.float32
NATURAL = (0, 1, 2, 3)
EVEN_ORDER = (0, 1, 2, 3)
ODD_ORDER = (1, 0, 3, 2)


def main_cells(offset):
    order = EVEN_ORDER if offset % 2 else ODD_ORDER
    return [(offset, column) for column in order]

def edge_cells(offset):
    return [(offset + 1, 4), (offset, 4), (offset, -1), (offset + 1, -1)]

def window_cells(rows):
    tiles = [main_cells(a) for a in range(rows + 2)]
    return tiles + [edge_cells(a) for a in range(0, rows + 2, 2)]

def spread_lanes(w):
    return jnp.concatenate([w] * (LANES // w.shape[-1]), axis=-1)

def lane_iota(rows):
    return lax.broadcasted_iota(jnp.int32, (rows, LANES), 1)

def slot_mix(rows, taps, column_in, order, width):
    slot = lane_iota(rows) // width
    mixed = jnp.zeros((rows, LANES), F32)
    for place, column in enumerate(order):
        tap = column_in - column + 1
        if 0 <= tap < 3:
            mixed = jnp.where(slot == place, taps[tap], mixed)
    return mixed

def build_first(w_ref, o, w1):
    for k in range(6):
        for half in range(2):
            order = ODD_ORDER if half else EVEN_ORDER
            mixes = []
            for ti in range(3):
                taps = [jnp.broadcast_to(spread_lanes(w_ref[o, ti, tj:tj+1, :].astype(F32)), (16, LANES)) for tj in range(3)]
                mixes.append(slot_mix(16, taps, k - 1, order, 32))
            row = lax.broadcasted_iota(jnp.int32, (16, LANES), 0)
            for t in range(4):
                value = jnp.zeros((16, LANES), F32)
                for ti in range(3):
                    value = jnp.where(row == 2 * t + half + ti, mixes[ti], value)
                at = t * 2 * LANES + half * LANES
                w1[k * 16:(k + 1) * 16, at:at + LANES] = value.astype(BF)

def build_hidden(w_ref, o, layer, wh):
    wide = [[spread_lanes(w_ref[o, layer, ti, tj].astype(F32)) for tj in range(3)] for ti in range(3)]
    inner = wide[0][0].shape[0]
    for n, tile in enumerate(window_cells(2)):
        for slot, (a, column) in enumerate(tile):
            at = n * LANES + slot * inner
            for half in range(2):
                ti = a - (half + 1) + 1
                if 0 <= ti < 3:
                    value = slot_mix(inner, wide[ti], column, ODD_ORDER if half else EVEN_ORDER, inner)
                else:
                    value = jnp.zeros((inner, LANES), F32)
                wh[layer, at:at + inner, half * LANES:(half + 1) * LANES] = value.astype(BF)

def column_of(row):
    inner = row.shape[1]
    r = lax.broadcasted_iota(jnp.int32, (inner, inner), 0)
    c = lax.broadcasted_iota(jnp.int32, (inner, inner), 1)
    picked = jnp.where(r == c, jnp.broadcast_to(row, (inner, inner)), 0.0)
    return jnp.broadcast_to(jnp.sum(picked, axis=1, keepdims=True), (inner, LANES))

def build_last(w_ref, o, wl):
    taps = [[column_of(w_ref[o, ti, tj:tj+1, :].astype(F32)) for tj in range(3)] for ti in range(3)]
    inner = taps[0][0].shape[0]
    lane = lane_iota(inner)
    row8 = lane % 8
    zero = jnp.zeros((inner, LANES), F32)
    rows = []
    for a in range(10):
        line = []
        for tj in range(3):
            value = zero
            for ti in range(3):
                if 0 <= a - ti < 8:
                    value = jnp.where(row8 == a - ti, taps[ti][tj], value)
            line.append(value)
        rows.append(line)
    for n, tile in enumerate(window_cells(8)):
        for slot, (a, column) in enumerate(tile):
            at = n * LANES + slot * inner
            wl[at:at + inner, :] = slot_mix(inner, rows[a], column, EVEN_ORDER, LANES // 4).astype(BF)


def axial_kernel(plan, edges_ref, cur_ref, cf_ref, ch_ref, cl_ref, out_ref, main, edge, w1, wh, wl, raw, xs, place, back, gathered_out):
    halo, chunk = plan
    slices, local, columns = cur_ref.shape
    rows = local + 2 * halo
    stored = rows + 8
    groups = columns // 4
    per = groups // STRIPS
    span = slices * groups
    layers = ch_ref.shape[1]
    tile = lax.axis_index("tile")
    at_start = tile == 0
    at_end = tile == lax.axis_size("tile") - 1
    fill_rows(raw, edges_ref, cur_ref, stored, halo)

    build_first(cf_ref, 0, w1)
    for layer in range(layers):
        build_hidden(ch_ref, 0, layer, wh)
    build_last(cl_ref, 0, wl)

    col = lax.broadcasted_iota(jnp.int32, (columns, groups), 0)
    m = lax.broadcasted_iota(jnp.int32, (columns, groups), 1)
    first_col = 4 * ((m % STRIPS) * per + m // STRIPS)
    for k in range(6):
        place[:, k * groups:(k + 1) * groups] = jnp.where(col == first_col + (k - 1), 1.0, 0.0).astype(BF)
    m = lax.broadcasted_iota(jnp.int32, (groups, columns), 0)
    col = lax.broadcasted_iota(jnp.int32, (groups, columns), 1)
    first_col = 4 * ((m % STRIPS) * per + m // STRIPS)
    for k in range(4):
        back[k * groups:(k + 1) * groups, :] = jnp.where(col == first_col + k, 1.0, 0.0).astype(BF)
    xs[...] = jnp.dot(raw[...].astype(BF), place[...], preferred_element_type=F32)

    slot = lane_iota(STRIPS) // (LANES // 4)
    even_slots = (slot == 0) | (slot == 3)
    right_slots = slot < 2
    strip = lax.broadcasted_iota(jnp.int32, (STRIPS, LANES), 0)
    zero_tile = jnp.zeros((slices, per, STRIPS, LANES), BF)

    for side in range(2):
        for r in (0, 1, 2, rows - 1, rows, rows + 1):
            main[side, r] = zero_tile
        for e in (0, 1, rows // 2 - 1, rows // 2):
            edge[side, e] = zero_tile

    def put_edge(side, e, odd_row, even_row):
        v = jnp.where(even_slots, even_row, odd_row)
        for z in range(slices):
            for i in range(per):
                if i + 1 < per:
                    right = v[z, i + 1]
                else:
                    right = jnp.where(strip == STRIPS - 1, 0.0, pltpu.roll(v[z, 0], STRIPS - 1, 0))
                if i > 0:
                    left = v[z, i - 1]
                else:
                    left = jnp.where(strip == 0, 0.0, pltpu.roll(v[z, per - 1], 1, 0))
                edge[side, e, z, i] = jnp.where(right_slots, right, left).astype(BF)

    def put_pairs(side, pair, count, y):
        before = main[side, 2 * pair].astype(F32)
        for t in range(count):
            row = 2 * (pair + t)
            outside = (at_start & (row < halo)) | (at_end & (row >= rows - halo))
            v = jnp.maximum(y(t), 0.0) * jnp.where(outside, 0.0, 1.0)
            even_row = v[:, :LANES].reshape(slices, per, STRIPS, LANES)
            odd_row = v[:, LANES:].reshape(slices, per, STRIPS, LANES)
            main[side, row + 1] = even_row.astype(BF)
            main[side, row + 2] = odd_row.astype(BF)
            put_edge(side, pair + t, before, even_row)
            before = odd_row

    def first_step(c, carry):
        parts = []
        for z in range(slices):
            at = pl.ds(pl.multiple_of(z * stored + 8 * c, 8), 16)
            parts.append(jnp.concatenate([xs[at, k * groups:(k + 1) * groups] for k in range(6)], axis=0).astype(BF))
        x = jnp.concatenate(parts, axis=1)
        y = lax.dot_general(x, w1[...], (((0,), (0,)), ((), ())), preferred_element_type=F32)
        put_pairs(0, 4 * c, 4, lambda t: y[:, t * 2 * LANES:(t + 1) * 2 * LANES])
        return carry

    lax.fori_loop(0, rows // 8, first_step, 0)

    def window(side, pair, out_rows):
        parts = [main[side, 2 * pair + a].reshape(span, LANES) for a in range(out_rows + 2)]
        parts += [edge[side, pair + e].reshape(span, LANES) for e in range(out_rows // 2 + 1)]
        return jnp.concatenate(parts, axis=1)

    pairs = rows // 2 - 2
    for layer in range(layers):
        source, target = layer % 2, (layer + 1) % 2

        def hidden_step(c, carry):
            pair = 1 + c * chunk
            x = jnp.concatenate([window(source, pair + t, 2) for t in range(chunk)], axis=0)
            y = jnp.dot(x, wh[layer], preferred_element_type=F32)
            put_pairs(target, pair, chunk, lambda t: y[t * span:(t + 1) * span])
            return carry

        lax.fori_loop(0, pairs // chunk, hidden_step, 0)
        end = rows // 2 - 1
        put_edge(target, end, main[target, 2 * end].astype(F32), jnp.zeros((slices, per, STRIPS, LANES), F32))

    eighths = local // 8
    quad = (lane_iota(span) // 8) % 4

    def last_step(q, carry):
        x = window(layers % 2, halo // 2 + 4 * q, 8)
        y = jnp.dot(x, wl[...], preferred_element_type=F32)
        gathered_out[q // 4] = jnp.where(quad == q % 4, y, gathered_out[q // 4])
        return carry

    gathered_out[...] = jnp.zeros_like(gathered_out)
    lax.fori_loop(0, eighths, last_step, 0)

    for big in range(gathered_out.shape[0]):
        height = min(32, local - 32 * big)
        turned = [gathered_out[big, z * groups:(z + 1) * groups, :].T for z in range(slices)]
        lines = [jnp.concatenate([turned[z][k * 32:(k + 1) * 32] for k in range(4)], axis=1) for z in range(slices)]
        values = jnp.concatenate(lines, axis=0)
        high = values.astype(BF)
        low = (values - high.astype(F32)).astype(BF)
        net = jnp.dot(high, back[...], preferred_element_type=F32) + jnp.dot(low, back[...], preferred_element_type=F32)
        for z in range(slices):
            at = pl.ds(32 * big, height)
            out_ref[z, at, :] = cur_ref[z, at, :] - 2.0 * net[z * 32:z * 32 + height]

def axial_reflect(edges, current, cf, ch, cl, halo):
    slices, local, columns = current.shape
    rows = local + 2 * halo
    groups = columns // 4
    per = groups // STRIPS
    stored = rows + 8
    whole = pl.BlockSpec(memory_space=pltpu.VMEM)
    return pl.pallas_call(
        functools.partial(axial_kernel, (halo, 2)),
        out_shape=jax.ShapeDtypeStruct(current.shape, F32),
        in_specs=[whole] * 5,
        out_specs=whole,
        scratch_shapes=[
            pltpu.VMEM((2, rows + 2, slices, per, STRIPS, LANES), BF),
            pltpu.VMEM((2, rows // 2 + 1, slices, per, STRIPS, LANES), BF),
            pltpu.VMEM((96, 8 * LANES), BF),
            pltpu.VMEM((ch.shape[1], 6 * LANES, 2 * LANES), BF),
            pltpu.VMEM((15 * LANES, LANES), BF),
            pltpu.VMEM((slices * stored, columns), F32),
            pltpu.VMEM((slices * stored, 6 * groups), F32),
            pltpu.VMEM((columns, 6 * groups), BF),
            pltpu.VMEM((4 * groups, columns), BF),
            pltpu.VMEM((-(-local // 32), slices * groups, LANES), F32),
        ],
        compiler_params=pltpu.CompilerParams(vmem_limit_bytes=60 * 1024 * 1024),
        name="net_axial",
    )(edges, current, cf, ch, cl)


def fill_rows(raw, edges_ref, cur_ref, stored, halo):
    slices, local, columns = cur_ref.shape
    zero = jnp.zeros((1, columns), F32)
    tail = jnp.zeros((stored - 1 - local - 2 * halo, columns), F32)
    for z in range(slices):
        above = edges_ref[0, z * halo:(z + 1) * halo, :].astype(F32)
        below = edges_ref[1, z * halo:(z + 1) * halo, :].astype(F32)
        raw[z * stored:(z + 1) * stored, :] = jnp.concatenate([zero, above, cur_ref[z], below, tail], axis=0)


def build_first_plane(w_ref, o, w1):
    row = lax.broadcasted_iota(jnp.int32, (16, LANES), 0)
    for z in range(4):
        mixes = []
        for tj in range(3):
            taps = [jnp.broadcast_to(spread_lanes(w_ref[o, ti, tj:tj+1, :].astype(F32)), (16, LANES)) for ti in range(3)]
            mixes.append(slot_mix(16, taps, z, NATURAL, 32))
        for t in range(8):
            value = jnp.zeros((16, LANES), F32)
            for tj in range(3):
                value = jnp.where(row == t + tj, mixes[tj], value)
            w1[z * 16:(z + 1) * 16, t * LANES:(t + 1) * LANES] = value.astype(BF)

def build_hidden_plane(w_ref, o, layer, wh):
    wide = [[spread_lanes(w_ref[o, layer, ti, tj].astype(F32)) for ti in range(3)] for tj in range(3)]
    inner = wide[0][0].shape[0]
    for a in range(4):
        for z in range(4):
            at = a * LANES + z * inner
            for half in range(2):
                if 0 <= a - half < 3:
                    value = slot_mix(inner, wide[a - half], z, NATURAL, inner)
                else:
                    value = jnp.zeros((inner, LANES), F32)
                wh[layer, at:at + inner, half * LANES:(half + 1) * LANES] = value.astype(BF)

def build_last_plane(w_ref, o, wl):
    taps = [[column_of(w_ref[o, ti, tj:tj+1, :].astype(F32)) for ti in range(3)] for tj in range(3)]
    inner = taps[0][0].shape[0]
    row8 = lane_iota(inner) % 8
    zero = jnp.zeros((inner, LANES), F32)
    for a in range(10):
        line = []
        for ti in range(3):
            value = zero
            for tj in range(3):
                if 0 <= a - tj < 8:
                    value = jnp.where(row8 == a - tj, taps[tj][ti], value)
            line.append(value)
        for z in range(4):
            at = a * LANES + z * inner
            wl[at:at + inner, :] = slot_mix(inner, line, z, NATURAL, LANES // 4).astype(BF)


def plane_kernel(plan, x_ref, cur_ref, cf_ref, ch_ref, cl_ref, out_ref, main, w1, wh, wl, xs, gathered_out):
    o, halo, chunk, strips = plan
    slices, local, span = out_ref.shape
    rows = local + 2 * halo
    stored = rows + 8
    layers = ch_ref.shape[1]
    if halo:
        tile = lax.axis_index("tile")
        at_start = tile == 0
        at_end = tile == lax.axis_size("tile") - 1

    build_first_plane(cf_ref, o, w1)
    for layer in range(layers):
        build_hidden_plane(ch_ref, o, layer, wh)
    build_last_plane(cl_ref, o, wl)
    if halo:
        fill_rows(xs, x_ref, cur_ref, stored, halo)
    else:
        xs[...] = x_ref[...].astype(F32)
    for side in range(2):
        for r in (0, rows + 1):
            main[side, r] = jnp.zeros((span, LANES), BF)

    def put_pairs(side, pair, count, y):
        for t in range(count):
            row = 2 * (pair + t)
            v = jnp.maximum(y(t), 0.0)
            if halo:
                outside = (at_start & (row < halo)) | (at_end & (row >= rows - halo))
                v = v * jnp.where(outside, 0.0, 1.0)
            main[side, row + 1] = v[:, :LANES].astype(BF)
            main[side, row + 2] = v[:, LANES:].astype(BF)

    def ends(side):
        if strips > 1:
            step = span // strips
            main[side, 0, step:span] = main[side, rows, 0:span - step]
            main[side, rows + 1, 0:span - step] = main[side, 1, step:span]

    def first_step(c, carry):
        parts = [xs[pl.ds(pl.multiple_of(z * stored + 8 * c, 8), 16)] for z in range(slices)]
        x = jnp.concatenate(parts, axis=0).astype(BF)
        y = lax.dot_general(x, w1[...], (((0,), (0,)), ((), ())), preferred_element_type=F32)
        put_pairs(0, 4 * c, 4, lambda t: y[:, t * 2 * LANES:(t + 1) * 2 * LANES])
        return carry

    lax.fori_loop(0, rows // 8, first_step, 0)
    ends(0)

    for layer in range(layers):
        source, target = layer % 2, (layer + 1) % 2

        def hidden_step(c, carry):
            pair = c * chunk
            tiles = [main[source, 2 * pair + a] for a in range(2 * chunk + 2)]
            x = jnp.concatenate([jnp.concatenate(tiles[2 * t:2 * t + 4], axis=1) for t in range(chunk)], axis=0)
            y = jnp.dot(x, wh[layer], preferred_element_type=F32)
            put_pairs(target, pair, chunk, lambda t: y[t * span:(t + 1) * span])
            return carry

        lax.fori_loop(0, rows // 2 // chunk, hidden_step, 0)
        ends(target)

    quad = (lane_iota(span) // 8) % 4

    def last_step(q, carry):
        x = jnp.concatenate([main[layers % 2, halo + 8 * q + a] for a in range(10)], axis=1)
        y = jnp.dot(x, wl[...], preferred_element_type=F32)
        gathered_out[q // 4] = jnp.where(quad == q % 4, y, gathered_out[q // 4])
        return carry

    gathered_out[...] = jnp.zeros_like(gathered_out)
    lax.fori_loop(0, local // 8, last_step, 0)
    for big in range(gathered_out.shape[0]):
        height = min(32, local - 32 * big)
        net = gathered_out[big].T
        for z in range(slices):
            at = pl.ds(32 * big, height)
            out_ref[z, at, :] = cur_ref[z, at, :] - 2.0 * net[z * 32:z * 32 + height]

def plane_call(o, x, current, cf, ch, cl, halo, strips):
    slices, local, span = current.shape
    rows = local + 2 * halo
    whole = pl.BlockSpec(memory_space=pltpu.VMEM)
    return pl.pallas_call(
        functools.partial(plane_kernel, (o, halo, 4, strips)),
        out_shape=jax.ShapeDtypeStruct(current.shape, F32),
        in_specs=[whole] * 5, out_specs=whole,
        scratch_shapes=[
            pltpu.VMEM((2, rows + 2, span, LANES), BF),
            pltpu.VMEM((64, 8 * LANES), BF),
            pltpu.VMEM((ch.shape[1], 4 * LANES, 2 * LANES), BF),
            pltpu.VMEM((10 * LANES, LANES), BF),
            pltpu.VMEM((slices * (rows + 8), span), F32),
            pltpu.VMEM((-(-local // 32), span, LANES), F32),
        ],
        compiler_params=pltpu.CompilerParams(vmem_limit_bytes=60 * 1024 * 1024),
        name="net_sagittal" if halo else "net_coronal",
    )(x, current, cf, ch, cl)

def coronal_reflect(current, cf, ch, cl):
    slices, local, columns = current.shape
    strips = columns // local
    turned = jnp.transpose(current.reshape(slices, local, strips, local), (0, 3, 2, 1))
    t = turned.astype(BF)
    none = jnp.zeros((slices, 1, 1, local), BF)
    before = jnp.concatenate([none, t[:, -1:, :-1]], axis=2)
    after = jnp.concatenate([t[:, :1, 1:], none], axis=2)
    rest = jnp.zeros((slices, 6, strips, local), BF)
    x = jnp.concatenate([before, t, after, rest], axis=1)
    x = x.reshape(-1, columns)
    out = plane_call(2, x, turned.reshape(slices, local, columns), cf, ch, cl, 0, strips)
    return jnp.transpose(out.reshape(slices, local, strips, local), (0, 3, 2, 1)).reshape(current.shape)

def halo_kernel(halo, cur_hbm, out_ref, edge, sent, load, send, recv):
    agent = lax.axis_index("agent")
    tile = lax.axis_index("tile")
    last = lax.axis_size("tile") - 1
    slices, local, columns = cur_hbm.shape
    rows = edge.shape[2]
    active = (agent == 1) | (agent == 2)

    def copy(side, peer):
        return pltpu.make_async_remote_copy(
            src_ref=sent.at[side],
            dst_ref=out_ref.at[1 - side],
            send_sem=send.at[side],
            recv_sem=recv.at[1 - side],
            device_id=(agent, peer),
            device_id_type=MESH,
        )

    @pl.when(active)
    def _():
        barrier = pltpu.get_barrier_semaphore()

        @pl.when(tile > 0)
        def _():
            pl.semaphore_signal(barrier, inc=1, device_id=(agent, tile - 1), device_id_type=MESH)

        @pl.when(tile < last)
        def _():
            pl.semaphore_signal(barrier, inc=1, device_id=(agent, tile + 1), device_id_type=MESH)

        loads = [
            pltpu.make_async_copy(cur_hbm.at[:, pl.ds(0, rows)], edge.at[0], load.at[0]),
            pltpu.make_async_copy(cur_hbm.at[:, pl.ds(local - rows, rows)], edge.at[1], load.at[1]),
        ]
        for item in loads:
            item.start()
        for item in loads:
            item.wait()
        for side in range(2):
            first = 0 if side == 0 else rows - halo
            parts = [edge[side, z, first:first + halo, :] for z in range(slices)]
            sent[side] = jnp.concatenate(parts, axis=0).astype(BF)

        pl.semaphore_wait(barrier, jnp.where(tile > 0, 1, 0) + jnp.where(tile < last, 1, 0))

        @pl.when(tile > 0)
        def _():
            copy(0, tile - 1).start()

        @pl.when(tile < last)
        def _():
            copy(1, tile + 1).start()

        @pl.when(tile == 0)
        def _():
            out_ref[0] = jnp.zeros(out_ref.shape[1:], BF)

        @pl.when(tile == last)
        def _():
            out_ref[1] = jnp.zeros(out_ref.shape[1:], BF)

        @pl.when(tile > 0)
        def _():
            copy(1, tile - 1).wait_recv()

        @pl.when(tile < last)
        def _():
            copy(0, tile + 1).wait_recv()

        @pl.when(tile > 0)
        def _():
            copy(0, tile - 1).wait_send()

        @pl.when(tile < last)
        def _():
            copy(1, tile + 1).wait_send()


def halo_exchange(current, halo):
    slices, local, columns = current.shape
    return pl.pallas_call(
        functools.partial(halo_kernel, halo),
        out_shape=jax.ShapeDtypeStruct((2, slices * halo, columns), BF),
        in_specs=[pl.BlockSpec(memory_space=pl.ANY)],
        out_specs=pl.BlockSpec(memory_space=pltpu.VMEM),
        scratch_shapes=[
            pltpu.VMEM((2, slices, 8, columns), F32),
            pltpu.VMEM((2, slices * halo, columns), BF),
            pltpu.SemaphoreType.DMA((2,)),
            pltpu.SemaphoreType.DMA((2,)),
            pltpu.SemaphoreType.DMA((2,)),
        ],
        compiler_params=pltpu.CompilerParams(collective_id=2, has_side_effects=True),
        name="halo_exchange",
    )(current)


def swap_bits(me, d):
    peer, bit = me, 1
    while bit <= d:
        if d & bit:
            peer = peer + bit * (1 - 2 * ((me // bit) % 2))
        bit *= 2
    return peer


def block_copy(blocks_hbm, held, sems, i):
    at = pl.ds(i * CHUNK, CHUNK)
    return pltpu.make_async_copy(blocks_hbm.at[at], held.at[at], sems.at[i])


def block_step(held, picked, y, slices, transposed, u):
    row = lax.broadcasted_iota(jnp.int32, (8, LANES), 0)
    at = pl.ds(pl.multiple_of(8 * u, 8), 8)
    p = [picked[at, z * LANES:(z + 1) * LANES] for z in range(slices)]
    halves = []
    for t in range(2):
        sides = []
        for side in range(2):
            mask = row // 2 == 2 * t + side
            sides.append(jnp.concatenate([jnp.where(mask, v, 0.0) for v in p], axis=0))
        lhs = jnp.concatenate(sides, axis=1).astype(BF)
        m = [held[8 * u + 4 * t + j] for j in range(4)]
        if transposed:
            top, bottom = jnp.concatenate([m[0], m[2]], axis=1), jnp.concatenate([m[1], m[3]], axis=1)
            dims = (((1,), (1,)), ((), ()))
        else:
            top, bottom = jnp.concatenate([m[0], m[1]], axis=1), jnp.concatenate([m[2], m[3]], axis=1)
            dims = (((1,), (0,)), ((), ()))
        rhs = jnp.concatenate([top, bottom], axis=0)
        halves.append(lax.dot_general(lhs, rhs, dims, preferred_element_type=F32))
    for z in range(slices):
        a, b = (h[8 * z:8 * z + 8] for h in halves)
        low = jnp.where(row < 4, a[:, :LANES], b[:, :LANES])
        high = jnp.where(row < 4, a[:, LANES:], b[:, LANES:])
        y[at, z * LANES:(z + 1) * LANES] = jnp.where(row % 2 == 0, low, high)


def block_sweep(blocks_hbm, held, sems, picked, y, slices, transposed, waiting):
    span = min(SPAN, held.shape[0])

    def chunk(i, carry):
        for j in range(span // 8):
            if waiting and j % (CHUNK // 8) == 0:
                block_copy(blocks_hbm, held, sems, i * (span // CHUNK) + j // (CHUNK // 8)).wait()
            block_step(held, picked, y, slices, transposed, i * (span // 8) + j)
        return carry

    lax.fori_loop(0, held.shape[0] // span, chunk, 0)


def gather_rows(hot, source):
    return jnp.dot(hot, source, preferred_element_type=F32)


def scatter_rows(hot, y):
    high = y.astype(BF)
    low = (y - high.astype(F32)).astype(BF)
    return jnp.dot(
        jnp.concatenate([hot, hot], axis=1), jnp.concatenate([high, low], axis=0), preferred_element_type=F32
    )


def join_kernel(
    plan, angle_ref, detector_ref, tile_ref, sino_ref, reflect_ref, cur_hbm, blocks_hbm, out_ref,
    held, cur, ray_hot, ray_turned, tile_hot, tile_turned, x, y, picked, total, part, got, fresh, full,
    own, pair, beside, across, onward,
    load, sems, send1, recv1, send2, recv2, ready,
    send_beside, recv_beside, send_across, recv_across, send_onward, recv_onward,
):
    agent = lax.axis_index("agent")
    me = lax.axis_index("tile")
    count, slices = plan
    chunks, height, columns = own.shape
    local = chunks * height // slices
    detectors = columns // LANES
    rays_here = fresh.shape[1]
    ray_total = count * rays_here
    tiles_here = detectors * local
    blocks_here = held.shape[0]
    order = list(range(count - 1, 0, -1))
    core = agent % 2
    neighbour = agent + 1 - 2 * core
    opposite = (agent + 2) % 4
    state = pltpu.make_async_copy(cur_hbm, cur, load.at[0])
    state.start()

    def send(source, target, s, r, k, to):
        return pltpu.make_async_remote_copy(
            src_ref=source.at[k], dst_ref=target.at[k], send_sem=s.at[k], recv_sem=r.at[k],
            device_id=(to, me), device_id_type=MESH,
        )

    def to_beside(k):
        return send(own, beside, send_beside, recv_beside, k, neighbour)

    def to_across(source, k):
        return send(source, across, send_across, recv_across, k, opposite)

    def to_onward(k):
        return send(across, onward, send_onward, recv_onward, k, neighbour)

    def rows_of(k):
        return slice(k * height, (k + 1) * height)

    def part_copy(step, d):
        return pltpu.make_async_remote_copy(
            src_ref=part.at[step, swap_bits(me, d)],
            dst_ref=got.at[step, d],
            send_sem=send1.at[step, d],
            recv_sem=recv1.at[step, d],
            device_id=(agent, swap_bits(me, d)),
            device_id_type=MESH,
        )

    def rest_copy(step, d):
        return pltpu.make_async_remote_copy(
            src_ref=fresh.at[step],
            dst_ref=full.at[step, me],
            send_sem=send2.at[step, d],
            recv_sem=recv2.at[step, d],
            device_id=(agent, swap_bits(me, d)),
            device_id_type=MESH,
        )

    def exchange(step):
        for slot in range(count):
            part[step, slot] = total[slot * rays_here:(slot + 1) * rays_here, :].astype(BF)
        for d in order:
            part_copy(step, d).start()
        own = total[pl.ds(pl.multiple_of(me * rays_here, 8), rays_here), :]
        measured = [sino_ref[pl.ds(z, rays_here, stride=slices), :] for z in range(slices)]
        value = own - jnp.concatenate(measured, axis=1)
        for d in reversed(order):
            part_copy(step, d).wait_recv()
            value = value + got[step, d].astype(F32)
        fresh[step] = value.astype(BF)
        for d in order:
            rest_copy(step, d).start()
        full[step, me] = fresh[step]
        for d in order:
            rest_copy(step, d).wait_recv()
        for d in order:
            part_copy(step, d).wait_send()
            rest_copy(step, d).wait_send()
        return full[step].reshape(ray_total, slices * LANES)

    @pl.when(agent == 0)
    def _():
        barrier = pltpu.get_barrier_semaphore()
        for d in order:
            pl.semaphore_signal(barrier, inc=1, device_id=(agent, swap_bits(me, d)), device_id_type=MESH)
        for peer in (neighbour, opposite):
            pl.semaphore_signal(barrier, inc=1, device_id=(peer, me), device_id_type=MESH)
        for i in range(blocks_here // CHUNK):
            block_copy(blocks_hbm, held, sems, i).start()

        hot_rows = lax.broadcasted_iota(jnp.int32, (ray_total, blocks_here), 0)
        ray = angle_ref[...] * detectors + detector_ref[...]
        hot = jnp.where(hot_rows == jnp.broadcast_to(ray, hot_rows.shape), 1.0, 0.0)
        ray_hot[...] = hot.astype(BF)
        ray_turned[...] = hot.T.astype(BF)
        hot_rows = lax.broadcasted_iota(jnp.int32, (tiles_here, blocks_here), 0)
        place = tile_ref[...]
        place = (place % detectors) * local + place // detectors
        hot = jnp.where(hot_rows == jnp.broadcast_to(place, hot_rows.shape), 1.0, 0.0)
        tile_hot[...] = hot.astype(BF)
        tile_turned[...] = hot.T.astype(BF)

        state.wait()
        for z in range(slices):
            for t in range(detectors):
                x[t * local:(t + 1) * local, z * LANES:(z + 1) * LANES] = cur[z * local:(z + 1) * local, t * LANES:(t + 1) * LANES]

        for step in range(DATA_STEPS):
            picked[...] = gather_rows(tile_turned[...], x[...].astype(BF))
            block_sweep(blocks_hbm, held, sems, picked, y, slices, True, step == 0)
            total[...] = scatter_rows(ray_hot[...], y[...])
            if step == 0:
                pl.semaphore_wait(barrier, count - 1)
            picked[...] = gather_rows(ray_turned[...], exchange(step))
            block_sweep(blocks_hbm, held, sems, picked, y, slices, False, False)
            x[...] = x[...] - 0.8 * scatter_rows(tile_hot[...], y[...])

        for z in range(slices):
            for t in range(detectors):
                moved = x[t * local:(t + 1) * local, z * LANES:(z + 1) * LANES]
                at = (slice(z * local, (z + 1) * local), slice(t * LANES, (t + 1) * LANES))
                out_ref[at] = 2.0 * moved - cur[at]
        for k in range(chunks):
            own[k] = out_ref[rows_of(k), :].astype(BF)
        out_ref[...] = 2.0 * cur[...] - out_ref[...]
        pl.semaphore_wait(ready.at[0], 2)

    @pl.when(agent != 0)
    def _():
        barrier = pltpu.get_barrier_semaphore()

        @pl.when(agent != 1)
        def _():
            pl.semaphore_signal(barrier, inc=1, device_id=(neighbour, me), device_id_type=MESH)

        @pl.when(agent != 2)
        def _():
            pl.semaphore_signal(barrier, inc=1, device_id=(opposite, me), device_id_type=MESH)

        for k in range(chunks):
            own[k] = reflect_ref[rows_of(k), :].astype(BF)
        state.wait()
        out_ref[...] = 2.0 * cur[...] - reflect_ref[...]
        pl.semaphore_wait(barrier, 2)

        @pl.when(agent != 3)
        def _():
            pl.semaphore_signal(ready.at[0], inc=1, device_id=(0, me), device_id_type=MESH)

    def add(k, others):
        out_ref[rows_of(k), :] = out_ref[rows_of(k), :] + others

    @pl.when(agent < 2)
    def _():
        for k in range(chunks):
            to_across(own, k).start()
            to_beside(k).start()
        for k in range(chunks):
            to_beside(k).wait_recv()
            to_across(own, k).wait_recv()
            add(k, beside[k].astype(F32) + across[k].astype(F32))
        for k in range(chunks):
            to_across(own, k).wait_send()
            to_beside(k).wait_send()

    @pl.when(agent >= 2)
    def _():
        for k in range(chunks):
            to_beside(k).start()
        for k in range(chunks):
            to_beside(k).wait_recv()
            pair[k] = (own[k].astype(F32) + beside[k].astype(F32)).astype(BF)
            to_across(pair, k).start()
        for k in range(chunks):
            to_across(pair, k).wait_recv()
            to_onward(k).start()
            add(k, beside[k].astype(F32) + across[k].astype(F32))
        for k in range(chunks):
            to_onward(k).wait_recv()
            add(k, onward[k].astype(F32))
        for k in range(chunks):
            to_beside(k).wait_send()
            to_across(pair, k).wait_send()
            to_onward(k).wait_send()


def idle_kernel(out_ref):
    pass


def join(angle, detector, tile, sinogram, reflect, current, blocks, count):
    slices, local, columns = current.shape
    rays_here = sinogram.shape[0]
    ray_total = rays_here * count
    tiles_here = columns // LANES * local
    blocks_here = blocks.shape[0]
    width = slices * LANES
    rows = slices * local
    chunks = max(1, rows // 32)
    chunk = (chunks, rows // chunks, columns)
    vmem = pl.BlockSpec(memory_space=pltpu.VMEM)
    anywhere = pl.BlockSpec(memory_space=pl.ANY)
    out = pl.pallas_call(
        functools.partial(join_kernel, (count, slices)),
        out_shape=pltpu.VMEM((rows, columns), F32),
        in_specs=[vmem] * 5 + [anywhere] * 2,
        out_specs=vmem,
        scratch_shapes=[
            pltpu.VMEM(blocks.shape, BF),
            pltpu.VMEM((rows, columns), F32),
            pltpu.VMEM((ray_total, blocks_here), BF),
            pltpu.VMEM((blocks_here, ray_total), BF),
            pltpu.VMEM((tiles_here, blocks_here), BF),
            pltpu.VMEM((blocks_here, tiles_here), BF),
            pltpu.VMEM((tiles_here, width), F32),
            pltpu.VMEM((blocks_here, width), F32),
            pltpu.VMEM((blocks_here, width), F32),
            pltpu.VMEM((ray_total, width), F32),
            pltpu.VMEM((DATA_STEPS, count, rays_here, width), BF),
            pltpu.VMEM((DATA_STEPS, count, rays_here, width), BF),
            pltpu.VMEM((DATA_STEPS, rays_here, width), BF),
            pltpu.VMEM((DATA_STEPS, count, rays_here, width), BF),
        ]
        + [pltpu.VMEM(chunk, BF)] * 5
        + [pltpu.SemaphoreType.DMA((1,)), pltpu.SemaphoreType.DMA((blocks_here // CHUNK,))]
        + [pltpu.SemaphoreType.DMA((DATA_STEPS, count))] * 4
        + [pltpu.SemaphoreType.REGULAR((1,))]
        + [pltpu.SemaphoreType.DMA((chunks,))] * 6,
        compiler_params=pltpu.CompilerParams(
            collective_id=0, has_side_effects=True, vmem_limit_bytes=58 * 1024 * 1024
        ),
        name="join_agents",
    )(
        angle.reshape(1, -1), detector.reshape(1, -1), tile.reshape(1, -1),
        sinogram.reshape(rays_here * slices, LANES), reflect.reshape(rows, columns),
        current.reshape(rows, columns), blocks,
    )
    return out.reshape(current.shape)


def per_device(
    states,
    sinogram,
    blocks,
    block_angle,
    block_detector,
    block_tile,
    conv_first,
    conv_hidden,
    conv_last,
):
    current = states[0]
    agent_place = lax.axis_index("agent")
    halo = conv_hidden.shape[1] + 2
    filters = (conv_first, conv_hidden, conv_last)
    edges = halo_exchange(current, halo)

    def data_only():
        return pl.pallas_call(
            idle_kernel,
            out_shape=jax.ShapeDtypeStruct(current.shape, F32),
            out_specs=pl.BlockSpec(memory_space=pl.ANY),
            name="idle",
        )()

    def axial_only():
        return axial_reflect(edges, current, *filters, halo)

    def sagittal_only():
        return plane_call(1, edges, current, *filters, halo, 1)

    def coronal_only():
        return coronal_reflect(current, *filters)

    reflect = lax.switch(agent_place, [data_only, axial_only, sagittal_only, coronal_only])
    joined = join(
        block_angle, block_detector, block_tile, sinogram, reflect, current, blocks, lax.axis_size("tile")
    )
    return (0.25 * joined)[None]


def solution(mesh):
    placed = (
        P("agent", None, "tile", None),
        P("tile", None, None),
        P("tile", None, None),
        P("tile"),
        P("tile"),
        P("tile"),
        P(),
        P(),
        P(),
    )
    return jax.shard_map(
        per_device,
        mesh=mesh,
        in_specs=placed,
        out_specs=P("agent", None, "tile", None),
        check_vma=False,
    )
```

```python
import functools

import jax
import jax.numpy as jnp
from jax import lax
from jax.experimental import pallas as pl
from jax.experimental.pallas import tpu as pltpu
from jax.sharding import PartitionSpec as P

DATA_STEPS = 2
MESH = pl.DeviceIdType.MESH
LANES = 128
STRIPS = 16
CHUNK = 64
SPAN = 256
BF = jnp.bfloat16
F32 = jnp.float32
NATURAL = (0, 1, 2, 3)
EVEN_ORDER = (0, 1, 2, 3)
ODD_ORDER = (1, 0, 3, 2)


def main_cells(offset):
    order = EVEN_ORDER if offset % 2 else ODD_ORDER
    return [(offset, column) for column in order]

def edge_cells(offset):
    return [(offset + 1, 4), (offset, 4), (offset, -1), (offset + 1, -1)]

def window_cells(rows):
    tiles = [main_cells(a) for a in range(rows + 2)]
    return tiles + [edge_cells(a) for a in range(0, rows + 2, 2)]

def spread_lanes(w):
    return jnp.concatenate([w] * (LANES // w.shape[-1]), axis=-1)

def lane_iota(rows):
    return lax.broadcasted_iota(jnp.int32, (rows, LANES), 1)

def slot_mix(rows, taps, column_in, order, width):
    slot = lane_iota(rows) // width
    mixed = jnp.zeros((rows, LANES), F32)
    for place, column in enumerate(order):
        tap = column_in - column + 1
        if 0 <= tap < 3:
            mixed = jnp.where(slot == place, taps[tap], mixed)
    return mixed

def build_first(w_ref, o, w1):
    for k in range(6):
        for half in range(2):
            order = ODD_ORDER if half else EVEN_ORDER
            mixes = []
            for ti in range(3):
                taps = [jnp.broadcast_to(spread_lanes(w_ref[o, ti, tj:tj+1, :].astype(F32)), (16, LANES)) for tj in range(3)]
                mixes.append(slot_mix(16, taps, k - 1, order, 32))
            row = lax.broadcasted_iota(jnp.int32, (16, LANES), 0)
            for t in range(4):
                value = jnp.zeros((16, LANES), F32)
                for ti in range(3):
                    value = jnp.where(row == 2 * t + half + ti, mixes[ti], value)
                at = t * 2 * LANES + half * LANES
                w1[k * 16:(k + 1) * 16, at:at + LANES] = value.astype(BF)

def build_hidden(w_ref, o, layer, wh):
    wide = [[spread_lanes(w_ref[o, layer, ti, tj].astype(F32)) for tj in range(3)] for ti in range(3)]
    inner = wide[0][0].shape[0]
    for n, tile in enumerate(window_cells(2)):
        for slot, (a, column) in enumerate(tile):
            at = n * LANES + slot * inner
            for half in range(2):
                ti = a - (half + 1) + 1
                if 0 <= ti < 3:
                    value = slot_mix(inner, wide[ti], column, ODD_ORDER if half else EVEN_ORDER, inner)
                else:
                    value = jnp.zeros((inner, LANES), F32)
                wh[layer, at:at + inner, half * LANES:(half + 1) * LANES] = value.astype(BF)

def column_of(row):
    inner = row.shape[1]
    r = lax.broadcasted_iota(jnp.int32, (inner, inner), 0)
    c = lax.broadcasted_iota(jnp.int32, (inner, inner), 1)
    picked = jnp.where(r == c, jnp.broadcast_to(row, (inner, inner)), 0.0)
    return jnp.broadcast_to(jnp.sum(picked, axis=1, keepdims=True), (inner, LANES))

def build_last(w_ref, o, wl):
    taps = [[column_of(w_ref[o, ti, tj:tj+1, :].astype(F32)) for tj in range(3)] for ti in range(3)]
    inner = taps[0][0].shape[0]
    lane = lane_iota(inner)
    row8 = lane % 8
    zero = jnp.zeros((inner, LANES), F32)
    rows = []
    for a in range(10):
        line = []
        for tj in range(3):
            value = zero
            for ti in range(3):
                if 0 <= a - ti < 8:
                    value = jnp.where(row8 == a - ti, taps[ti][tj], value)
            line.append(value)
        rows.append(line)
    for n, tile in enumerate(window_cells(8)):
        for slot, (a, column) in enumerate(tile):
            at = n * LANES + slot * inner
            wl[at:at + inner, :] = slot_mix(inner, rows[a], column, EVEN_ORDER, LANES // 4).astype(BF)


def axial_kernel(plan, edges_ref, cur_ref, cf_ref, ch_ref, cl_ref, out_ref, main, edge, w1, wh, wl, raw, xs, place, back, gathered_out):
    halo, chunk = plan
    slices, local, columns = cur_ref.shape
    rows = local + 2 * halo
    stored = rows + 8
    groups = columns // 4
    per = groups // STRIPS
    span = slices * groups
    layers = ch_ref.shape[1]
    tile = lax.axis_index("tile")
    at_start = tile == 0
    at_end = tile == lax.axis_size("tile") - 1
    fill_rows(raw, edges_ref, cur_ref, stored, halo)

    build_first(cf_ref, 0, w1)
    for layer in range(layers):
        build_hidden(ch_ref, 0, layer, wh)
    build_last(cl_ref, 0, wl)

    col = lax.broadcasted_iota(jnp.int32, (columns, groups), 0)
    m = lax.broadcasted_iota(jnp.int32, (columns, groups), 1)
    first_col = 4 * ((m % STRIPS) * per + m // STRIPS)
    for k in range(6):
        place[:, k * groups:(k + 1) * groups] = jnp.where(col == first_col + (k - 1), 1.0, 0.0).astype(BF)
    m = lax.broadcasted_iota(jnp.int32, (groups, columns), 0)
    col = lax.broadcasted_iota(jnp.int32, (groups, columns), 1)
    first_col = 4 * ((m % STRIPS) * per + m // STRIPS)
    for k in range(4):
        back[k * groups:(k + 1) * groups, :] = jnp.where(col == first_col + k, 1.0, 0.0).astype(BF)
    xs[...] = jnp.dot(raw[...].astype(BF), place[...], preferred_element_type=F32)

    slot = lane_iota(STRIPS) // (LANES // 4)
    even_slots = (slot == 0) | (slot == 3)
    right_slots = slot < 2
    strip = lax.broadcasted_iota(jnp.int32, (STRIPS, LANES), 0)
    zero_tile = jnp.zeros((slices, per, STRIPS, LANES), BF)

    for side in range(2):
        for r in (0, 1, 2, rows - 1, rows, rows + 1):
            main[side, r] = zero_tile
        for e in (0, 1, rows // 2 - 1, rows // 2):
            edge[side, e] = zero_tile

    def put_edge(side, e, odd_row, even_row):
        v = jnp.where(even_slots, even_row, odd_row)
        for z in range(slices):
            for i in range(per):
                if i + 1 < per:
                    right = v[z, i + 1]
                else:
                    right = jnp.where(strip == STRIPS - 1, 0.0, pltpu.roll(v[z, 0], STRIPS - 1, 0))
                if i > 0:
                    left = v[z, i - 1]
                else:
                    left = jnp.where(strip == 0, 0.0, pltpu.roll(v[z, per - 1], 1, 0))
                edge[side, e, z, i] = jnp.where(right_slots, right, left).astype(BF)

    def put_pairs(side, pair, count, y):
        before = main[side, 2 * pair].astype(F32)
        for t in range(count):
            row = 2 * (pair + t)
            outside = (at_start & (row < halo)) | (at_end & (row >= rows - halo))
            v = jnp.maximum(y(t), 0.0) * jnp.where(outside, 0.0, 1.0)
            even_row = v[:, :LANES].reshape(slices, per, STRIPS, LANES)
            odd_row = v[:, LANES:].reshape(slices, per, STRIPS, LANES)
            main[side, row + 1] = even_row.astype(BF)
            main[side, row + 2] = odd_row.astype(BF)
            put_edge(side, pair + t, before, even_row)
            before = odd_row

    def first_step(c, carry):
        parts = []
        for z in range(slices):
            at = pl.ds(pl.multiple_of(z * stored + 8 * c, 8), 16)
            parts.append(jnp.concatenate([xs[at, k * groups:(k + 1) * groups] for k in range(6)], axis=0).astype(BF))
        x = jnp.concatenate(parts, axis=1)
        y = lax.dot_general(x, w1[...], (((0,), (0,)), ((), ())), preferred_element_type=F32)
        put_pairs(0, 4 * c, 4, lambda t: y[:, t * 2 * LANES:(t + 1) * 2 * LANES])
        return carry

    lax.fori_loop(0, rows // 8, first_step, 0)

    def window(side, pair, out_rows):
        parts = [main[side, 2 * pair + a].reshape(span, LANES) for a in range(out_rows + 2)]
        parts += [edge[side, pair + e].reshape(span, LANES) for e in range(out_rows // 2 + 1)]
        return jnp.concatenate(parts, axis=1)

    pairs = rows // 2 - 2
    for layer in range(layers):
        source, target = layer % 2, (layer + 1) % 2

        def hidden_step(c, carry):
            pair = 1 + c * chunk
            x = jnp.concatenate([window(source, pair + t, 2) for t in range(chunk)], axis=0)
            y = jnp.dot(x, wh[layer], preferred_element_type=F32)
            put_pairs(target, pair, chunk, lambda t: y[t * span:(t + 1) * span])
            return carry

        lax.fori_loop(0, pairs // chunk, hidden_step, 0)
        end = rows // 2 - 1
        put_edge(target, end, main[target, 2 * end].astype(F32), jnp.zeros((slices, per, STRIPS, LANES), F32))

    eighths = local // 8
    quad = (lane_iota(span) // 8) % 4

    def last_step(q, carry):
        x = window(layers % 2, halo // 2 + 4 * q, 8)
        y = jnp.dot(x, wl[...], preferred_element_type=F32)
        gathered_out[q // 4] = jnp.where(quad == q % 4, y, gathered_out[q // 4])
        return carry

    gathered_out[...] = jnp.zeros_like(gathered_out)
    lax.fori_loop(0, eighths, last_step, 0)

    for big in range(gathered_out.shape[0]):
        height = min(32, local - 32 * big)
        turned = [gathered_out[big, z * groups:(z + 1) * groups, :].T for z in range(slices)]
        lines = [jnp.concatenate([turned[z][k * 32:(k + 1) * 32] for k in range(4)], axis=1) for z in range(slices)]
        values = jnp.concatenate(lines, axis=0)
        high = values.astype(BF)
        low = (values - high.astype(F32)).astype(BF)
        net = jnp.dot(high, back[...], preferred_element_type=F32) + jnp.dot(low, back[...], preferred_element_type=F32)
        for z in range(slices):
            at = pl.ds(32 * big, height)
            out_ref[z, at, :] = cur_ref[z, at, :] - 2.0 * net[z * 32:z * 32 + height]

def axial_reflect(edges, current, cf, ch, cl, halo):
    slices, local, columns = current.shape
    rows = local + 2 * halo
    groups = columns // 4
    per = groups // STRIPS
    stored = rows + 8
    whole = pl.BlockSpec(memory_space=pltpu.VMEM)
    return pl.pallas_call(
        functools.partial(axial_kernel, (halo, 2)),
        out_shape=jax.ShapeDtypeStruct(current.shape, F32),
        in_specs=[whole] * 5,
        out_specs=whole,
        scratch_shapes=[
            pltpu.VMEM((2, rows + 2, slices, per, STRIPS, LANES), BF),
            pltpu.VMEM((2, rows // 2 + 1, slices, per, STRIPS, LANES), BF),
            pltpu.VMEM((96, 8 * LANES), BF),
            pltpu.VMEM((ch.shape[1], 6 * LANES, 2 * LANES), BF),
            pltpu.VMEM((15 * LANES, LANES), BF),
            pltpu.VMEM((slices * stored, columns), F32),
            pltpu.VMEM((slices * stored, 6 * groups), F32),
            pltpu.VMEM((columns, 6 * groups), BF),
            pltpu.VMEM((4 * groups, columns), BF),
            pltpu.VMEM((-(-local // 32), slices * groups, LANES), F32),
        ],
        compiler_params=pltpu.CompilerParams(vmem_limit_bytes=60 * 1024 * 1024),
        name="net_axial",
    )(edges, current, cf, ch, cl)


def fill_rows(raw, edges_ref, cur_ref, stored, halo):
    slices, local, columns = cur_ref.shape
    zero = jnp.zeros((1, columns), F32)
    tail = jnp.zeros((stored - 1 - local - 2 * halo, columns), F32)
    for z in range(slices):
        above = edges_ref[0, z * halo:(z + 1) * halo, :].astype(F32)
        below = edges_ref[1, z * halo:(z + 1) * halo, :].astype(F32)
        raw[z * stored:(z + 1) * stored, :] = jnp.concatenate([zero, above, cur_ref[z], below, tail], axis=0)


def build_first_plane(w_ref, o, w1):
    row = lax.broadcasted_iota(jnp.int32, (16, LANES), 0)
    for z in range(4):
        mixes = []
        for tj in range(3):
            taps = [jnp.broadcast_to(spread_lanes(w_ref[o, ti, tj:tj+1, :].astype(F32)), (16, LANES)) for ti in range(3)]
            mixes.append(slot_mix(16, taps, z, NATURAL, 32))
        for t in range(8):
            value = jnp.zeros((16, LANES), F32)
            for tj in range(3):
                value = jnp.where(row == t + tj, mixes[tj], value)
            w1[z * 16:(z + 1) * 16, t * LANES:(t + 1) * LANES] = value.astype(BF)

def build_hidden_plane(w_ref, o, layer, wh):
    wide = [[spread_lanes(w_ref[o, layer, ti, tj].astype(F32)) for ti in range(3)] for tj in range(3)]
    inner = wide[0][0].shape[0]
    for a in range(4):
        for z in range(4):
            at = a * LANES + z * inner
            for half in range(2):
                if 0 <= a - half < 3:
                    value = slot_mix(inner, wide[a - half], z, NATURAL, inner)
                else:
                    value = jnp.zeros((inner, LANES), F32)
                wh[layer, at:at + inner, half * LANES:(half + 1) * LANES] = value.astype(BF)

def build_last_plane(w_ref, o, wl):
    taps = [[column_of(w_ref[o, ti, tj:tj+1, :].astype(F32)) for ti in range(3)] for tj in range(3)]
    inner = taps[0][0].shape[0]
    row8 = lane_iota(inner) % 8
    zero = jnp.zeros((inner, LANES), F32)
    for a in range(10):
        line = []
        for ti in range(3):
            value = zero
            for tj in range(3):
                if 0 <= a - tj < 8:
                    value = jnp.where(row8 == a - tj, taps[tj][ti], value)
            line.append(value)
        for z in range(4):
            at = a * LANES + z * inner
            wl[at:at + inner, :] = slot_mix(inner, line, z, NATURAL, LANES // 4).astype(BF)


def plane_kernel(plan, x_ref, cur_ref, cf_ref, ch_ref, cl_ref, out_ref, main, w1, wh, wl, xs, gathered_out):
    o, halo, chunk, strips = plan
    slices, local, span = out_ref.shape
    rows = local + 2 * halo
    stored = rows + 8
    layers = ch_ref.shape[1]
    if halo:
        tile = lax.axis_index("tile")
        at_start = tile == 0
        at_end = tile == lax.axis_size("tile") - 1

    build_first_plane(cf_ref, o, w1)
    for layer in range(layers):
        build_hidden_plane(ch_ref, o, layer, wh)
    build_last_plane(cl_ref, o, wl)
    if halo:
        fill_rows(xs, x_ref, cur_ref, stored, halo)
    else:
        xs[...] = x_ref[...].astype(F32)
    for side in range(2):
        for r in (0, rows + 1):
            main[side, r] = jnp.zeros((span, LANES), BF)

    def put_pairs(side, pair, count, y):
        for t in range(count):
            row = 2 * (pair + t)
            v = jnp.maximum(y(t), 0.0)
            if halo:
                outside = (at_start & (row < halo)) | (at_end & (row >= rows - halo))
                v = v * jnp.where(outside, 0.0, 1.0)
            main[side, row + 1] = v[:, :LANES].astype(BF)
            main[side, row + 2] = v[:, LANES:].astype(BF)

    def ends(side):
        if strips > 1:
            step = span // strips
            main[side, 0, step:span] = main[side, rows, 0:span - step]
            main[side, rows + 1, 0:span - step] = main[side, 1, step:span]

    def first_step(c, carry):
        parts = [xs[pl.ds(pl.multiple_of(z * stored + 8 * c, 8), 16)] for z in range(slices)]
        x = jnp.concatenate(parts, axis=0).astype(BF)
        y = lax.dot_general(x, w1[...], (((0,), (0,)), ((), ())), preferred_element_type=F32)
        put_pairs(0, 4 * c, 4, lambda t: y[:, t * 2 * LANES:(t + 1) * 2 * LANES])
        return carry

    lax.fori_loop(0, rows // 8, first_step, 0)
    ends(0)

    for layer in range(layers):
        source, target = layer % 2, (layer + 1) % 2

        def hidden_step(c, carry):
            pair = c * chunk
            tiles = [main[source, 2 * pair + a] for a in range(2 * chunk + 2)]
            x = jnp.concatenate([jnp.concatenate(tiles[2 * t:2 * t + 4], axis=1) for t in range(chunk)], axis=0)
            y = jnp.dot(x, wh[layer], preferred_element_type=F32)
            put_pairs(target, pair, chunk, lambda t: y[t * span:(t + 1) * span])
            return carry

        lax.fori_loop(0, rows // 2 // chunk, hidden_step, 0)
        ends(target)

    quad = (lane_iota(span) // 8) % 4

    def last_step(q, carry):
        x = jnp.concatenate([main[layers % 2, halo + 8 * q + a] for a in range(10)], axis=1)
        y = jnp.dot(x, wl[...], preferred_element_type=F32)
        gathered_out[q // 4] = jnp.where(quad == q % 4, y, gathered_out[q // 4])
        return carry

    gathered_out[...] = jnp.zeros_like(gathered_out)
    lax.fori_loop(0, local // 8, last_step, 0)
    for big in range(gathered_out.shape[0]):
        height = min(32, local - 32 * big)
        net = gathered_out[big].T
        for z in range(slices):
            at = pl.ds(32 * big, height)
            out_ref[z, at, :] = cur_ref[z, at, :] - 2.0 * net[z * 32:z * 32 + height]

def plane_call(o, x, current, cf, ch, cl, halo, strips):
    slices, local, span = current.shape
    rows = local + 2 * halo
    whole = pl.BlockSpec(memory_space=pltpu.VMEM)
    return pl.pallas_call(
        functools.partial(plane_kernel, (o, halo, 4, strips)),
        out_shape=jax.ShapeDtypeStruct(current.shape, F32),
        in_specs=[whole] * 5, out_specs=whole,
        scratch_shapes=[
            pltpu.VMEM((2, rows + 2, span, LANES), BF),
            pltpu.VMEM((64, 8 * LANES), BF),
            pltpu.VMEM((ch.shape[1], 4 * LANES, 2 * LANES), BF),
            pltpu.VMEM((10 * LANES, LANES), BF),
            pltpu.VMEM((slices * (rows + 8), span), F32),
            pltpu.VMEM((-(-local // 32), span, LANES), F32),
        ],
        compiler_params=pltpu.CompilerParams(vmem_limit_bytes=60 * 1024 * 1024),
        name="net_sagittal" if halo else "net_coronal",
    )(x, current, cf, ch, cl)

def coronal_reflect(current, cf, ch, cl):
    slices, local, columns = current.shape
    strips = columns // local
    turned = jnp.transpose(current.reshape(slices, local, strips, local), (0, 3, 2, 1))
    t = turned.astype(BF)
    none = jnp.zeros((slices, 1, 1, local), BF)
    before = jnp.concatenate([none, t[:, -1:, :-1]], axis=2)
    after = jnp.concatenate([t[:, :1, 1:], none], axis=2)
    rest = jnp.zeros((slices, 6, strips, local), BF)
    x = jnp.concatenate([before, t, after, rest], axis=1)
    x = x.reshape(-1, columns)
    out = plane_call(2, x, turned.reshape(slices, local, columns), cf, ch, cl, 0, strips)
    return jnp.transpose(out.reshape(slices, local, strips, local), (0, 3, 2, 1)).reshape(current.shape)

def halo_kernel(halo, cur_hbm, out_ref, edge, sent, load, send, recv):
    agent = lax.axis_index("agent")
    tile = lax.axis_index("tile")
    last = lax.axis_size("tile") - 1
    slices, local, columns = cur_hbm.shape
    rows = edge.shape[2]
    active = (agent == 1) | (agent == 2)

    def copy(side, peer):
        return pltpu.make_async_remote_copy(
            src_ref=sent.at[side],
            dst_ref=out_ref.at[1 - side],
            send_sem=send.at[side],
            recv_sem=recv.at[1 - side],
            device_id=(agent, peer),
            device_id_type=MESH,
        )

    @pl.when(active)
    def _():
        barrier = pltpu.get_barrier_semaphore()

        @pl.when(tile > 0)
        def _():
            pl.semaphore_signal(barrier, inc=1, device_id=(agent, tile - 1), device_id_type=MESH)

        @pl.when(tile < last)
        def _():
            pl.semaphore_signal(barrier, inc=1, device_id=(agent, tile + 1), device_id_type=MESH)

        loads = [
            pltpu.make_async_copy(cur_hbm.at[:, pl.ds(0, rows)], edge.at[0], load.at[0]),
            pltpu.make_async_copy(cur_hbm.at[:, pl.ds(local - rows, rows)], edge.at[1], load.at[1]),
        ]
        for item in loads:
            item.start()
        for item in loads:
            item.wait()
        for side in range(2):
            first = 0 if side == 0 else rows - halo
            parts = [edge[side, z, first:first + halo, :] for z in range(slices)]
            sent[side] = jnp.concatenate(parts, axis=0).astype(BF)

        pl.semaphore_wait(barrier, jnp.where(tile > 0, 1, 0) + jnp.where(tile < last, 1, 0))

        @pl.when(tile > 0)
        def _():
            copy(0, tile - 1).start()

        @pl.when(tile < last)
        def _():
            copy(1, tile + 1).start()

        @pl.when(tile == 0)
        def _():
            out_ref[0] = jnp.zeros(out_ref.shape[1:], BF)

        @pl.when(tile == last)
        def _():
            out_ref[1] = jnp.zeros(out_ref.shape[1:], BF)

        @pl.when(tile > 0)
        def _():
            copy(1, tile - 1).wait_recv()

        @pl.when(tile < last)
        def _():
            copy(0, tile + 1).wait_recv()

        @pl.when(tile > 0)
        def _():
            copy(0, tile - 1).wait_send()

        @pl.when(tile < last)
        def _():
            copy(1, tile + 1).wait_send()


def halo_exchange(current, halo):
    slices, local, columns = current.shape
    return pl.pallas_call(
        functools.partial(halo_kernel, halo),
        out_shape=jax.ShapeDtypeStruct((2, slices * halo, columns), BF),
        in_specs=[pl.BlockSpec(memory_space=pl.ANY)],
        out_specs=pl.BlockSpec(memory_space=pltpu.VMEM),
        scratch_shapes=[
            pltpu.VMEM((2, slices, 8, columns), F32),
            pltpu.VMEM((2, slices * halo, columns), BF),
            pltpu.SemaphoreType.DMA((2,)),
            pltpu.SemaphoreType.DMA((2,)),
            pltpu.SemaphoreType.DMA((2,)),
        ],
        compiler_params=pltpu.CompilerParams(collective_id=2, has_side_effects=True),
        name="halo_exchange",
    )(current)


def swap_bits(me, d):
    peer, bit = me, 1
    while bit <= d:
        if d & bit:
            peer = peer + bit * (1 - 2 * ((me // bit) % 2))
        bit *= 2
    return peer


def block_copy(blocks_hbm, held, sems, i):
    at = pl.ds(i * CHUNK, CHUNK)
    return pltpu.make_async_copy(blocks_hbm.at[at], held.at[at], sems.at[i])


def block_step(held, picked, y, slices, transposed, u):
    row = lax.broadcasted_iota(jnp.int32, (8, LANES), 0)
    at = pl.ds(pl.multiple_of(8 * u, 8), 8)
    p = [picked[at, z * LANES:(z + 1) * LANES] for z in range(slices)]
    halves = []
    for t in range(2):
        sides = []
        for side in range(2):
            mask = row // 2 == 2 * t + side
            sides.append(jnp.concatenate([jnp.where(mask, v, 0.0) for v in p], axis=0))
        lhs = jnp.concatenate(sides, axis=1).astype(BF)
        m = [held[8 * u + 4 * t + j] for j in range(4)]
        if transposed:
            top, bottom = jnp.concatenate([m[0], m[2]], axis=1), jnp.concatenate([m[1], m[3]], axis=1)
            dims = (((1,), (1,)), ((), ()))
        else:
            top, bottom = jnp.concatenate([m[0], m[1]], axis=1), jnp.concatenate([m[2], m[3]], axis=1)
            dims = (((1,), (0,)), ((), ()))
        rhs = jnp.concatenate([top, bottom], axis=0)
        halves.append(lax.dot_general(lhs, rhs, dims, preferred_element_type=F32))
    for z in range(slices):
        a, b = (h[8 * z:8 * z + 8] for h in halves)
        low = jnp.where(row < 4, a[:, :LANES], b[:, :LANES])
        high = jnp.where(row < 4, a[:, LANES:], b[:, LANES:])
        y[at, z * LANES:(z + 1) * LANES] = jnp.where(row % 2 == 0, low, high)


def block_sweep(blocks_hbm, held, sems, picked, y, slices, transposed, waiting):
    span = min(SPAN, held.shape[0])

    def chunk(i, carry):
        for j in range(span // 8):
            if waiting and j % (CHUNK // 8) == 0:
                block_copy(blocks_hbm, held, sems, i * (span // CHUNK) + j // (CHUNK // 8)).wait()
            block_step(held, picked, y, slices, transposed, i * (span // 8) + j)
        return carry

    lax.fori_loop(0, held.shape[0] // span, chunk, 0)


def gather_rows(hot, source):
    return jnp.dot(hot, source, preferred_element_type=F32)


def scatter_rows(hot, y):
    high = y.astype(BF)
    low = (y - high.astype(F32)).astype(BF)
    return jnp.dot(
        jnp.concatenate([hot, hot], axis=1), jnp.concatenate([high, low], axis=0), preferred_element_type=F32
    )


def join_kernel(
    plan, angle_ref, detector_ref, tile_ref, sino_ref, reflect_ref, cur_hbm, blocks_hbm, out_ref,
    held, cur, ray_hot, ray_turned, tile_hot, tile_turned, x, y, picked, total, part, got, fresh, full,
    own, pair, beside, across, onward,
    load, sems, send1, recv1, send2, recv2, ready,
    send_beside, recv_beside, send_across, recv_across, send_onward, recv_onward,
):
    agent = lax.axis_index("agent")
    me = lax.axis_index("tile")
    count, slices = plan
    chunks, height, columns = own.shape
    local = chunks * height // slices
    detectors = columns // LANES
    rays_here = fresh.shape[1]
    ray_total = count * rays_here
    tiles_here = detectors * local
    blocks_here = held.shape[0]
    order = list(range(count - 1, 0, -1))
    core = agent % 2
    neighbour = agent + 1 - 2 * core
    opposite = (agent + 2) % 4
    state = pltpu.make_async_copy(cur_hbm, cur, load.at[0])
    state.start()

    def send(source, target, s, r, k, to):
        return pltpu.make_async_remote_copy(
            src_ref=source.at[k], dst_ref=target.at[k], send_sem=s.at[k], recv_sem=r.at[k],
            device_id=(to, me), device_id_type=MESH,
        )

    def to_beside(k):
        return send(own, beside, send_beside, recv_beside, k, neighbour)

    def to_across(source, k):
        return send(source, across, send_across, recv_across, k, opposite)

    def to_onward(k):
        return send(across, onward, send_onward, recv_onward, k, neighbour)

    def rows_of(k):
        return slice(k * height, (k + 1) * height)

    def part_copy(step, d):
        return pltpu.make_async_remote_copy(
            src_ref=part.at[step, swap_bits(me, d)],
            dst_ref=got.at[step, d],
            send_sem=send1.at[step, d],
            recv_sem=recv1.at[step, d],
            device_id=(agent, swap_bits(me, d)),
            device_id_type=MESH,
        )

    def rest_copy(step, d):
        return pltpu.make_async_remote_copy(
            src_ref=fresh.at[step],
            dst_ref=full.at[step, me],
            send_sem=send2.at[step, d],
            recv_sem=recv2.at[step, d],
            device_id=(agent, swap_bits(me, d)),
            device_id_type=MESH,
        )

    def exchange(step):
        for slot in range(count):
            part[step, slot] = total[slot * rays_here:(slot + 1) * rays_here, :].astype(BF)
        for d in order:
            part_copy(step, d).start()
        own = total[pl.ds(pl.multiple_of(me * rays_here, 8), rays_here), :]
        measured = [sino_ref[pl.ds(z, rays_here, stride=slices), :] for z in range(slices)]
        value = own - jnp.concatenate(measured, axis=1)
        for d in reversed(order):
            part_copy(step, d).wait_recv()
            value = value + got[step, d].astype(F32)
        fresh[step] = value.astype(BF)
        for d in order:
            rest_copy(step, d).start()
        full[step, me] = fresh[step]
        for d in order:
            rest_copy(step, d).wait_recv()
        for d in order:
            part_copy(step, d).wait_send()
            rest_copy(step, d).wait_send()
        return full[step].reshape(ray_total, slices * LANES)

    middle = chunks // 2

    def half_of(side):
        return range(side * middle, chunks if side else middle)

    def last_update(side):
        first, count_here = side * (slices // 2), slices // 2 if side == 0 else slices - slices // 2
        at = slice(first * LANES, (first + count_here) * LANES)
        moved = x[:, at] - 0.8 * scatter_rows(tile_hot[...], y[:, at])
        for z in range(count_here):
            for t in range(detectors):
                place = (slice((first + z) * local, (first + z + 1) * local), slice(t * LANES, (t + 1) * LANES))
                piece = moved[t * local:(t + 1) * local, z * LANES:(z + 1) * LANES]
                out_ref[place] = 2.0 * piece - cur[place]

    def finish(k, base, others):
        out_ref[rows_of(k), :] = 2.0 * cur[rows_of(k), :] - base[rows_of(k), :] + others

    def low_part(side, base):
        mine, rest = half_of(side), half_of(1 - side)
        for part_of in (rest, mine):
            if side == 0:
                last_update(0 if part_of is mine else 1)
                for k in part_of:
                    own[k] = out_ref[rows_of(k), :].astype(BF)
                if part_of is rest:
                    pl.semaphore_wait(ready.at[0], 2)
            for k in part_of:
                to_beside(k).start()
        for k in mine:
            to_beside(k).wait_recv()
            pair[k] = (own[k].astype(F32) + beside[k].astype(F32)).astype(BF)
            to_across(pair, k).start()
        for part_of in (mine, rest):
            for k in part_of:
                if part_of is rest:
                    to_beside(k).wait_recv()
                to_across(pair, k).wait_recv()
                finish(k, base, beside[k].astype(F32) + across[k].astype(F32))
        for k in range(chunks):
            to_beside(k).wait_send()
        for k in mine:
            to_across(pair, k).wait_send()

    def high_part(side):
        mine, rest = half_of(side), half_of(1 - side)
        for k in range(chunks):
            to_beside(k).start()
        for k in range(chunks):
            to_beside(k).wait_recv()
            pair[k] = (own[k].astype(F32) + beside[k].astype(F32)).astype(BF)
            to_across(pair, k).start()
        for k in mine:
            to_across(pair, k).wait_recv()
            to_onward(k).start()
            finish(k, reflect_ref, beside[k].astype(F32) + across[k].astype(F32))
        for k in rest:
            to_onward(k).wait_recv()
            finish(k, reflect_ref, beside[k].astype(F32) + onward[k].astype(F32))
        for k in range(chunks):
            to_beside(k).wait_send()
            to_across(pair, k).wait_send()
        for k in mine:
            to_onward(k).wait_send()

    @pl.when(agent == 0)
    def _():
        barrier = pltpu.get_barrier_semaphore()
        for d in order:
            pl.semaphore_signal(barrier, inc=1, device_id=(agent, swap_bits(me, d)), device_id_type=MESH)
        for peer in (neighbour, opposite):
            pl.semaphore_signal(barrier, inc=1, device_id=(peer, me), device_id_type=MESH)
        for i in range(blocks_here // CHUNK):
            block_copy(blocks_hbm, held, sems, i).start()

        hot_rows = lax.broadcasted_iota(jnp.int32, (ray_total, blocks_here), 0)
        ray = angle_ref[...] * detectors + detector_ref[...]
        hot = jnp.where(hot_rows == jnp.broadcast_to(ray, hot_rows.shape), 1.0, 0.0)
        ray_hot[...] = hot.astype(BF)
        ray_turned[...] = hot.T.astype(BF)
        hot_rows = lax.broadcasted_iota(jnp.int32, (tiles_here, blocks_here), 0)
        place = tile_ref[...]
        place = (place % detectors) * local + place // detectors
        hot = jnp.where(hot_rows == jnp.broadcast_to(place, hot_rows.shape), 1.0, 0.0)
        tile_hot[...] = hot.astype(BF)
        tile_turned[...] = hot.T.astype(BF)

        state.wait()
        for z in range(slices):
            for t in range(detectors):
                x[t * local:(t + 1) * local, z * LANES:(z + 1) * LANES] = cur[z * local:(z + 1) * local, t * LANES:(t + 1) * LANES]

        for step in range(DATA_STEPS):
            picked[...] = gather_rows(tile_turned[...], x[...].astype(BF))
            block_sweep(blocks_hbm, held, sems, picked, y, slices, True, step == 0)
            total[...] = scatter_rows(ray_hot[...], y[...])
            if step == 0:
                pl.semaphore_wait(barrier, count - 1)
            picked[...] = gather_rows(ray_turned[...], exchange(step))
            block_sweep(blocks_hbm, held, sems, picked, y, slices, False, False)
            if step < DATA_STEPS - 1:
                x[...] = x[...] - 0.8 * scatter_rows(tile_hot[...], y[...])

        low_part(0, out_ref)

    @pl.when(agent != 0)
    def _():
        barrier = pltpu.get_barrier_semaphore()

        @pl.when(agent != 1)
        def _():
            pl.semaphore_signal(barrier, inc=1, device_id=(neighbour, me), device_id_type=MESH)

        @pl.when(agent != 2)
        def _():
            pl.semaphore_signal(barrier, inc=1, device_id=(opposite, me), device_id_type=MESH)

        for k in range(chunks):
            own[k] = reflect_ref[rows_of(k), :].astype(BF)
        state.wait()
        pl.semaphore_wait(barrier, 2)

        @pl.when(agent != 3)
        def _():
            pl.semaphore_signal(ready.at[0], inc=1, device_id=(0, me), device_id_type=MESH)

        @pl.when(agent == 1)
        def _():
            low_part(1, reflect_ref)

        @pl.when(agent == 2)
        def _():
            high_part(0)

        @pl.when(agent == 3)
        def _():
            high_part(1)


def idle_kernel(out_ref):
    pass


def join(angle, detector, tile, sinogram, reflect, current, blocks, count):
    slices, local, columns = current.shape
    rays_here = sinogram.shape[0]
    ray_total = rays_here * count
    tiles_here = columns // LANES * local
    blocks_here = blocks.shape[0]
    width = slices * LANES
    rows = slices * local
    chunks = max(2, rows // 32)
    chunk = (chunks, rows // chunks, columns)
    vmem = pl.BlockSpec(memory_space=pltpu.VMEM)
    anywhere = pl.BlockSpec(memory_space=pl.ANY)
    out = pl.pallas_call(
        functools.partial(join_kernel, (count, slices)),
        out_shape=pltpu.VMEM((rows, columns), F32),
        in_specs=[vmem] * 5 + [anywhere] * 2,
        out_specs=vmem,
        scratch_shapes=[
            pltpu.VMEM(blocks.shape, BF),
            pltpu.VMEM((rows, columns), F32),
            pltpu.VMEM((ray_total, blocks_here), BF),
            pltpu.VMEM((blocks_here, ray_total), BF),
            pltpu.VMEM((tiles_here, blocks_here), BF),
            pltpu.VMEM((blocks_here, tiles_here), BF),
            pltpu.VMEM((tiles_here, width), F32),
            pltpu.VMEM((blocks_here, width), F32),
            pltpu.VMEM((blocks_here, width), F32),
            pltpu.VMEM((ray_total, width), F32),
            pltpu.VMEM((DATA_STEPS, count, rays_here, width), BF),
            pltpu.VMEM((DATA_STEPS, count, rays_here, width), BF),
            pltpu.VMEM((DATA_STEPS, rays_here, width), BF),
            pltpu.VMEM((DATA_STEPS, count, rays_here, width), BF),
        ]
        + [pltpu.VMEM(chunk, BF)] * 5
        + [pltpu.SemaphoreType.DMA((1,)), pltpu.SemaphoreType.DMA((blocks_here // CHUNK,))]
        + [pltpu.SemaphoreType.DMA((DATA_STEPS, count))] * 4
        + [pltpu.SemaphoreType.REGULAR((1,))]
        + [pltpu.SemaphoreType.DMA((chunks,))] * 6,
        compiler_params=pltpu.CompilerParams(
            collective_id=0, has_side_effects=True, vmem_limit_bytes=58 * 1024 * 1024
        ),
        name="join_agents",
    )(
        angle.reshape(1, -1), detector.reshape(1, -1), tile.reshape(1, -1),
        sinogram.reshape(rays_here * slices, LANES), reflect.reshape(rows, columns),
        current.reshape(rows, columns), blocks,
    )
    return out.reshape(current.shape)


def per_device(
    states,
    sinogram,
    blocks,
    block_angle,
    block_detector,
    block_tile,
    conv_first,
    conv_hidden,
    conv_last,
):
    current = states[0]
    agent_place = lax.axis_index("agent")
    halo = conv_hidden.shape[1] + 2
    filters = (conv_first, conv_hidden, conv_last)
    edges = halo_exchange(current, halo)

    def data_only():
        return pl.pallas_call(
            idle_kernel,
            out_shape=jax.ShapeDtypeStruct(current.shape, F32),
            out_specs=pl.BlockSpec(memory_space=pl.ANY),
            name="idle",
        )()

    def axial_only():
        return axial_reflect(edges, current, *filters, halo)

    def sagittal_only():
        return plane_call(1, edges, current, *filters, halo, 1)

    def coronal_only():
        return coronal_reflect(current, *filters)

    reflect = lax.switch(agent_place, [data_only, axial_only, sagittal_only, coronal_only])
    joined = join(
        block_angle, block_detector, block_tile, sinogram, reflect, current, blocks, lax.axis_size("tile")
    )
    return (0.25 * joined)[None]


def solution(mesh):
    placed = (
        P("agent", None, "tile", None),
        P("tile", None, None),
        P("tile", None, None),
        P("tile"),
        P("tile"),
        P("tile"),
        P(),
        P(),
        P(),
    )
    return jax.shard_map(
        per_device,
        mesh=mesh,
        in_specs=placed,
        out_specs=P("agent", None, "tile", None),
        check_vma=False,
    )
```

```python
import functools

import jax
import jax.numpy as jnp
from jax import lax
from jax.experimental import pallas as pl
from jax.experimental.pallas import tpu as pltpu
from jax.sharding import PartitionSpec as P

DATA_STEPS = 2
MESH = pl.DeviceIdType.MESH
LANES = 128
STRIPS = 16
CHUNK = 64
DEPTH = 2
BF = jnp.bfloat16
F32 = jnp.float32
NATURAL = (0, 1, 2, 3)
EVEN_ORDER = (0, 1, 2, 3)
ODD_ORDER = (1, 0, 3, 2)


def main_cells(offset):
    order = EVEN_ORDER if offset % 2 else ODD_ORDER
    return [(offset, column) for column in order]

def edge_cells(offset):
    return [(offset + 1, 4), (offset, 4), (offset, -1), (offset + 1, -1)]

def window_cells(rows):
    tiles = [main_cells(a) for a in range(rows + 2)]
    return tiles + [edge_cells(a) for a in range(0, rows + 2, 2)]

def spread_lanes(w):
    return jnp.concatenate([w] * (LANES // w.shape[-1]), axis=-1)

def lane_iota(rows):
    return lax.broadcasted_iota(jnp.int32, (rows, LANES), 1)

def slot_mix(rows, taps, column_in, order, width):
    slot = lane_iota(rows) // width
    mixed = jnp.zeros((rows, LANES), F32)
    for place, column in enumerate(order):
        tap = column_in - column + 1
        if 0 <= tap < 3:
            mixed = jnp.where(slot == place, taps[tap], mixed)
    return mixed

def build_first(w_ref, o, w1):
    for k in range(6):
        for half in range(2):
            order = ODD_ORDER if half else EVEN_ORDER
            mixes = []
            for ti in range(3):
                taps = [jnp.broadcast_to(spread_lanes(w_ref[o, ti, tj:tj+1, :].astype(F32)), (16, LANES)) for tj in range(3)]
                mixes.append(slot_mix(16, taps, k - 1, order, 32))
            row = lax.broadcasted_iota(jnp.int32, (16, LANES), 0)
            for t in range(4):
                value = jnp.zeros((16, LANES), F32)
                for ti in range(3):
                    value = jnp.where(row == 2 * t + half + ti, mixes[ti], value)
                at = t * 2 * LANES + half * LANES
                w1[k * 16:(k + 1) * 16, at:at + LANES] = value.astype(BF)

def build_hidden(w_ref, o, layer, wh):
    wide = [[spread_lanes(w_ref[o, layer, ti, tj].astype(F32)) for tj in range(3)] for ti in range(3)]
    inner = wide[0][0].shape[0]
    for n, tile in enumerate(window_cells(2)):
        for slot, (a, column) in enumerate(tile):
            at = n * LANES + slot * inner
            for half in range(2):
                ti = a - (half + 1) + 1
                if 0 <= ti < 3:
                    value = slot_mix(inner, wide[ti], column, ODD_ORDER if half else EVEN_ORDER, inner)
                else:
                    value = jnp.zeros((inner, LANES), F32)
                wh[layer, at:at + inner, half * LANES:(half + 1) * LANES] = value.astype(BF)

def column_of(row):
    inner = row.shape[1]
    r = lax.broadcasted_iota(jnp.int32, (inner, inner), 0)
    c = lax.broadcasted_iota(jnp.int32, (inner, inner), 1)
    picked = jnp.where(r == c, jnp.broadcast_to(row, (inner, inner)), 0.0)
    return jnp.broadcast_to(jnp.sum(picked, axis=1, keepdims=True), (inner, LANES))

def build_last(w_ref, o, wl):
    taps = [[column_of(w_ref[o, ti, tj:tj+1, :].astype(F32)) for tj in range(3)] for ti in range(3)]
    inner = taps[0][0].shape[0]
    lane = lane_iota(inner)
    row8 = lane % 8
    zero = jnp.zeros((inner, LANES), F32)
    rows = []
    for a in range(10):
        line = []
        for tj in range(3):
            value = zero
            for ti in range(3):
                if 0 <= a - ti < 8:
                    value = jnp.where(row8 == a - ti, taps[ti][tj], value)
            line.append(value)
        rows.append(line)
    for n, tile in enumerate(window_cells(8)):
        for slot, (a, column) in enumerate(tile):
            at = n * LANES + slot * inner
            wl[at:at + inner, :] = slot_mix(inner, rows[a], column, EVEN_ORDER, LANES // 4).astype(BF)


def axial_kernel(plan, edges_ref, cur_ref, cf_ref, ch_ref, cl_ref, out_ref, main, edge, w1, wh, wl, raw, xs, place, back, gathered_out):
    halo, chunk = plan
    slices, local, columns = cur_ref.shape
    rows = local + 2 * halo
    stored = rows + 8
    groups = columns // 4
    per = groups // STRIPS
    span = slices * groups
    layers = ch_ref.shape[1]
    tile = lax.axis_index("tile")
    at_start = tile == 0
    at_end = tile == lax.axis_size("tile") - 1
    fill_rows(raw, edges_ref, cur_ref, stored, halo)

    build_first(cf_ref, 0, w1)
    for layer in range(layers):
        build_hidden(ch_ref, 0, layer, wh)
    build_last(cl_ref, 0, wl)

    col = lax.broadcasted_iota(jnp.int32, (columns, groups), 0)
    m = lax.broadcasted_iota(jnp.int32, (columns, groups), 1)
    first_col = 4 * ((m % STRIPS) * per + m // STRIPS)
    for k in range(6):
        place[:, k * groups:(k + 1) * groups] = jnp.where(col == first_col + (k - 1), 1.0, 0.0).astype(BF)
    m = lax.broadcasted_iota(jnp.int32, (groups, columns), 0)
    col = lax.broadcasted_iota(jnp.int32, (groups, columns), 1)
    first_col = 4 * ((m % STRIPS) * per + m // STRIPS)
    for k in range(4):
        back[k * groups:(k + 1) * groups, :] = jnp.where(col == first_col + k, 1.0, 0.0).astype(BF)
    xs[...] = jnp.dot(raw[...].astype(BF), place[...], preferred_element_type=F32)

    slot = lane_iota(STRIPS) // (LANES // 4)
    even_slots = (slot == 0) | (slot == 3)
    right_slots = slot < 2
    strip = lax.broadcasted_iota(jnp.int32, (STRIPS, LANES), 0)
    zero_tile = jnp.zeros((slices, per, STRIPS, LANES), BF)

    for side in range(2):
        for r in (0, 1, 2, rows - 1, rows, rows + 1):
            main[side, r] = zero_tile
        for e in (0, 1, rows // 2 - 1, rows // 2):
            edge[side, e] = zero_tile

    def put_edge(side, e, odd_row, even_row):
        v = jnp.where(even_slots, even_row, odd_row)
        for z in range(slices):
            for i in range(per):
                if i + 1 < per:
                    right = v[z, i + 1]
                else:
                    right = jnp.where(strip == STRIPS - 1, 0.0, pltpu.roll(v[z, 0], STRIPS - 1, 0))
                if i > 0:
                    left = v[z, i - 1]
                else:
                    left = jnp.where(strip == 0, 0.0, pltpu.roll(v[z, per - 1], 1, 0))
                edge[side, e, z, i] = jnp.where(right_slots, right, left).astype(BF)

    def put_pairs(side, pair, count, y):
        before = main[side, 2 * pair].astype(F32)
        for t in range(count):
            row = 2 * (pair + t)
            v = jnp.maximum(y(t), 0.0)
            if row < halo:
                v = v * jnp.where(at_start, 0.0, 1.0)
            elif row >= rows - halo:
                v = v * jnp.where(at_end, 0.0, 1.0)
            even_row = v[:, :LANES].reshape(slices, per, STRIPS, LANES)
            odd_row = v[:, LANES:].reshape(slices, per, STRIPS, LANES)
            main[side, row + 1] = even_row.astype(BF)
            main[side, row + 2] = odd_row.astype(BF)
            put_edge(side, pair + t, before, even_row)
            before = odd_row

    def first_step(c):
        parts = []
        for z in range(slices):
            at = pl.ds(z * stored + 8 * c, 16)
            parts.append(jnp.concatenate([xs[at, k * groups:(k + 1) * groups] for k in range(6)], axis=0).astype(BF))
        x = jnp.concatenate(parts, axis=1)
        y = lax.dot_general(x, w1[...], (((0,), (0,)), ((), ())), preferred_element_type=F32)
        put_pairs(0, 4 * c, 4, lambda t: y[:, t * 2 * LANES:(t + 1) * 2 * LANES])

    for c in range(rows // 8):
        first_step(c)

    def window(side, pair, out_rows):
        parts = [main[side, 2 * pair + a].reshape(span, LANES) for a in range(out_rows + 2)]
        parts += [edge[side, pair + e].reshape(span, LANES) for e in range(out_rows // 2 + 1)]
        return jnp.concatenate(parts, axis=1)

    pairs = rows // 2 - 2
    def layer_step(layer, carry):
        source, target = layer % 2, (layer + 1) % 2
        for c in range(pairs // chunk):
            pair = 1 + c * chunk
            x = jnp.concatenate([window(source, pair + t, 2) for t in range(chunk)], axis=0)
            y = jnp.dot(x, wh[layer], preferred_element_type=F32)
            put_pairs(target, pair, chunk, lambda t: y[t * span:(t + 1) * span])
        end = rows // 2 - 1
        put_edge(target, end, main[target, 2 * end].astype(F32), jnp.zeros((slices, per, STRIPS, LANES), F32))
        return carry

    lax.fori_loop(0, layers, layer_step, 0)

    eighths = local // 8
    quad = (lane_iota(span) // 8) % 4

    def last_step(q):
        x = window(layers % 2, halo // 2 + 4 * q, 8)
        y = jnp.dot(x, wl[...], preferred_element_type=F32)
        gathered_out[q // 4] = jnp.where(quad == q % 4, y, gathered_out[q // 4])

    gathered_out[...] = jnp.zeros_like(gathered_out)
    for q in range(eighths):
        last_step(q)

    for big in range(gathered_out.shape[0]):
        height = min(32, local - 32 * big)
        turned = [gathered_out[big, z * groups:(z + 1) * groups, :].T for z in range(slices)]
        lines = [jnp.concatenate([turned[z][k * 32:(k + 1) * 32] for k in range(4)], axis=1) for z in range(slices)]
        values = jnp.concatenate(lines, axis=0)
        high = values.astype(BF)
        low = (values - high.astype(F32)).astype(BF)
        net = jnp.dot(high, back[...], preferred_element_type=F32) + jnp.dot(low, back[...], preferred_element_type=F32)
        for z in range(slices):
            at = pl.ds(32 * big, height)
            out_ref[z, at, :] = cur_ref[z, at, :] - 2.0 * net[z * 32:z * 32 + height]

def axial_reflect(edges, current, cf, ch, cl, halo):
    slices, local, columns = current.shape
    rows = local + 2 * halo
    groups = columns // 4
    per = groups // STRIPS
    stored = rows + 8
    whole = pl.BlockSpec(memory_space=pltpu.VMEM)
    return pl.pallas_call(
        functools.partial(axial_kernel, (halo, 2)),
        out_shape=jax.ShapeDtypeStruct(current.shape, F32),
        in_specs=[whole] * 5,
        out_specs=whole,
        scratch_shapes=[
            pltpu.VMEM((2, rows + 2, slices, per, STRIPS, LANES), BF),
            pltpu.VMEM((2, rows // 2 + 1, slices, per, STRIPS, LANES), BF),
            pltpu.VMEM((96, 8 * LANES), BF),
            pltpu.VMEM((ch.shape[1], 6 * LANES, 2 * LANES), BF),
            pltpu.VMEM((15 * LANES, LANES), BF),
            pltpu.VMEM((slices * stored, columns), F32),
            pltpu.VMEM((slices * stored, 6 * groups), F32),
            pltpu.VMEM((columns, 6 * groups), BF),
            pltpu.VMEM((4 * groups, columns), BF),
            pltpu.VMEM((-(-local // 32), slices * groups, LANES), F32),
        ],
        compiler_params=pltpu.CompilerParams(vmem_limit_bytes=60 * 1024 * 1024),
        name="net_axial",
    )(edges, current, cf, ch, cl)


def fill_rows(raw, edges_ref, cur_ref, stored, halo):
    slices, local, columns = cur_ref.shape
    zero = jnp.zeros((1, columns), F32)
    tail = jnp.zeros((stored - 1 - local - 2 * halo, columns), F32)
    for z in range(slices):
        above = edges_ref[0, z * halo:(z + 1) * halo, :].astype(F32)
        below = edges_ref[1, z * halo:(z + 1) * halo, :].astype(F32)
        raw[z * stored:(z + 1) * stored, :] = jnp.concatenate([zero, above, cur_ref[z], below, tail], axis=0)


def build_first_plane(w_ref, o, w1):
    row = lax.broadcasted_iota(jnp.int32, (16, LANES), 0)
    for z in range(4):
        mixes = []
        for tj in range(3):
            taps = [jnp.broadcast_to(spread_lanes(w_ref[o, ti, tj:tj+1, :].astype(F32)), (16, LANES)) for ti in range(3)]
            mixes.append(slot_mix(16, taps, z, NATURAL, 32))
        for t in range(8):
            value = jnp.zeros((16, LANES), F32)
            for tj in range(3):
                value = jnp.where(row == t + tj, mixes[tj], value)
            w1[z * 16:(z + 1) * 16, t * LANES:(t + 1) * LANES] = value.astype(BF)

def build_hidden_plane(w_ref, o, layer, wh):
    wide = [[spread_lanes(w_ref[o, layer, ti, tj].astype(F32)) for ti in range(3)] for tj in range(3)]
    inner = wide[0][0].shape[0]
    for a in range(4):
        for z in range(4):
            at = a * LANES + z * inner
            for half in range(2):
                if 0 <= a - half < 3:
                    value = slot_mix(inner, wide[a - half], z, NATURAL, inner)
                else:
                    value = jnp.zeros((inner, LANES), F32)
                wh[layer, at:at + inner, half * LANES:(half + 1) * LANES] = value.astype(BF)

def build_last_plane(w_ref, o, wl):
    taps = [[column_of(w_ref[o, ti, tj:tj+1, :].astype(F32)) for ti in range(3)] for tj in range(3)]
    inner = taps[0][0].shape[0]
    row8 = lane_iota(inner) % 8
    zero = jnp.zeros((inner, LANES), F32)
    for a in range(10):
        line = []
        for ti in range(3):
            value = zero
            for tj in range(3):
                if 0 <= a - tj < 8:
                    value = jnp.where(row8 == a - tj, taps[tj][ti], value)
            line.append(value)
        for z in range(4):
            at = a * LANES + z * inner
            wl[at:at + inner, :] = slot_mix(inner, line, z, NATURAL, LANES // 4).astype(BF)


def plane_kernel(plan, x_ref, cur_ref, cf_ref, ch_ref, cl_ref, out_ref, main, w1, wh, wl, xs, gathered_out):
    o, halo, chunk, strips = plan
    slices, local, span = out_ref.shape
    rows = local + 2 * halo
    stored = rows + 8
    layers = ch_ref.shape[1]
    if halo:
        tile = lax.axis_index("tile")
        at_start = tile == 0
        at_end = tile == lax.axis_size("tile") - 1

    build_first_plane(cf_ref, o, w1)
    for layer in range(layers):
        build_hidden_plane(ch_ref, o, layer, wh)
    build_last_plane(cl_ref, o, wl)
    if halo:
        fill_rows(xs, x_ref, cur_ref, stored, halo)
    else:
        xs[...] = x_ref[...].astype(F32)
    for side in range(2):
        for r in (0, rows + 1):
            main[side, r] = jnp.zeros((span, LANES), BF)

    def put_pairs(side, pair, count, y):
        for t in range(count):
            row = 2 * (pair + t)
            v = jnp.maximum(y(t), 0.0)
            if halo:
                outside = (at_start & (row < halo)) | (at_end & (row >= rows - halo))
                v = v * jnp.where(outside, 0.0, 1.0)
            main[side, row + 1] = v[:, :LANES].astype(BF)
            main[side, row + 2] = v[:, LANES:].astype(BF)

    def ends(side):
        if strips > 1:
            step = span // strips
            main[side, 0, step:span] = main[side, rows, 0:span - step]
            main[side, rows + 1, 0:span - step] = main[side, 1, step:span]

    def first_step(c, carry):
        parts = [xs[pl.ds(pl.multiple_of(z * stored + 8 * c, 8), 16)] for z in range(slices)]
        x = jnp.concatenate(parts, axis=0).astype(BF)
        y = lax.dot_general(x, w1[...], (((0,), (0,)), ((), ())), preferred_element_type=F32)
        put_pairs(0, 4 * c, 4, lambda t: y[:, t * 2 * LANES:(t + 1) * 2 * LANES])
        return carry

    lax.fori_loop(0, rows // 8, first_step, 0)
    ends(0)

    for layer in range(layers):
        source, target = layer % 2, (layer + 1) % 2

        def hidden_step(c, carry):
            pair = c * chunk
            tiles = [main[source, 2 * pair + a] for a in range(2 * chunk + 2)]
            x = jnp.concatenate([jnp.concatenate(tiles[2 * t:2 * t + 4], axis=1) for t in range(chunk)], axis=0)
            y = jnp.dot(x, wh[layer], preferred_element_type=F32)
            put_pairs(target, pair, chunk, lambda t: y[t * span:(t + 1) * span])
            return carry

        lax.fori_loop(0, rows // 2 // chunk, hidden_step, 0)
        ends(target)

    quad = (lane_iota(span) // 8) % 4

    def last_step(q, carry):
        x = jnp.concatenate([main[layers % 2, halo + 8 * q + a] for a in range(10)], axis=1)
        y = jnp.dot(x, wl[...], preferred_element_type=F32)
        gathered_out[q // 4] = jnp.where(quad == q % 4, y, gathered_out[q // 4])
        return carry

    gathered_out[...] = jnp.zeros_like(gathered_out)
    lax.fori_loop(0, local // 8, last_step, 0)
    for big in range(gathered_out.shape[0]):
        height = min(32, local - 32 * big)
        net = gathered_out[big].T
        for z in range(slices):
            at = pl.ds(32 * big, height)
            out_ref[z, at, :] = cur_ref[z, at, :] - 2.0 * net[z * 32:z * 32 + height]

def plane_call(o, x, current, cf, ch, cl, halo, strips):
    slices, local, span = current.shape
    rows = local + 2 * halo
    whole = pl.BlockSpec(memory_space=pltpu.VMEM)
    return pl.pallas_call(
        functools.partial(plane_kernel, (o, halo, 4, strips)),
        out_shape=jax.ShapeDtypeStruct(current.shape, F32),
        in_specs=[whole] * 5, out_specs=whole,
        scratch_shapes=[
            pltpu.VMEM((2, rows + 2, span, LANES), BF),
            pltpu.VMEM((64, 8 * LANES), BF),
            pltpu.VMEM((ch.shape[1], 4 * LANES, 2 * LANES), BF),
            pltpu.VMEM((10 * LANES, LANES), BF),
            pltpu.VMEM((slices * (rows + 8), span), F32),
            pltpu.VMEM((-(-local // 32), span, LANES), F32),
        ],
        compiler_params=pltpu.CompilerParams(vmem_limit_bytes=60 * 1024 * 1024),
        name="net_sagittal" if halo else "net_coronal",
    )(x, current, cf, ch, cl)

def coronal_reflect(current, cf, ch, cl):
    slices, local, columns = current.shape
    strips = columns // local
    turned = jnp.transpose(current.reshape(slices, local, strips, local), (0, 3, 2, 1))
    t = turned.astype(BF)
    none = jnp.zeros((slices, 1, 1, local), BF)
    before = jnp.concatenate([none, t[:, -1:, :-1]], axis=2)
    after = jnp.concatenate([t[:, :1, 1:], none], axis=2)
    rest = jnp.zeros((slices, 6, strips, local), BF)
    x = jnp.concatenate([before, t, after, rest], axis=1)
    x = x.reshape(-1, columns)
    out = plane_call(2, x, turned.reshape(slices, local, columns), cf, ch, cl, 0, strips)
    return jnp.transpose(out.reshape(slices, local, strips, local), (0, 3, 2, 1)).reshape(current.shape)

def halo_kernel(halo, cur_hbm, out_ref, edge, sent, load, send, recv):
    agent = lax.axis_index("agent")
    tile = lax.axis_index("tile")
    last = lax.axis_size("tile") - 1
    slices, local, columns = cur_hbm.shape
    rows = edge.shape[2]
    active = (agent == 1) | (agent == 2)

    def copy(side, peer):
        return pltpu.make_async_remote_copy(
            src_ref=sent.at[side],
            dst_ref=out_ref.at[1 - side],
            send_sem=send.at[side],
            recv_sem=recv.at[1 - side],
            device_id=(agent, peer),
            device_id_type=MESH,
        )

    @pl.when(active)
    def _():
        barrier = pltpu.get_barrier_semaphore()

        @pl.when(tile > 0)
        def _():
            pl.semaphore_signal(barrier, inc=1, device_id=(agent, tile - 1), device_id_type=MESH)

        @pl.when(tile < last)
        def _():
            pl.semaphore_signal(barrier, inc=1, device_id=(agent, tile + 1), device_id_type=MESH)

        loads = [
            pltpu.make_async_copy(cur_hbm.at[:, pl.ds(0, rows)], edge.at[0], load.at[0]),
            pltpu.make_async_copy(cur_hbm.at[:, pl.ds(local - rows, rows)], edge.at[1], load.at[1]),
        ]
        for item in loads:
            item.start()
        for item in loads:
            item.wait()
        for side in range(2):
            first = 0 if side == 0 else rows - halo
            parts = [edge[side, z, first:first + halo, :] for z in range(slices)]
            sent[side] = jnp.concatenate(parts, axis=0).astype(BF)

        pl.semaphore_wait(barrier, jnp.where(tile > 0, 1, 0) + jnp.where(tile < last, 1, 0))

        @pl.when(tile > 0)
        def _():
            copy(0, tile - 1).start()

        @pl.when(tile < last)
        def _():
            copy(1, tile + 1).start()

        @pl.when(tile == 0)
        def _():
            out_ref[0] = jnp.zeros(out_ref.shape[1:], BF)

        @pl.when(tile == last)
        def _():
            out_ref[1] = jnp.zeros(out_ref.shape[1:], BF)

        @pl.when(tile > 0)
        def _():
            copy(1, tile - 1).wait_recv()

        @pl.when(tile < last)
        def _():
            copy(0, tile + 1).wait_recv()

        @pl.when(tile > 0)
        def _():
            copy(0, tile - 1).wait_send()

        @pl.when(tile < last)
        def _():
            copy(1, tile + 1).wait_send()


def halo_exchange(current, halo):
    slices, local, columns = current.shape
    return pl.pallas_call(
        functools.partial(halo_kernel, halo),
        out_shape=jax.ShapeDtypeStruct((2, slices * halo, columns), BF),
        in_specs=[pl.BlockSpec(memory_space=pl.ANY)],
        out_specs=pl.BlockSpec(memory_space=pltpu.VMEM),
        scratch_shapes=[
            pltpu.VMEM((2, slices, 8, columns), F32),
            pltpu.VMEM((2, slices * halo, columns), BF),
            pltpu.SemaphoreType.DMA((2,)),
            pltpu.SemaphoreType.DMA((2,)),
            pltpu.SemaphoreType.DMA((2,)),
        ],
        compiler_params=pltpu.CompilerParams(collective_id=2, has_side_effects=True),
        name="halo_exchange",
    )(current)


def swap_bits(me, d):
    peer, bit = me, 1
    while bit <= d:
        if d & bit:
            peer = peer + bit * (1 - 2 * ((me // bit) % 2))
        bit *= 2
    return peer


def block_copy(blocks_hbm, held, sems, i):
    at = pl.ds(i * CHUNK, CHUNK)
    return pltpu.make_async_copy(blocks_hbm.at[at], held.at[at], sems.at[i])


def block_step(held, picked, y, slices, transposed, u):
    row = lax.broadcasted_iota(jnp.int32, (8, LANES), 0)
    upper, even = row < 4, row % 2 == 0
    at = pl.ds(pl.multiple_of(8 * u, 8), 8)

    def turned(v):
        return pltpu.roll(v, 4, 0)

    rows = [[], []]
    for z in range(0, slices, 2):
        v, w = (picked[at, (z + i) * LANES:(z + i + 1) * LANES] for i in range(2))
        rows[0].append(jnp.where(upper, v, turned(w)))
        rows[1].append(jnp.where(upper, turned(v), w))
    outs = []
    for t in range(2):
        sides = [
            jnp.concatenate([jnp.where(row % 4 // 2 == side, v, 0.0) for v in rows[t]], axis=0) for side in range(2)
        ]
        lhs = jnp.concatenate(sides, axis=1).astype(BF)
        m = [held[8 * u + 4 * t + j] for j in range(4)]
        if transposed:
            top, bottom = jnp.concatenate([m[0], m[2]], axis=1), jnp.concatenate([m[1], m[3]], axis=1)
            dims = (((1,), (1,)), ((), ()))
        else:
            top, bottom = jnp.concatenate([m[0], m[1]], axis=1), jnp.concatenate([m[2], m[3]], axis=1)
            dims = (((1,), (0,)), ((), ()))
        rhs = jnp.concatenate([top, bottom], axis=0)
        out = lax.dot_general(lhs, rhs, dims, preferred_element_type=F32)
        outs.append(jnp.where(jnp.concatenate([even] * (slices // 2), axis=0), out[:, :LANES], out[:, LANES:]))
    for z in range(0, slices, 2):
        v, w = (o[4 * z:4 * z + 8] for o in outs)
        y[at, z * LANES:(z + 1) * LANES] = jnp.where(upper, v, turned(w))
        y[at, (z + 1) * LANES:(z + 2) * LANES] = jnp.where(upper, turned(v), w)


def block_sweep(blocks_hbm, held, sems, picked, y, slices, transposed, waiting):
    pieces = held.shape[0] // CHUNK
    for i in range(pieces):
        if waiting:
            block_copy(blocks_hbm, held, sems, i).wait()
            if i + DEPTH < pieces:
                block_copy(blocks_hbm, held, sems, i + DEPTH).start()
        for j in range(CHUNK // 8):
            block_step(held, picked, y, slices, transposed, i * (CHUNK // 8) + j)


def gather_rows(hot, source):
    return jnp.dot(hot, source, preferred_element_type=F32)


def scatter_rows(hot, y):
    high = y.astype(BF)
    low = (y - high.astype(F32)).astype(BF)
    return jnp.dot(
        jnp.concatenate([hot, hot], axis=1), jnp.concatenate([high, low], axis=0), preferred_element_type=F32
    )


def join_kernel(
    plan, angle_ref, detector_ref, tile_ref, sino_ref, reflect_ref, cur_hbm, blocks_hbm, out_ref,
    held, cur, ray_hot, ray_turned, tile_hot, tile_turned, x, y, picked, total, part, got, fresh, full,
    own, pair, beside, across, onward,
    load, sems, send1, recv1, send2, recv2, ready,
    send_beside, recv_beside, send_across, recv_across, send_onward, recv_onward,
):
    agent = lax.axis_index("agent")
    me = lax.axis_index("tile")
    count, slices = plan
    chunks, height, columns = own.shape
    local = chunks * height // slices
    detectors = columns // LANES
    rays_here = fresh.shape[2]
    ray_total = count * rays_here
    tiles_here = detectors * local
    blocks_here = held.shape[0]
    order = list(range(count - 1, 0, -1))
    core = agent % 2
    neighbour = agent + 1 - 2 * core
    opposite = (agent + 2) % 4
    state = pltpu.make_async_copy(cur_hbm, cur, load.at[0])
    state.start()

    def send(source, target, s, r, k, to):
        return pltpu.make_async_remote_copy(
            src_ref=source.at[k], dst_ref=target.at[k], send_sem=s.at[k], recv_sem=r.at[k],
            device_id=(to, me), device_id_type=MESH,
        )

    def to_beside(k):
        return send(own, beside, send_beside, recv_beside, k, neighbour)

    def to_across(source, k):
        return send(source, across, send_across, recv_across, k, opposite)

    def to_onward(k):
        return send(across, onward, send_onward, recv_onward, k, neighbour)

    def rows_of(k):
        return slice(k * height, (k + 1) * height)

    width = slices // 2 * LANES

    def columns_of(h):
        return slice(h * width, (h + 1) * width)

    def part_copy(step, h, d):
        return pltpu.make_async_remote_copy(
            src_ref=part.at[step, h, swap_bits(me, d)],
            dst_ref=got.at[step, h, d],
            send_sem=send1.at[step, h, d],
            recv_sem=recv1.at[step, h, d],
            device_id=(agent, swap_bits(me, d)),
            device_id_type=MESH,
        )

    def rest_copy(step, h, d):
        return pltpu.make_async_remote_copy(
            src_ref=fresh.at[step, h],
            dst_ref=full.at[step, h, me],
            send_sem=send2.at[step, h, d],
            recv_sem=recv2.at[step, h, d],
            device_id=(agent, swap_bits(me, d)),
            device_id_type=MESH,
        )

    def exchange(step, barrier):
        for h in range(2):
            total[h] = scatter_rows(ray_hot[...], y[:, columns_of(h)])
            for slot in range(count):
                part[step, h, slot] = total[h, slot * rays_here:(slot + 1) * rays_here, :].astype(BF)
            if step == 0 and h == 0:
                pl.semaphore_wait(barrier, count - 1)
            for d in order:
                part_copy(step, h, d).start()
        for h in range(2):
            value = total[h, pl.ds(pl.multiple_of(me * rays_here, 8), rays_here), :]
            measured = [
                sino_ref[pl.ds(h * (slices // 2) + z, rays_here, stride=slices), :] for z in range(slices // 2)
            ]
            value = value - jnp.concatenate(measured, axis=1)
            for d in reversed(order):
                part_copy(step, h, d).wait_recv()
                value = value + got[step, h, d].astype(F32)
            fresh[step, h] = value.astype(BF)
            for d in order:
                rest_copy(step, h, d).start()
            full[step, h, me] = fresh[step, h]
        for h in range(2):
            for d in order:
                rest_copy(step, h, d).wait_recv()
            picked[:, columns_of(h)] = gather_rows(ray_turned[...], full[step, h].reshape(ray_total, width))

    def exchanged(step):
        for h in range(2):
            for d in order:
                part_copy(step, h, d).wait_send()
                rest_copy(step, h, d).wait_send()

    middle = chunks // 2

    def half_of(side):
        return range(side * middle, chunks if side else middle)

    def last_update(side):
        first, count_here = side * (slices // 2), slices // 2 if side == 0 else slices - slices // 2
        at = slice(first * LANES, (first + count_here) * LANES)
        moved = x[:, at] - 0.8 * scatter_rows(tile_hot[...], y[:, at])
        for z in range(count_here):
            for t in range(detectors):
                place = (slice((first + z) * local, (first + z + 1) * local), slice(t * LANES, (t + 1) * LANES))
                piece = moved[t * local:(t + 1) * local, z * LANES:(z + 1) * LANES]
                out_ref[place] = 2.0 * piece - cur[place]

    def finish(k, base, others):
        out_ref[rows_of(k), :] = 2.0 * cur[rows_of(k), :] - base[rows_of(k), :] + others

    def low_part(side, base):
        mine, rest = half_of(side), half_of(1 - side)
        for part_of in (rest, mine):
            if side == 0:
                last_update(0 if part_of is mine else 1)
                for k in part_of:
                    own[k] = out_ref[rows_of(k), :].astype(BF)
                if part_of is rest:
                    pl.semaphore_wait(ready.at[0], 2)
            for k in part_of:
                to_beside(k).start()
        for k in mine:
            to_beside(k).wait_recv()
            pair[k] = (own[k].astype(F32) + beside[k].astype(F32)).astype(BF)
            to_across(pair, k).start()
        for part_of in (mine, rest):
            for k in part_of:
                if part_of is rest:
                    to_beside(k).wait_recv()
                to_across(pair, k).wait_recv()
                finish(k, base, beside[k].astype(F32) + across[k].astype(F32))
        for k in range(chunks):
            to_beside(k).wait_send()
        for k in mine:
            to_across(pair, k).wait_send()

    def high_part(side):
        mine, rest = half_of(side), half_of(1 - side)
        for k in range(chunks):
            to_beside(k).start()
        for k in range(chunks):
            to_beside(k).wait_recv()
            pair[k] = (own[k].astype(F32) + beside[k].astype(F32)).astype(BF)
            to_across(pair, k).start()
        for k in mine:
            to_across(pair, k).wait_recv()
            to_onward(k).start()
            finish(k, reflect_ref, beside[k].astype(F32) + across[k].astype(F32))
        for k in rest:
            to_onward(k).wait_recv()
            finish(k, reflect_ref, beside[k].astype(F32) + onward[k].astype(F32))
        for k in range(chunks):
            to_beside(k).wait_send()
            to_across(pair, k).wait_send()
        for k in mine:
            to_onward(k).wait_send()

    @pl.when(agent == 0)
    def _():
        barrier = pltpu.get_barrier_semaphore()
        for d in order:
            pl.semaphore_signal(barrier, inc=1, device_id=(agent, swap_bits(me, d)), device_id_type=MESH)
        for peer in (neighbour, opposite):
            pl.semaphore_signal(barrier, inc=1, device_id=(peer, me), device_id_type=MESH)
        for i in range(min(DEPTH, blocks_here // CHUNK)):
            block_copy(blocks_hbm, held, sems, i).start()

        hot_rows = lax.broadcasted_iota(jnp.int32, (ray_total, blocks_here), 0)
        ray = angle_ref[...] * detectors + detector_ref[...]
        hot = jnp.where(hot_rows == jnp.broadcast_to(ray, hot_rows.shape), 1.0, 0.0)
        ray_hot[...] = hot.astype(BF)
        ray_turned[...] = hot.T.astype(BF)
        hot_rows = lax.broadcasted_iota(jnp.int32, (tiles_here, blocks_here), 0)
        place = tile_ref[...]
        place = (place % detectors) * local + place // detectors
        hot = jnp.where(hot_rows == jnp.broadcast_to(place, hot_rows.shape), 1.0, 0.0)
        tile_hot[...] = hot.astype(BF)
        tile_turned[...] = hot.T.astype(BF)

        state.wait()
        for z in range(slices):
            for t in range(detectors):
                x[t * local:(t + 1) * local, z * LANES:(z + 1) * LANES] = cur[z * local:(z + 1) * local, t * LANES:(t + 1) * LANES]

        for step in range(DATA_STEPS):
            picked[...] = gather_rows(tile_turned[...], x[...].astype(BF))
            block_sweep(blocks_hbm, held, sems, picked, y, slices, True, step == 0)
            exchange(step, barrier)
            block_sweep(blocks_hbm, held, sems, picked, y, slices, False, False)
            exchanged(step)
            if step < DATA_STEPS - 1:
                x[...] = x[...] - 0.8 * scatter_rows(tile_hot[...], y[...])

        low_part(0, out_ref)

    @pl.when(agent != 0)
    def _():
        barrier = pltpu.get_barrier_semaphore()

        @pl.when(agent != 1)
        def _():
            pl.semaphore_signal(barrier, inc=1, device_id=(neighbour, me), device_id_type=MESH)

        @pl.when(agent != 2)
        def _():
            pl.semaphore_signal(barrier, inc=1, device_id=(opposite, me), device_id_type=MESH)

        for k in range(chunks):
            own[k] = reflect_ref[rows_of(k), :].astype(BF)
        state.wait()
        pl.semaphore_wait(barrier, 2)

        @pl.when(agent != 3)
        def _():
            pl.semaphore_signal(ready.at[0], inc=1, device_id=(0, me), device_id_type=MESH)

        @pl.when(agent == 1)
        def _():
            low_part(1, reflect_ref)

        @pl.when(agent == 2)
        def _():
            high_part(0)

        @pl.when(agent == 3)
        def _():
            high_part(1)


def idle_kernel(out_ref):
    pass


def join(angle, detector, tile, sinogram, reflect, current, blocks, count):
    slices, local, columns = current.shape
    rays_here = sinogram.shape[0]
    ray_total = rays_here * count
    tiles_here = columns // LANES * local
    blocks_here = blocks.shape[0]
    width = slices * LANES
    rows = slices * local
    chunks = max(2, rows // 32)
    chunk = (chunks, rows // chunks, columns)
    vmem = pl.BlockSpec(memory_space=pltpu.VMEM)
    anywhere = pl.BlockSpec(memory_space=pl.ANY)
    out = pl.pallas_call(
        functools.partial(join_kernel, (count, slices)),
        out_shape=pltpu.VMEM((rows, columns), F32),
        in_specs=[vmem] * 5 + [anywhere] * 2,
        out_specs=vmem,
        scratch_shapes=[
            pltpu.VMEM(blocks.shape, BF),
            pltpu.VMEM((rows, columns), F32),
            pltpu.VMEM((ray_total, blocks_here), BF),
            pltpu.VMEM((blocks_here, ray_total), BF),
            pltpu.VMEM((tiles_here, blocks_here), BF),
            pltpu.VMEM((blocks_here, tiles_here), BF),
            pltpu.VMEM((tiles_here, width), F32),
            pltpu.VMEM((blocks_here, width), F32),
            pltpu.VMEM((blocks_here, width), F32),
            pltpu.VMEM((2, ray_total, width // 2), F32),
            pltpu.VMEM((DATA_STEPS, 2, count, rays_here, width // 2), BF),
            pltpu.VMEM((DATA_STEPS, 2, count, rays_here, width // 2), BF),
            pltpu.VMEM((DATA_STEPS, 2, rays_here, width // 2), BF),
            pltpu.VMEM((DATA_STEPS, 2, count, rays_here, width // 2), BF),
        ]
        + [pltpu.VMEM(chunk, BF)] * 5
        + [pltpu.SemaphoreType.DMA((1,)), pltpu.SemaphoreType.DMA((blocks_here // CHUNK,))]
        + [pltpu.SemaphoreType.DMA((DATA_STEPS, 2, count))] * 4
        + [pltpu.SemaphoreType.REGULAR((1,))]
        + [pltpu.SemaphoreType.DMA((chunks,))] * 6,
        compiler_params=pltpu.CompilerParams(
            collective_id=0, has_side_effects=True, vmem_limit_bytes=58 * 1024 * 1024
        ),
        name="join_agents",
    )(
        angle.reshape(1, -1), detector.reshape(1, -1), tile.reshape(1, -1),
        sinogram.reshape(rays_here * slices, LANES), reflect.reshape(rows, columns),
        current.reshape(rows, columns), blocks,
    )
    return out.reshape(current.shape)


def per_device(
    states,
    sinogram,
    blocks,
    block_angle,
    block_detector,
    block_tile,
    conv_first,
    conv_hidden,
    conv_last,
):
    current = states[0]
    agent_place = lax.axis_index("agent")
    halo = conv_hidden.shape[1] + 2
    filters = (conv_first, conv_hidden, conv_last)
    edges = halo_exchange(current, halo)

    def data_only():
        return pl.pallas_call(
            idle_kernel,
            out_shape=jax.ShapeDtypeStruct(current.shape, F32),
            out_specs=pl.BlockSpec(memory_space=pl.ANY),
            name="idle",
        )()

    def axial_only():
        return axial_reflect(edges, current, *filters, halo)

    def sagittal_only():
        return plane_call(1, edges, current, *filters, halo, 1)

    def coronal_only():
        return coronal_reflect(current, *filters)

    reflect = lax.switch(agent_place, [data_only, axial_only, sagittal_only, coronal_only])
    joined = join(
        block_angle, block_detector, block_tile, sinogram, reflect, current, blocks, lax.axis_size("tile")
    )
    return (0.25 * joined)[None]


def solution(mesh):
    placed = (
        P("agent", None, "tile", None),
        P("tile", None, None),
        P("tile", None, None),
        P("tile"),
        P("tile"),
        P("tile"),
        P(),
        P(),
        P(),
    )
    return jax.shard_map(
        per_device,
        mesh=mesh,
        in_specs=placed,
        out_specs=P("agent", None, "tile", None),
        check_vma=False,
    )
```

```python
import functools

import jax
import jax.numpy as jnp
from jax import lax
from jax.experimental import pallas as pl
from jax.experimental.pallas import tpu as pltpu
from jax.sharding import PartitionSpec as P

DATA_STEPS = 2
MESH = pl.DeviceIdType.MESH
LANES = 128
STRIPS = 16
CHUNK = 64
DEPTH = 2
BF = jnp.bfloat16
F32 = jnp.float32
NATURAL = (0, 1, 2, 3)
EVEN_ORDER = (0, 1, 2, 3)
ODD_ORDER = (1, 0, 3, 2)


def main_cells(offset):
    order = EVEN_ORDER if offset % 2 else ODD_ORDER
    return [(offset, column) for column in order]

def edge_cells(offset):
    return [(offset + 1, 4), (offset, 4), (offset, -1), (offset + 1, -1)]

def window_cells(rows):
    tiles = [main_cells(a) for a in range(rows + 2)]
    return tiles + [edge_cells(a) for a in range(0, rows + 2, 2)]

def spread_lanes(w):
    return jnp.concatenate([w] * (LANES // w.shape[-1]), axis=-1)

def lane_iota(rows):
    return lax.broadcasted_iota(jnp.int32, (rows, LANES), 1)

def slot_mix(rows, taps, column_in, order, width):
    slot = lane_iota(rows) // width
    mixed = jnp.zeros((rows, LANES), F32)
    for place, column in enumerate(order):
        tap = column_in - column + 1
        if 0 <= tap < 3:
            mixed = jnp.where(slot == place, taps[tap], mixed)
    return mixed

def build_first(w_ref, o, w1):
    for k in range(6):
        for half in range(2):
            order = ODD_ORDER if half else EVEN_ORDER
            mixes = []
            for ti in range(3):
                taps = [jnp.broadcast_to(spread_lanes(w_ref[o, ti, tj:tj+1, :].astype(F32)), (16, LANES)) for tj in range(3)]
                mixes.append(slot_mix(16, taps, k - 1, order, 32))
            row = lax.broadcasted_iota(jnp.int32, (16, LANES), 0)
            for t in range(4):
                value = jnp.zeros((16, LANES), F32)
                for ti in range(3):
                    value = jnp.where(row == 2 * t + half + ti, mixes[ti], value)
                at = t * 2 * LANES + half * LANES
                w1[k * 16:(k + 1) * 16, at:at + LANES] = value.astype(BF)

def build_hidden(w_ref, o, layer, wh):
    wide = [[spread_lanes(w_ref[o, layer, ti, tj].astype(F32)) for tj in range(3)] for ti in range(3)]
    inner = wide[0][0].shape[0]
    for n, tile in enumerate(window_cells(2)):
        for slot, (a, column) in enumerate(tile):
            at = n * LANES + slot * inner
            for half in range(2):
                ti = a - (half + 1) + 1
                if 0 <= ti < 3:
                    value = slot_mix(inner, wide[ti], column, ODD_ORDER if half else EVEN_ORDER, inner)
                else:
                    value = jnp.zeros((inner, LANES), F32)
                wh[layer, at:at + inner, half * LANES:(half + 1) * LANES] = value.astype(BF)

def column_of(row):
    inner = row.shape[1]
    r = lax.broadcasted_iota(jnp.int32, (inner, inner), 0)
    c = lax.broadcasted_iota(jnp.int32, (inner, inner), 1)
    picked = jnp.where(r == c, jnp.broadcast_to(row, (inner, inner)), 0.0)
    return jnp.broadcast_to(jnp.sum(picked, axis=1, keepdims=True), (inner, LANES))

def build_last(w_ref, o, wl):
    taps = [[column_of(w_ref[o, ti, tj:tj+1, :].astype(F32)) for tj in range(3)] for ti in range(3)]
    inner = taps[0][0].shape[0]
    lane = lane_iota(inner)
    row8 = lane % 8
    zero = jnp.zeros((inner, LANES), F32)
    rows = []
    for a in range(10):
        line = []
        for tj in range(3):
            value = zero
            for ti in range(3):
                if 0 <= a - ti < 8:
                    value = jnp.where(row8 == a - ti, taps[ti][tj], value)
            line.append(value)
        rows.append(line)
    for n, tile in enumerate(window_cells(8)):
        for slot, (a, column) in enumerate(tile):
            at = n * LANES + slot * inner
            wl[at:at + inner, :] = slot_mix(inner, rows[a], column, EVEN_ORDER, LANES // 4).astype(BF)


def axial_kernel(plan, edges_ref, cur_ref, cf_ref, ch_ref, cl_ref, out_ref, main, edge, w1, wh, wl, raw, xs, place, back, gathered_out):
    halo = plan
    slices, local, columns = cur_ref.shape
    rows = local + 2 * halo
    stored = rows + 8
    groups = columns // 4
    per = groups // STRIPS
    span = slices * groups
    layers = ch_ref.shape[1]
    tile = lax.axis_index("tile")
    at_start = tile == 0
    at_end = tile == lax.axis_size("tile") - 1
    fill_rows(raw, edges_ref, cur_ref, stored, halo)

    build_first(cf_ref, 0, w1)
    for layer in range(layers):
        build_hidden(ch_ref, 0, layer, wh)
    build_last(cl_ref, 0, wl)

    col = lax.broadcasted_iota(jnp.int32, (columns, groups), 0)
    m = lax.broadcasted_iota(jnp.int32, (columns, groups), 1)
    first_col = 4 * ((m % STRIPS) * per + m // STRIPS)
    for k in range(6):
        place[:, k * groups:(k + 1) * groups] = jnp.where(col == first_col + (k - 1), 1.0, 0.0).astype(BF)
    m = lax.broadcasted_iota(jnp.int32, (groups, columns), 0)
    col = lax.broadcasted_iota(jnp.int32, (groups, columns), 1)
    first_col = 4 * ((m % STRIPS) * per + m // STRIPS)
    for k in range(4):
        back[k * groups:(k + 1) * groups, :] = jnp.where(col == first_col + k, 1.0, 0.0).astype(BF)
    xs[...] = jnp.dot(raw[...].astype(BF), place[...], preferred_element_type=F32)

    slot = lane_iota(STRIPS) // (LANES // 4)
    even_slots = (slot == 0) | (slot == 3)
    right_slots = slot < 2
    strip = lax.broadcasted_iota(jnp.int32, (STRIPS, LANES), 0)
    zero_tile = jnp.zeros((slices, per, STRIPS, LANES), BF)

    for side in range(2):
        for r in (0, 1, 2, rows - 1, rows, rows + 1):
            main[side, r] = zero_tile
        for e in (0, 1, rows // 2 - 1, rows // 2):
            edge[side, e] = zero_tile

    def put_edge(side, e, odd_row, even_row):
        v = jnp.where(even_slots, even_row, odd_row)
        for z in range(slices):
            for i in range(per):
                if i + 1 < per:
                    right = v[z, i + 1]
                else:
                    right = jnp.where(strip == STRIPS - 1, 0.0, pltpu.roll(v[z, 0], STRIPS - 1, 0))
                if i > 0:
                    left = v[z, i - 1]
                else:
                    left = jnp.where(strip == 0, 0.0, pltpu.roll(v[z, per - 1], 1, 0))
                edge[side, e, z, i] = jnp.where(right_slots, right, left).astype(BF)

    def put_pairs(side, pair, count, y):
        before = main[side, 2 * pair].astype(F32)
        for t in range(count):
            row = 2 * (pair + t)
            v = jnp.maximum(y(t), 0.0)
            if not isinstance(row, int):
                outside = (at_start & (row < halo)) | (at_end & (row >= rows - halo))
                v = v * jnp.where(outside, 0.0, 1.0)
            elif row < halo:
                v = v * jnp.where(at_start, 0.0, 1.0)
            elif row >= rows - halo:
                v = v * jnp.where(at_end, 0.0, 1.0)
            even_row = v[:, :LANES].reshape(slices, per, STRIPS, LANES)
            odd_row = v[:, LANES:].reshape(slices, per, STRIPS, LANES)
            main[side, row + 1] = even_row.astype(BF)
            main[side, row + 2] = odd_row.astype(BF)
            put_edge(side, pair + t, before, even_row)
            before = odd_row

    def first_step(c):
        parts = []
        for z in range(slices):
            at = pl.ds(z * stored + 8 * c, 16)
            parts.append(jnp.concatenate([xs[at, k * groups:(k + 1) * groups] for k in range(6)], axis=0).astype(BF))
        x = jnp.concatenate(parts, axis=1)
        y = lax.dot_general(x, w1[...], (((0,), (0,)), ((), ())), preferred_element_type=F32)
        put_pairs(0, 4 * c, 4, lambda t: y[:, t * 2 * LANES:(t + 1) * 2 * LANES])

    for c in range(rows // 8):
        first_step(c)

    def window(side, pair, out_rows):
        parts = [main[side, 2 * pair + a].reshape(span, LANES) for a in range(out_rows + 2)]
        parts += [edge[side, pair + e].reshape(span, LANES) for e in range(out_rows // 2 + 1)]
        return jnp.concatenate(parts, axis=1)

    pairs = rows // 2 - 2
    run = max(n for n in range(1, 18) if pairs % n == 0)
    for layer in range(layers):
        source, target = layer % 2, (layer + 1) % 2

        def hidden_steps(c, carry):
            for j in range(run):
                pair = 1 + c * run + j
                y = jnp.dot(window(source, pair, 2), wh[layer], preferred_element_type=F32)
                put_pairs(target, pair, 1, lambda t: y)
            return carry

        lax.fori_loop(0, pairs // run, hidden_steps, 0)
        end = rows // 2 - 1
        put_edge(target, end, main[target, 2 * end].astype(F32), jnp.zeros((slices, per, STRIPS, LANES), F32))

    eighths = local // 8
    quad = (lane_iota(span) // 8) % 4

    four = 4 if eighths % 4 == 0 else eighths

    def last_steps(c, carry):
        value = jnp.zeros((span, LANES), F32)
        for j in range(four):
            x = window(layers % 2, halo // 2 + 4 * (c * four + j), 8)
            y = jnp.dot(x, wl[...], preferred_element_type=F32)
            value = jnp.where(quad == j, y, value)
        gathered_out[c] = value
        return carry

    lax.fori_loop(0, eighths // four, last_steps, 0)

    for big in range(gathered_out.shape[0]):
        height = min(32, local - 32 * big)
        turned = [gathered_out[big, z * groups:(z + 1) * groups, :].T for z in range(slices)]
        lines = [jnp.concatenate([turned[z][k * 32:(k + 1) * 32] for k in range(4)], axis=1) for z in range(slices)]
        values = jnp.concatenate(lines, axis=0)
        high = values.astype(BF)
        low = (values - high.astype(F32)).astype(BF)
        net = jnp.dot(high, back[...], preferred_element_type=F32) + jnp.dot(low, back[...], preferred_element_type=F32)
        for z in range(slices):
            at = pl.ds(32 * big, height)
            out_ref[z, at, :] = cur_ref[z, at, :] - 2.0 * net[z * 32:z * 32 + height]

def axial_reflect(edges, current, cf, ch, cl, halo):
    slices, local, columns = current.shape
    rows = local + 2 * halo
    groups = columns // 4
    per = groups // STRIPS
    stored = rows + 8
    whole = pl.BlockSpec(memory_space=pltpu.VMEM)
    return pl.pallas_call(
        functools.partial(axial_kernel, halo),
        out_shape=jax.ShapeDtypeStruct(current.shape, F32),
        in_specs=[whole] * 5,
        out_specs=whole,
        scratch_shapes=[
            pltpu.VMEM((2, rows + 2, slices, per, STRIPS, LANES), BF),
            pltpu.VMEM((2, rows // 2 + 1, slices, per, STRIPS, LANES), BF),
            pltpu.VMEM((96, 8 * LANES), BF),
            pltpu.VMEM((ch.shape[1], 6 * LANES, 2 * LANES), BF),
            pltpu.VMEM((15 * LANES, LANES), BF),
            pltpu.VMEM((slices * stored, columns), F32),
            pltpu.VMEM((slices * stored, 6 * groups), F32),
            pltpu.VMEM((columns, 6 * groups), BF),
            pltpu.VMEM((4 * groups, columns), BF),
            pltpu.VMEM((-(-local // 32), slices * groups, LANES), F32),
        ],
        compiler_params=pltpu.CompilerParams(vmem_limit_bytes=60 * 1024 * 1024),
        name="net_axial",
    )(edges, current, cf, ch, cl)


def fill_rows(raw, edges_ref, cur_ref, stored, halo):
    slices, local, columns = cur_ref.shape
    zero = jnp.zeros((1, columns), F32)
    tail = jnp.zeros((stored - 1 - local - 2 * halo, columns), F32)
    for z in range(slices):
        above = edges_ref[0, z * halo:(z + 1) * halo, :].astype(F32)
        below = edges_ref[1, z * halo:(z + 1) * halo, :].astype(F32)
        raw[z * stored:(z + 1) * stored, :] = jnp.concatenate([zero, above, cur_ref[z], below, tail], axis=0)


def build_first_plane(w_ref, o, w1):
    row = lax.broadcasted_iota(jnp.int32, (16, LANES), 0)
    for z in range(4):
        mixes = []
        for tj in range(3):
            taps = [jnp.broadcast_to(spread_lanes(w_ref[o, ti, tj:tj+1, :].astype(F32)), (16, LANES)) for ti in range(3)]
            mixes.append(slot_mix(16, taps, z, NATURAL, 32))
        for t in range(8):
            value = jnp.zeros((16, LANES), F32)
            for tj in range(3):
                value = jnp.where(row == t + tj, mixes[tj], value)
            w1[z * 16:(z + 1) * 16, t * LANES:(t + 1) * LANES] = value.astype(BF)

def build_hidden_plane(w_ref, o, layer, wh):
    wide = [[spread_lanes(w_ref[o, layer, ti, tj].astype(F32)) for ti in range(3)] for tj in range(3)]
    inner = wide[0][0].shape[0]
    for a in range(4):
        for z in range(4):
            at = a * LANES + z * inner
            for half in range(2):
                if 0 <= a - half < 3:
                    value = slot_mix(inner, wide[a - half], z, NATURAL, inner)
                else:
                    value = jnp.zeros((inner, LANES), F32)
                wh[layer, at:at + inner, half * LANES:(half + 1) * LANES] = value.astype(BF)

def build_last_plane(w_ref, o, wl):
    taps = [[column_of(w_ref[o, ti, tj:tj+1, :].astype(F32)) for ti in range(3)] for tj in range(3)]
    inner = taps[0][0].shape[0]
    row8 = lane_iota(inner) % 8
    zero = jnp.zeros((inner, LANES), F32)
    for a in range(10):
        line = []
        for ti in range(3):
            value = zero
            for tj in range(3):
                if 0 <= a - tj < 8:
                    value = jnp.where(row8 == a - tj, taps[tj][ti], value)
            line.append(value)
        for z in range(4):
            at = a * LANES + z * inner
            wl[at:at + inner, :] = slot_mix(inner, line, z, NATURAL, LANES // 4).astype(BF)


def plane_kernel(plan, x_ref, cur_ref, cf_ref, ch_ref, cl_ref, out_ref, main, w1, wh, wl, xs, gathered_out):
    o, halo, chunk, strips = plan
    slices, local, span = out_ref.shape
    rows = local + 2 * halo
    stored = rows + 8
    layers = ch_ref.shape[1]
    if halo:
        tile = lax.axis_index("tile")
        at_start = tile == 0
        at_end = tile == lax.axis_size("tile") - 1

    build_first_plane(cf_ref, o, w1)
    for layer in range(layers):
        build_hidden_plane(ch_ref, o, layer, wh)
    build_last_plane(cl_ref, o, wl)
    if halo:
        fill_rows(xs, x_ref, cur_ref, stored, halo)
    else:
        xs[...] = x_ref[...].astype(F32)
    for side in range(2):
        for r in (0, rows + 1):
            main[side, r] = jnp.zeros((span, LANES), BF)

    def put_pairs(side, pair, count, y):
        for t in range(count):
            row = 2 * (pair + t)
            v = jnp.maximum(y(t), 0.0)
            if halo:
                outside = (at_start & (row < halo)) | (at_end & (row >= rows - halo))
                v = v * jnp.where(outside, 0.0, 1.0)
            main[side, row + 1] = v[:, :LANES].astype(BF)
            main[side, row + 2] = v[:, LANES:].astype(BF)

    def ends(side):
        if strips > 1:
            step = span // strips
            main[side, 0, step:span] = main[side, rows, 0:span - step]
            main[side, rows + 1, 0:span - step] = main[side, 1, step:span]

    def first_step(c, carry):
        parts = [xs[pl.ds(pl.multiple_of(z * stored + 8 * c, 8), 16)] for z in range(slices)]
        x = jnp.concatenate(parts, axis=0).astype(BF)
        y = lax.dot_general(x, w1[...], (((0,), (0,)), ((), ())), preferred_element_type=F32)
        put_pairs(0, 4 * c, 4, lambda t: y[:, t * 2 * LANES:(t + 1) * 2 * LANES])
        return carry

    lax.fori_loop(0, rows // 8, first_step, 0)
    ends(0)

    for layer in range(layers):
        source, target = layer % 2, (layer + 1) % 2

        def hidden_step(c, carry):
            pair = c * chunk
            tiles = [main[source, 2 * pair + a] for a in range(2 * chunk + 2)]
            x = jnp.concatenate([jnp.concatenate(tiles[2 * t:2 * t + 4], axis=1) for t in range(chunk)], axis=0)
            y = jnp.dot(x, wh[layer], preferred_element_type=F32)
            put_pairs(target, pair, chunk, lambda t: y[t * span:(t + 1) * span])
            return carry

        lax.fori_loop(0, rows // 2 // chunk, hidden_step, 0)
        ends(target)

    quad = (lane_iota(span) // 8) % 4

    def last_step(q, carry):
        x = jnp.concatenate([main[layers % 2, halo + 8 * q + a] for a in range(10)], axis=1)
        y = jnp.dot(x, wl[...], preferred_element_type=F32)
        gathered_out[q // 4] = jnp.where(quad == q % 4, y, gathered_out[q // 4])
        return carry

    gathered_out[...] = jnp.zeros_like(gathered_out)
    lax.fori_loop(0, local // 8, last_step, 0)
    for big in range(gathered_out.shape[0]):
        height = min(32, local - 32 * big)
        net = gathered_out[big].T
        for z in range(slices):
            at = pl.ds(32 * big, height)
            out_ref[z, at, :] = cur_ref[z, at, :] - 2.0 * net[z * 32:z * 32 + height]

def plane_call(o, x, current, cf, ch, cl, halo, strips):
    slices, local, span = current.shape
    rows = local + 2 * halo
    whole = pl.BlockSpec(memory_space=pltpu.VMEM)
    return pl.pallas_call(
        functools.partial(plane_kernel, (o, halo, 4, strips)),
        out_shape=jax.ShapeDtypeStruct(current.shape, F32),
        in_specs=[whole] * 5, out_specs=whole,
        scratch_shapes=[
            pltpu.VMEM((2, rows + 2, span, LANES), BF),
            pltpu.VMEM((64, 8 * LANES), BF),
            pltpu.VMEM((ch.shape[1], 4 * LANES, 2 * LANES), BF),
            pltpu.VMEM((10 * LANES, LANES), BF),
            pltpu.VMEM((slices * (rows + 8), span), F32),
            pltpu.VMEM((-(-local // 32), span, LANES), F32),
        ],
        compiler_params=pltpu.CompilerParams(vmem_limit_bytes=60 * 1024 * 1024),
        name="net_sagittal" if halo else "net_coronal",
    )(x, current, cf, ch, cl)

def coronal_reflect(current, cf, ch, cl):
    slices, local, columns = current.shape
    strips = columns // local
    turned = jnp.transpose(current.reshape(slices, local, strips, local), (0, 3, 2, 1))
    t = turned.astype(BF)
    none = jnp.zeros((slices, 1, 1, local), BF)
    before = jnp.concatenate([none, t[:, -1:, :-1]], axis=2)
    after = jnp.concatenate([t[:, :1, 1:], none], axis=2)
    rest = jnp.zeros((slices, 6, strips, local), BF)
    x = jnp.concatenate([before, t, after, rest], axis=1)
    x = x.reshape(-1, columns)
    out = plane_call(2, x, turned.reshape(slices, local, columns), cf, ch, cl, 0, strips)
    return jnp.transpose(out.reshape(slices, local, strips, local), (0, 3, 2, 1)).reshape(current.shape)

def halo_kernel(halo, cur_hbm, out_ref, edge, sent, load, send, recv):
    agent = lax.axis_index("agent")
    tile = lax.axis_index("tile")
    last = lax.axis_size("tile") - 1
    slices, local, columns = cur_hbm.shape
    rows = edge.shape[2]
    active = (agent == 1) | (agent == 2)

    def copy(side, peer):
        return pltpu.make_async_remote_copy(
            src_ref=sent.at[side],
            dst_ref=out_ref.at[1 - side],
            send_sem=send.at[side],
            recv_sem=recv.at[1 - side],
            device_id=(agent, peer),
            device_id_type=MESH,
        )

    @pl.when(active)
    def _():
        barrier = pltpu.get_barrier_semaphore()

        @pl.when(tile > 0)
        def _():
            pl.semaphore_signal(barrier, inc=1, device_id=(agent, tile - 1), device_id_type=MESH)

        @pl.when(tile < last)
        def _():
            pl.semaphore_signal(barrier, inc=1, device_id=(agent, tile + 1), device_id_type=MESH)

        loads = [
            pltpu.make_async_copy(cur_hbm.at[:, pl.ds(0, rows)], edge.at[0], load.at[0]),
            pltpu.make_async_copy(cur_hbm.at[:, pl.ds(local - rows, rows)], edge.at[1], load.at[1]),
        ]
        for item in loads:
            item.start()
        for item in loads:
            item.wait()
        for side in range(2):
            first = 0 if side == 0 else rows - halo
            parts = [edge[side, z, first:first + halo, :] for z in range(slices)]
            sent[side] = jnp.concatenate(parts, axis=0).astype(BF)

        pl.semaphore_wait(barrier, jnp.where(tile > 0, 1, 0) + jnp.where(tile < last, 1, 0))

        @pl.when(tile > 0)
        def _():
            copy(0, tile - 1).start()

        @pl.when(tile < last)
        def _():
            copy(1, tile + 1).start()

        @pl.when(tile == 0)
        def _():
            out_ref[0] = jnp.zeros(out_ref.shape[1:], BF)

        @pl.when(tile == last)
        def _():
            out_ref[1] = jnp.zeros(out_ref.shape[1:], BF)

        @pl.when(tile > 0)
        def _():
            copy(1, tile - 1).wait_recv()

        @pl.when(tile < last)
        def _():
            copy(0, tile + 1).wait_recv()

        @pl.when(tile > 0)
        def _():
            copy(0, tile - 1).wait_send()

        @pl.when(tile < last)
        def _():
            copy(1, tile + 1).wait_send()


def halo_exchange(current, halo):
    slices, local, columns = current.shape
    return pl.pallas_call(
        functools.partial(halo_kernel, halo),
        out_shape=jax.ShapeDtypeStruct((2, slices * halo, columns), BF),
        in_specs=[pl.BlockSpec(memory_space=pl.ANY)],
        out_specs=pl.BlockSpec(memory_space=pltpu.VMEM),
        scratch_shapes=[
            pltpu.VMEM((2, slices, 8, columns), F32),
            pltpu.VMEM((2, slices * halo, columns), BF),
            pltpu.SemaphoreType.DMA((2,)),
            pltpu.SemaphoreType.DMA((2,)),
            pltpu.SemaphoreType.DMA((2,)),
        ],
        compiler_params=pltpu.CompilerParams(collective_id=2, has_side_effects=True),
        name="halo_exchange",
    )(current)


def swap_bits(me, d):
    peer, bit = me, 1
    while bit <= d:
        if d & bit:
            peer = peer + bit * (1 - 2 * ((me // bit) % 2))
        bit *= 2
    return peer


def block_copy(blocks_hbm, held, sems, i):
    at = pl.ds(i * CHUNK, CHUNK)
    return pltpu.make_async_copy(blocks_hbm.at[at], held.at[at], sems.at[i])


def block_step(held, picked, y, slices, transposed, u):
    row = lax.broadcasted_iota(jnp.int32, (8, LANES), 0)
    upper, even = row < 4, row % 2 == 0
    at = pl.ds(pl.multiple_of(8 * u, 8), 8)

    def turned(v):
        return pltpu.roll(v, 4, 0)

    rows = [[], []]
    for z in range(0, slices, 2):
        v, w = (picked[at, (z + i) * LANES:(z + i + 1) * LANES] for i in range(2))
        rows[0].append(jnp.where(upper, v, turned(w)))
        rows[1].append(jnp.where(upper, turned(v), w))
    outs = []
    for t in range(2):
        sides = [
            jnp.concatenate([jnp.where(row % 4 // 2 == side, v, 0.0) for v in rows[t]], axis=0) for side in range(2)
        ]
        lhs = jnp.concatenate(sides, axis=1).astype(BF)
        m = [held[8 * u + 4 * t + j] for j in range(4)]
        if transposed:
            top, bottom = jnp.concatenate([m[0], m[2]], axis=1), jnp.concatenate([m[1], m[3]], axis=1)
            dims = (((1,), (1,)), ((), ()))
        else:
            top, bottom = jnp.concatenate([m[0], m[1]], axis=1), jnp.concatenate([m[2], m[3]], axis=1)
            dims = (((1,), (0,)), ((), ()))
        rhs = jnp.concatenate([top, bottom], axis=0)
        out = lax.dot_general(lhs, rhs, dims, preferred_element_type=F32)
        outs.append(jnp.where(jnp.concatenate([even] * (slices // 2), axis=0), out[:, :LANES], out[:, LANES:]))
    for z in range(0, slices, 2):
        v, w = (o[4 * z:4 * z + 8] for o in outs)
        y[at, z * LANES:(z + 1) * LANES] = jnp.where(upper, v, turned(w))
        y[at, (z + 1) * LANES:(z + 2) * LANES] = jnp.where(upper, turned(v), w)


def block_sweep(blocks_hbm, held, sems, picked, y, slices, transposed, waiting):
    pieces = held.shape[0] // CHUNK
    for i in range(pieces):
        if waiting:
            block_copy(blocks_hbm, held, sems, i).wait()
            if i + DEPTH < pieces:
                block_copy(blocks_hbm, held, sems, i + DEPTH).start()
        for j in range(CHUNK // 8):
            block_step(held, picked, y, slices, transposed, i * (CHUNK // 8) + j)


def gather_rows(hot, source):
    return jnp.dot(hot, source, preferred_element_type=F32)


def scatter_rows(hot, y):
    high = y.astype(BF)
    low = (y - high.astype(F32)).astype(BF)
    return jnp.dot(
        jnp.concatenate([hot, hot], axis=1), jnp.concatenate([high, low], axis=0), preferred_element_type=F32
    )


def join_kernel(
    plan, angle_ref, detector_ref, tile_ref, sino_ref, reflect_ref, cur_hbm, blocks_hbm, out_ref,
    held, cur, ray_hot, ray_turned, tile_hot, tile_turned, x, y, picked, total, part, got, fresh, full,
    own, pair, beside, across, onward,
    load, sems, send1, recv1, send2, recv2, ready,
    send_beside, recv_beside, send_across, recv_across, send_onward, recv_onward,
):
    agent = lax.axis_index("agent")
    me = lax.axis_index("tile")
    count, slices = plan
    chunks, height, columns = own.shape
    local = chunks * height // slices
    detectors = columns // LANES
    rays_here = fresh.shape[2]
    ray_total = count * rays_here
    tiles_here = detectors * local
    blocks_here = held.shape[0]
    order = list(range(count - 1, 0, -1))
    core = agent % 2
    neighbour = agent + 1 - 2 * core
    opposite = (agent + 2) % 4
    state = pltpu.make_async_copy(cur_hbm, cur, load.at[0])
    state.start()

    def send(source, target, s, r, k, to):
        return pltpu.make_async_remote_copy(
            src_ref=source.at[k], dst_ref=target.at[k], send_sem=s.at[k], recv_sem=r.at[k],
            device_id=(to, me), device_id_type=MESH,
        )

    def to_beside(k):
        return send(own, beside, send_beside, recv_beside, k, neighbour)

    def to_across(source, k):
        return send(source, across, send_across, recv_across, k, opposite)

    def to_onward(k):
        return send(across, onward, send_onward, recv_onward, k, neighbour)

    def rows_of(k):
        return slice(k * height, (k + 1) * height)

    width = slices // 2 * LANES

    def columns_of(h):
        return slice(h * width, (h + 1) * width)

    def part_copy(step, h, d):
        return pltpu.make_async_remote_copy(
            src_ref=part.at[step, h, swap_bits(me, d)],
            dst_ref=got.at[step, h, d],
            send_sem=send1.at[step, h, d],
            recv_sem=recv1.at[step, h, d],
            device_id=(agent, swap_bits(me, d)),
            device_id_type=MESH,
        )

    def rest_copy(step, h, d):
        return pltpu.make_async_remote_copy(
            src_ref=fresh.at[step, h],
            dst_ref=full.at[step, h, me],
            send_sem=send2.at[step, h, d],
            recv_sem=recv2.at[step, h, d],
            device_id=(agent, swap_bits(me, d)),
            device_id_type=MESH,
        )

    def exchange(step, barrier):
        for h in range(2):
            total[h] = scatter_rows(ray_hot[...], y[:, columns_of(h)])
            for slot in range(count):
                part[step, h, slot] = total[h, slot * rays_here:(slot + 1) * rays_here, :].astype(BF)
            if step == 0 and h == 0:
                pl.semaphore_wait(barrier, count - 1)
            for d in order:
                part_copy(step, h, d).start()
        for h in range(2):
            value = total[h, pl.ds(pl.multiple_of(me * rays_here, 8), rays_here), :]
            measured = [
                sino_ref[pl.ds(h * (slices // 2) + z, rays_here, stride=slices), :] for z in range(slices // 2)
            ]
            value = value - jnp.concatenate(measured, axis=1)
            for d in reversed(order):
                part_copy(step, h, d).wait_recv()
                value = value + got[step, h, d].astype(F32)
            fresh[step, h] = value.astype(BF)
            for d in order:
                rest_copy(step, h, d).start()
            full[step, h, me] = fresh[step, h]
        for h in range(2):
            for d in order:
                rest_copy(step, h, d).wait_recv()
            picked[:, columns_of(h)] = gather_rows(ray_turned[...], full[step, h].reshape(ray_total, width))

    def exchanged(step):
        for h in range(2):
            for d in order:
                part_copy(step, h, d).wait_send()
                rest_copy(step, h, d).wait_send()

    middle = chunks // 2

    def half_of(side):
        return range(side * middle, chunks if side else middle)

    def last_update(side):
        first, count_here = side * (slices // 2), slices // 2 if side == 0 else slices - slices // 2
        at = slice(first * LANES, (first + count_here) * LANES)
        moved = x[:, at] - 0.8 * scatter_rows(tile_hot[...], y[:, at])
        for z in range(count_here):
            for t in range(detectors):
                place = (slice((first + z) * local, (first + z + 1) * local), slice(t * LANES, (t + 1) * LANES))
                piece = moved[t * local:(t + 1) * local, z * LANES:(z + 1) * LANES]
                out_ref[place] = 2.0 * piece - cur[place]

    def finish(k, base, others):
        out_ref[rows_of(k), :] = 2.0 * cur[rows_of(k), :] - base[rows_of(k), :] + others

    def low_part(side, base):
        mine, rest = half_of(side), half_of(1 - side)
        for part_of in (rest, mine):
            if side == 0:
                last_update(0 if part_of is mine else 1)
                for k in part_of:
                    own[k] = out_ref[rows_of(k), :].astype(BF)
                if part_of is rest:
                    pl.semaphore_wait(ready.at[0], 2)
            for k in part_of:
                to_beside(k).start()
        for k in mine:
            to_beside(k).wait_recv()
            pair[k] = (own[k].astype(F32) + beside[k].astype(F32)).astype(BF)
            to_across(pair, k).start()
        for part_of in (mine, rest):
            for k in part_of:
                if part_of is rest:
                    to_beside(k).wait_recv()
                to_across(pair, k).wait_recv()
                finish(k, base, beside[k].astype(F32) + across[k].astype(F32))
        for k in range(chunks):
            to_beside(k).wait_send()
        for k in mine:
            to_across(pair, k).wait_send()

    def high_part(side):
        mine, rest = half_of(side), half_of(1 - side)
        for k in range(chunks):
            to_beside(k).start()
        for k in range(chunks):
            to_beside(k).wait_recv()
            pair[k] = (own[k].astype(F32) + beside[k].astype(F32)).astype(BF)
            to_across(pair, k).start()
        for k in mine:
            to_across(pair, k).wait_recv()
            to_onward(k).start()
            finish(k, reflect_ref, beside[k].astype(F32) + across[k].astype(F32))
        for k in rest:
            to_onward(k).wait_recv()
            finish(k, reflect_ref, beside[k].astype(F32) + onward[k].astype(F32))
        for k in range(chunks):
            to_beside(k).wait_send()
            to_across(pair, k).wait_send()
        for k in mine:
            to_onward(k).wait_send()

    @pl.when(agent == 0)
    def _():
        barrier = pltpu.get_barrier_semaphore()
        for d in order:
            pl.semaphore_signal(barrier, inc=1, device_id=(agent, swap_bits(me, d)), device_id_type=MESH)
        for peer in (neighbour, opposite):
            pl.semaphore_signal(barrier, inc=1, device_id=(peer, me), device_id_type=MESH)
        for i in range(min(DEPTH, blocks_here // CHUNK)):
            block_copy(blocks_hbm, held, sems, i).start()

        hot_rows = lax.broadcasted_iota(jnp.int32, (ray_total, blocks_here), 0)
        ray = angle_ref[...] * detectors + detector_ref[...]
        hot = jnp.where(hot_rows == jnp.broadcast_to(ray, hot_rows.shape), 1.0, 0.0)
        ray_hot[...] = hot.astype(BF)
        ray_turned[...] = hot.T.astype(BF)
        hot_rows = lax.broadcasted_iota(jnp.int32, (tiles_here, blocks_here), 0)
        place = tile_ref[...]
        place = (place % detectors) * local + place // detectors
        hot = jnp.where(hot_rows == jnp.broadcast_to(place, hot_rows.shape), 1.0, 0.0)
        tile_hot[...] = hot.astype(BF)
        tile_turned[...] = hot.T.astype(BF)

        state.wait()
        for z in range(slices):
            for t in range(detectors):
                x[t * local:(t + 1) * local, z * LANES:(z + 1) * LANES] = cur[z * local:(z + 1) * local, t * LANES:(t + 1) * LANES]

        for step in range(DATA_STEPS):
            picked[...] = gather_rows(tile_turned[...], x[...].astype(BF))
            block_sweep(blocks_hbm, held, sems, picked, y, slices, True, step == 0)
            exchange(step, barrier)
            block_sweep(blocks_hbm, held, sems, picked, y, slices, False, False)
            exchanged(step)
            if step < DATA_STEPS - 1:
                x[...] = x[...] - 0.8 * scatter_rows(tile_hot[...], y[...])

        low_part(0, out_ref)

    @pl.when(agent != 0)
    def _():
        barrier = pltpu.get_barrier_semaphore()

        @pl.when(agent != 1)
        def _():
            pl.semaphore_signal(barrier, inc=1, device_id=(neighbour, me), device_id_type=MESH)

        @pl.when(agent != 2)
        def _():
            pl.semaphore_signal(barrier, inc=1, device_id=(opposite, me), device_id_type=MESH)

        for k in range(chunks):
            own[k] = reflect_ref[rows_of(k), :].astype(BF)
        state.wait()
        pl.semaphore_wait(barrier, 2)

        @pl.when(agent != 3)
        def _():
            pl.semaphore_signal(ready.at[0], inc=1, device_id=(0, me), device_id_type=MESH)

        @pl.when(agent == 1)
        def _():
            low_part(1, reflect_ref)

        @pl.when(agent == 2)
        def _():
            high_part(0)

        @pl.when(agent == 3)
        def _():
            high_part(1)


def idle_kernel(out_ref):
    pass


def join(angle, detector, tile, sinogram, reflect, current, blocks, count):
    slices, local, columns = current.shape
    rays_here = sinogram.shape[0]
    ray_total = rays_here * count
    tiles_here = columns // LANES * local
    blocks_here = blocks.shape[0]
    width = slices * LANES
    rows = slices * local
    chunks = max(2, rows // 32)
    chunk = (chunks, rows // chunks, columns)
    vmem = pl.BlockSpec(memory_space=pltpu.VMEM)
    anywhere = pl.BlockSpec(memory_space=pl.ANY)
    out = pl.pallas_call(
        functools.partial(join_kernel, (count, slices)),
        out_shape=pltpu.VMEM((rows, columns), F32),
        in_specs=[vmem] * 5 + [anywhere] * 2,
        out_specs=vmem,
        scratch_shapes=[
            pltpu.VMEM(blocks.shape, BF),
            pltpu.VMEM((rows, columns), F32),
            pltpu.VMEM((ray_total, blocks_here), BF),
            pltpu.VMEM((blocks_here, ray_total), BF),
            pltpu.VMEM((tiles_here, blocks_here), BF),
            pltpu.VMEM((blocks_here, tiles_here), BF),
            pltpu.VMEM((tiles_here, width), F32),
            pltpu.VMEM((blocks_here, width), F32),
            pltpu.VMEM((blocks_here, width), F32),
            pltpu.VMEM((2, ray_total, width // 2), F32),
            pltpu.VMEM((DATA_STEPS, 2, count, rays_here, width // 2), BF),
            pltpu.VMEM((DATA_STEPS, 2, count, rays_here, width // 2), BF),
            pltpu.VMEM((DATA_STEPS, 2, rays_here, width // 2), BF),
            pltpu.VMEM((DATA_STEPS, 2, count, rays_here, width // 2), BF),
        ]
        + [pltpu.VMEM(chunk, BF)] * 5
        + [pltpu.SemaphoreType.DMA((1,)), pltpu.SemaphoreType.DMA((blocks_here // CHUNK,))]
        + [pltpu.SemaphoreType.DMA((DATA_STEPS, 2, count))] * 4
        + [pltpu.SemaphoreType.REGULAR((1,))]
        + [pltpu.SemaphoreType.DMA((chunks,))] * 6,
        compiler_params=pltpu.CompilerParams(
            collective_id=0, has_side_effects=True, vmem_limit_bytes=58 * 1024 * 1024
        ),
        name="join_agents",
    )(
        angle.reshape(1, -1), detector.reshape(1, -1), tile.reshape(1, -1),
        sinogram.reshape(rays_here * slices, LANES), reflect.reshape(rows, columns),
        current.reshape(rows, columns), blocks,
    )
    return out.reshape(current.shape)


def per_device(
    states,
    sinogram,
    blocks,
    block_angle,
    block_detector,
    block_tile,
    conv_first,
    conv_hidden,
    conv_last,
):
    current = states[0]
    agent_place = lax.axis_index("agent")
    halo = conv_hidden.shape[1] + 2
    filters = (conv_first, conv_hidden, conv_last)
    edges = halo_exchange(current, halo)

    def data_only():
        return pl.pallas_call(
            idle_kernel,
            out_shape=jax.ShapeDtypeStruct(current.shape, F32),
            out_specs=pl.BlockSpec(memory_space=pl.ANY),
            name="idle",
        )()

    def axial_only():
        return axial_reflect(edges, current, *filters, halo)

    def sagittal_only():
        return plane_call(1, edges, current, *filters, halo, 1)

    def coronal_only():
        return coronal_reflect(current, *filters)

    reflect = lax.switch(agent_place, [data_only, axial_only, sagittal_only, coronal_only])
    joined = join(
        block_angle, block_detector, block_tile, sinogram, reflect, current, blocks, lax.axis_size("tile")
    )
    return (0.25 * joined)[None]


def solution(mesh):
    placed = (
        P("agent", None, "tile", None),
        P("tile", None, None),
        P("tile", None, None),
        P("tile"),
        P("tile"),
        P("tile"),
        P(),
        P(),
        P(),
    )
    return jax.shard_map(
        per_device,
        mesh=mesh,
        in_specs=placed,
        out_specs=P("agent", None, "tile", None),
        check_vma=False,
    )
```

```python
import functools

import jax
import jax.numpy as jnp
from jax import lax
from jax.experimental import pallas as pl
from jax.experimental.pallas import tpu as pltpu
from jax.sharding import PartitionSpec as P

DATA_STEPS = 2
MESH = pl.DeviceIdType.MESH
LANES = 128
STRIPS = 16
CHUNK = 96
DEPTH = 2
BF = jnp.bfloat16
F32 = jnp.float32
NATURAL = (0, 1, 2, 3)
EVEN_ORDER = (0, 1, 2, 3)
ODD_ORDER = (1, 0, 3, 2)


def main_cells(offset):
    order = EVEN_ORDER if offset % 2 else ODD_ORDER
    return [(offset, column) for column in order]

def edge_cells(offset):
    return [(offset + 1, 4), (offset, 4), (offset, -1), (offset + 1, -1)]

def window_cells(rows):
    tiles = [main_cells(a) for a in range(rows + 2)]
    return tiles + [edge_cells(a) for a in range(0, rows + 2, 2)]

def spread_lanes(w):
    return jnp.concatenate([w] * (LANES // w.shape[-1]), axis=-1)

def lane_iota(rows):
    return lax.broadcasted_iota(jnp.int32, (rows, LANES), 1)

def slot_mix(rows, taps, column_in, order, width):
    slot = lane_iota(rows) // width
    mixed = jnp.zeros((rows, LANES), F32)
    for place, column in enumerate(order):
        tap = column_in - column + 1
        if 0 <= tap < 3:
            mixed = jnp.where(slot == place, taps[tap], mixed)
    return mixed

def build_first(w_ref, o, w1):
    for k in range(6):
        for half in range(2):
            order = ODD_ORDER if half else EVEN_ORDER
            mixes = []
            for ti in range(3):
                taps = [jnp.broadcast_to(spread_lanes(w_ref[o, ti, tj:tj+1, :].astype(F32)), (16, LANES)) for tj in range(3)]
                mixes.append(slot_mix(16, taps, k - 1, order, 32))
            row = lax.broadcasted_iota(jnp.int32, (16, LANES), 0)
            for t in range(4):
                value = jnp.zeros((16, LANES), F32)
                for ti in range(3):
                    value = jnp.where(row == 2 * t + half + ti, mixes[ti], value)
                at = t * 2 * LANES + half * LANES
                w1[k * 16:(k + 1) * 16, at:at + LANES] = value.astype(BF)

def build_hidden(w_ref, o, layer, wh):
    wide = [[spread_lanes(w_ref[o, layer, ti, tj].astype(F32)) for tj in range(3)] for ti in range(3)]
    inner = wide[0][0].shape[0]
    for n, tile in enumerate(window_cells(2)):
        for slot, (a, column) in enumerate(tile):
            at = n * LANES + slot * inner
            for half in range(2):
                ti = a - (half + 1) + 1
                if 0 <= ti < 3:
                    value = slot_mix(inner, wide[ti], column, ODD_ORDER if half else EVEN_ORDER, inner)
                else:
                    value = jnp.zeros((inner, LANES), F32)
                wh[layer, at:at + inner, half * LANES:(half + 1) * LANES] = value.astype(BF)

def column_of(row):
    inner = row.shape[1]
    r = lax.broadcasted_iota(jnp.int32, (inner, inner), 0)
    c = lax.broadcasted_iota(jnp.int32, (inner, inner), 1)
    picked = jnp.where(r == c, jnp.broadcast_to(row, (inner, inner)), 0.0)
    return jnp.broadcast_to(jnp.sum(picked, axis=1, keepdims=True), (inner, LANES))

def build_last(w_ref, o, wl):
    taps = [[column_of(w_ref[o, ti, tj:tj+1, :].astype(F32)) for tj in range(3)] for ti in range(3)]
    inner = taps[0][0].shape[0]
    lane = lane_iota(inner)
    row8 = lane % 8
    zero = jnp.zeros((inner, LANES), F32)
    rows = []
    for a in range(10):
        line = []
        for tj in range(3):
            value = zero
            for ti in range(3):
                if 0 <= a - ti < 8:
                    value = jnp.where(row8 == a - ti, taps[ti][tj], value)
            line.append(value)
        rows.append(line)
    for n, tile in enumerate(window_cells(8)):
        for slot, (a, column) in enumerate(tile):
            at = n * LANES + slot * inner
            wl[at:at + inner, :] = slot_mix(inner, rows[a], column, EVEN_ORDER, LANES // 4).astype(BF)


def axial_kernel(plan, edges_ref, cur_ref, cf_ref, ch_ref, cl_ref, out_ref, main, edge, w1, wh, wl, raw, xs, place, back, gathered_out):
    halo = plan
    slices, local, columns = cur_ref.shape
    rows = local + 2 * halo
    stored = rows + 8
    groups = columns // 4
    per = groups // STRIPS
    span = slices * groups
    layers = ch_ref.shape[1]
    tile = lax.axis_index("tile")
    at_start = tile == 0
    at_end = tile == lax.axis_size("tile") - 1
    fill_rows(raw, edges_ref, cur_ref, stored, halo)

    build_first(cf_ref, 0, w1)
    for layer in range(layers):
        build_hidden(ch_ref, 0, layer, wh)
    build_last(cl_ref, 0, wl)

    col = lax.broadcasted_iota(jnp.int32, (columns, groups), 0)
    m = lax.broadcasted_iota(jnp.int32, (columns, groups), 1)
    first_col = 4 * ((m % STRIPS) * per + m // STRIPS)
    for k in range(6):
        place[:, k * groups:(k + 1) * groups] = jnp.where(col == first_col + (k - 1), 1.0, 0.0).astype(BF)
    m = lax.broadcasted_iota(jnp.int32, (groups, columns), 0)
    col = lax.broadcasted_iota(jnp.int32, (groups, columns), 1)
    first_col = 4 * ((m % STRIPS) * per + m // STRIPS)
    for k in range(4):
        back[k * groups:(k + 1) * groups, :] = jnp.where(col == first_col + k, 1.0, 0.0).astype(BF)
    xs[...] = jnp.dot(raw[...].astype(BF), place[...], preferred_element_type=F32)

    slot = lane_iota(STRIPS) // (LANES // 4)
    even_slots = (slot == 0) | (slot == 3)
    right_slots = slot < 2
    strip = lax.broadcasted_iota(jnp.int32, (STRIPS, LANES), 0)
    zero_tile = jnp.zeros((slices, per, STRIPS, LANES), BF)

    for side in range(2):
        for r in (0, 1, 2, rows - 1, rows, rows + 1):
            main[side, r] = zero_tile
        for e in (0, 1, rows // 2 - 1, rows // 2):
            edge[side, e] = zero_tile

    def put_edge(side, e, odd_row, even_row):
        v = jnp.where(even_slots, even_row, odd_row)
        for z in range(slices):
            for i in range(per):
                if i + 1 < per:
                    right = v[z, i + 1]
                else:
                    right = jnp.where(strip == STRIPS - 1, 0.0, pltpu.roll(v[z, 0], STRIPS - 1, 0))
                if i > 0:
                    left = v[z, i - 1]
                else:
                    left = jnp.where(strip == 0, 0.0, pltpu.roll(v[z, per - 1], 1, 0))
                edge[side, e, z, i] = jnp.where(right_slots, right, left).astype(BF)

    def put_pairs(side, pair, count, y):
        before = main[side, 2 * pair].astype(F32)
        for t in range(count):
            row = 2 * (pair + t)
            v = jnp.maximum(y(t), 0.0)
            if not isinstance(row, int):
                outside = (at_start & (row < halo)) | (at_end & (row >= rows - halo))
                v = v * jnp.where(outside, 0.0, 1.0)
            elif row < halo:
                v = v * jnp.where(at_start, 0.0, 1.0)
            elif row >= rows - halo:
                v = v * jnp.where(at_end, 0.0, 1.0)
            even_row = v[:, :LANES].reshape(slices, per, STRIPS, LANES)
            odd_row = v[:, LANES:].reshape(slices, per, STRIPS, LANES)
            main[side, row + 1] = even_row.astype(BF)
            main[side, row + 2] = odd_row.astype(BF)
            put_edge(side, pair + t, before, even_row)
            before = odd_row

    def first_step(c):
        parts = []
        for z in range(slices):
            at = pl.ds(z * stored + 8 * c, 16)
            parts.append(jnp.concatenate([xs[at, k * groups:(k + 1) * groups] for k in range(6)], axis=0).astype(BF))
        x = jnp.concatenate(parts, axis=1)
        y = lax.dot_general(x, w1[...], (((0,), (0,)), ((), ())), preferred_element_type=F32)
        put_pairs(0, 4 * c, 4, lambda t: y[:, t * 2 * LANES:(t + 1) * 2 * LANES])

    for c in range(rows // 8):
        first_step(c)

    def window(side, pair, out_rows):
        parts = [main[side, 2 * pair + a].reshape(span, LANES) for a in range(out_rows + 2)]
        parts += [edge[side, pair + e].reshape(span, LANES) for e in range(out_rows // 2 + 1)]
        return jnp.concatenate(parts, axis=1)

    pairs = rows // 2 - 2
    run = max(n for n in range(1, 18) if pairs % n == 0)
    for layer in range(layers):
        source, target = layer % 2, (layer + 1) % 2

        def hidden_steps(c, carry):
            for j in range(run):
                pair = 1 + c * run + j
                y = jnp.dot(window(source, pair, 2), wh[layer], preferred_element_type=F32)
                put_pairs(target, pair, 1, lambda t: y)
            return carry

        lax.fori_loop(0, pairs // run, hidden_steps, 0)
        end = rows // 2 - 1
        put_edge(target, end, main[target, 2 * end].astype(F32), jnp.zeros((slices, per, STRIPS, LANES), F32))

    eighths = local // 8
    quad = (lane_iota(span) // 8) % 4

    four = 4 if eighths % 4 == 0 else eighths

    def last_steps(c, carry):
        value = jnp.zeros((span, LANES), F32)
        for j in range(four):
            x = window(layers % 2, halo // 2 + 4 * (c * four + j), 8)
            y = jnp.dot(x, wl[...], preferred_element_type=F32)
            value = jnp.where(quad == j, y, value)
        gathered_out[c] = value
        return carry

    lax.fori_loop(0, eighths // four, last_steps, 0)

    for big in range(gathered_out.shape[0]):
        height = min(32, local - 32 * big)
        turned = [gathered_out[big, z * groups:(z + 1) * groups, :].T for z in range(slices)]
        lines = [jnp.concatenate([turned[z][k * 32:(k + 1) * 32] for k in range(4)], axis=1) for z in range(slices)]
        values = jnp.concatenate(lines, axis=0)
        high = values.astype(BF)
        low = (values - high.astype(F32)).astype(BF)
        net = jnp.dot(high, back[...], preferred_element_type=F32) + jnp.dot(low, back[...], preferred_element_type=F32)
        for z in range(slices):
            at = pl.ds(32 * big, height)
            out_ref[z, at, :] = cur_ref[z, at, :] - 2.0 * net[z * 32:z * 32 + height]

def axial_reflect(edges, current, cf, ch, cl, halo):
    slices, local, columns = current.shape
    rows = local + 2 * halo
    groups = columns // 4
    per = groups // STRIPS
    stored = rows + 8
    whole = pl.BlockSpec(memory_space=pltpu.VMEM)
    return pl.pallas_call(
        functools.partial(axial_kernel, halo),
        out_shape=jax.ShapeDtypeStruct(current.shape, F32),
        in_specs=[whole] * 5,
        out_specs=whole,
        scratch_shapes=[
            pltpu.VMEM((2, rows + 2, slices, per, STRIPS, LANES), BF),
            pltpu.VMEM((2, rows // 2 + 1, slices, per, STRIPS, LANES), BF),
            pltpu.VMEM((96, 8 * LANES), BF),
            pltpu.VMEM((ch.shape[1], 6 * LANES, 2 * LANES), BF),
            pltpu.VMEM((15 * LANES, LANES), BF),
            pltpu.VMEM((slices * stored, columns), F32),
            pltpu.VMEM((slices * stored, 6 * groups), F32),
            pltpu.VMEM((columns, 6 * groups), BF),
            pltpu.VMEM((4 * groups, columns), BF),
            pltpu.VMEM((-(-local // 32), slices * groups, LANES), F32),
        ],
        compiler_params=pltpu.CompilerParams(vmem_limit_bytes=60 * 1024 * 1024),
        name="net_axial",
    )(edges, current, cf, ch, cl)


def fill_rows(raw, edges_ref, cur_ref, stored, halo):
    slices, local, columns = cur_ref.shape
    zero = jnp.zeros((1, columns), F32)
    tail = jnp.zeros((stored - 1 - local - 2 * halo, columns), F32)
    for z in range(slices):
        above = edges_ref[0, z * halo:(z + 1) * halo, :].astype(F32)
        below = edges_ref[1, z * halo:(z + 1) * halo, :].astype(F32)
        raw[z * stored:(z + 1) * stored, :] = jnp.concatenate([zero, above, cur_ref[z], below, tail], axis=0)


def build_first_plane(w_ref, o, w1):
    row = lax.broadcasted_iota(jnp.int32, (16, LANES), 0)
    for z in range(4):
        mixes = []
        for tj in range(3):
            taps = [jnp.broadcast_to(spread_lanes(w_ref[o, ti, tj:tj+1, :].astype(F32)), (16, LANES)) for ti in range(3)]
            mixes.append(slot_mix(16, taps, z, NATURAL, 32))
        for t in range(8):
            value = jnp.zeros((16, LANES), F32)
            for tj in range(3):
                value = jnp.where(row == t + tj, mixes[tj], value)
            w1[z * 16:(z + 1) * 16, t * LANES:(t + 1) * LANES] = value.astype(BF)

def build_hidden_plane(w_ref, o, layer, wh):
    wide = [[spread_lanes(w_ref[o, layer, ti, tj].astype(F32)) for ti in range(3)] for tj in range(3)]
    inner = wide[0][0].shape[0]
    for a in range(4):
        for z in range(4):
            at = a * LANES + z * inner
            for half in range(2):
                if 0 <= a - half < 3:
                    value = slot_mix(inner, wide[a - half], z, NATURAL, inner)
                else:
                    value = jnp.zeros((inner, LANES), F32)
                wh[layer, at:at + inner, half * LANES:(half + 1) * LANES] = value.astype(BF)

def build_last_plane(w_ref, o, wl):
    taps = [[column_of(w_ref[o, ti, tj:tj+1, :].astype(F32)) for ti in range(3)] for tj in range(3)]
    inner = taps[0][0].shape[0]
    row8 = lane_iota(inner) % 8
    zero = jnp.zeros((inner, LANES), F32)
    for a in range(10):
        line = []
        for ti in range(3):
            value = zero
            for tj in range(3):
                if 0 <= a - tj < 8:
                    value = jnp.where(row8 == a - tj, taps[tj][ti], value)
            line.append(value)
        for z in range(4):
            at = a * LANES + z * inner
            wl[at:at + inner, :] = slot_mix(inner, line, z, NATURAL, LANES // 4).astype(BF)


def plane_kernel(plan, x_ref, cur_ref, cf_ref, ch_ref, cl_ref, out_ref, main, w1, wh, wl, xs, gathered_out):
    o, halo, chunk, strips = plan
    slices, local, span = out_ref.shape
    rows = local + 2 * halo
    stored = rows + 8
    layers = ch_ref.shape[1]
    if halo:
        tile = lax.axis_index("tile")
        at_start = tile == 0
        at_end = tile == lax.axis_size("tile") - 1

    build_first_plane(cf_ref, o, w1)
    for layer in range(layers):
        build_hidden_plane(ch_ref, o, layer, wh)
    build_last_plane(cl_ref, o, wl)
    if halo:
        fill_rows(xs, x_ref, cur_ref, stored, halo)
    else:
        xs[...] = x_ref[...].astype(F32)
    for side in range(2):
        for r in (0, rows + 1):
            main[side, r] = jnp.zeros((span, LANES), BF)

    def put_pairs(side, pair, count, y):
        for t in range(count):
            row = 2 * (pair + t)
            v = jnp.maximum(y(t), 0.0)
            if halo:
                outside = (at_start & (row < halo)) | (at_end & (row >= rows - halo))
                v = v * jnp.where(outside, 0.0, 1.0)
            main[side, row + 1] = v[:, :LANES].astype(BF)
            main[side, row + 2] = v[:, LANES:].astype(BF)

    def ends(side):
        if strips > 1:
            step = span // strips
            main[side, 0, step:span] = main[side, rows, 0:span - step]
            main[side, rows + 1, 0:span - step] = main[side, 1, step:span]

    def first_step(c, carry):
        parts = [xs[pl.ds(pl.multiple_of(z * stored + 8 * c, 8), 16)] for z in range(slices)]
        x = jnp.concatenate(parts, axis=0).astype(BF)
        y = lax.dot_general(x, w1[...], (((0,), (0,)), ((), ())), preferred_element_type=F32)
        put_pairs(0, 4 * c, 4, lambda t: y[:, t * 2 * LANES:(t + 1) * 2 * LANES])
        return carry

    lax.fori_loop(0, rows // 8, first_step, 0)
    ends(0)

    for layer in range(layers):
        source, target = layer % 2, (layer + 1) % 2

        def hidden_step(c, carry):
            pair = c * chunk
            tiles = [main[source, 2 * pair + a] for a in range(2 * chunk + 2)]
            x = jnp.concatenate([jnp.concatenate(tiles[2 * t:2 * t + 4], axis=1) for t in range(chunk)], axis=0)
            y = jnp.dot(x, wh[layer], preferred_element_type=F32)
            put_pairs(target, pair, chunk, lambda t: y[t * span:(t + 1) * span])
            return carry

        lax.fori_loop(0, rows // 2 // chunk, hidden_step, 0)
        ends(target)

    quad = (lane_iota(span) // 8) % 4

    def last_step(q, carry):
        x = jnp.concatenate([main[layers % 2, halo + 8 * q + a] for a in range(10)], axis=1)
        y = jnp.dot(x, wl[...], preferred_element_type=F32)
        gathered_out[q // 4] = jnp.where(quad == q % 4, y, gathered_out[q // 4])
        return carry

    gathered_out[...] = jnp.zeros_like(gathered_out)
    lax.fori_loop(0, local // 8, last_step, 0)
    for big in range(gathered_out.shape[0]):
        height = min(32, local - 32 * big)
        net = gathered_out[big].T
        for z in range(slices):
            at = pl.ds(32 * big, height)
            out_ref[z, at, :] = cur_ref[z, at, :] - 2.0 * net[z * 32:z * 32 + height]

def plane_call(o, x, current, cf, ch, cl, halo, strips):
    slices, local, span = current.shape
    rows = local + 2 * halo
    whole = pl.BlockSpec(memory_space=pltpu.VMEM)
    return pl.pallas_call(
        functools.partial(plane_kernel, (o, halo, 4, strips)),
        out_shape=jax.ShapeDtypeStruct(current.shape, F32),
        in_specs=[whole] * 5, out_specs=whole,
        scratch_shapes=[
            pltpu.VMEM((2, rows + 2, span, LANES), BF),
            pltpu.VMEM((64, 8 * LANES), BF),
            pltpu.VMEM((ch.shape[1], 4 * LANES, 2 * LANES), BF),
            pltpu.VMEM((10 * LANES, LANES), BF),
            pltpu.VMEM((slices * (rows + 8), span), F32),
            pltpu.VMEM((-(-local // 32), span, LANES), F32),
        ],
        compiler_params=pltpu.CompilerParams(vmem_limit_bytes=60 * 1024 * 1024),
        name="net_sagittal" if halo else "net_coronal",
    )(x, current, cf, ch, cl)

def coronal_reflect(current, cf, ch, cl):
    slices, local, columns = current.shape
    strips = columns // local
    turned = jnp.transpose(current.reshape(slices, local, strips, local), (0, 3, 2, 1))
    t = turned.astype(BF)
    none = jnp.zeros((slices, 1, 1, local), BF)
    before = jnp.concatenate([none, t[:, -1:, :-1]], axis=2)
    after = jnp.concatenate([t[:, :1, 1:], none], axis=2)
    rest = jnp.zeros((slices, 6, strips, local), BF)
    x = jnp.concatenate([before, t, after, rest], axis=1)
    x = x.reshape(-1, columns)
    out = plane_call(2, x, turned.reshape(slices, local, columns), cf, ch, cl, 0, strips)
    return jnp.transpose(out.reshape(slices, local, strips, local), (0, 3, 2, 1)).reshape(current.shape)

def halo_kernel(halo, cur_hbm, out_ref, edge, sent, load, send, recv):
    agent = lax.axis_index("agent")
    tile = lax.axis_index("tile")
    last = lax.axis_size("tile") - 1
    slices, local, columns = cur_hbm.shape
    rows = edge.shape[2]
    active = (agent == 1) | (agent == 2)

    def copy(side, peer):
        return pltpu.make_async_remote_copy(
            src_ref=sent.at[side],
            dst_ref=out_ref.at[1 - side],
            send_sem=send.at[side],
            recv_sem=recv.at[1 - side],
            device_id=(agent, peer),
            device_id_type=MESH,
        )

    @pl.when(active)
    def _():
        barrier = pltpu.get_barrier_semaphore()

        @pl.when(tile > 0)
        def _():
            pl.semaphore_signal(barrier, inc=1, device_id=(agent, tile - 1), device_id_type=MESH)

        @pl.when(tile < last)
        def _():
            pl.semaphore_signal(barrier, inc=1, device_id=(agent, tile + 1), device_id_type=MESH)

        loads = [
            pltpu.make_async_copy(cur_hbm.at[:, pl.ds(0, rows)], edge.at[0], load.at[0]),
            pltpu.make_async_copy(cur_hbm.at[:, pl.ds(local - rows, rows)], edge.at[1], load.at[1]),
        ]
        for item in loads:
            item.start()
        for item in loads:
            item.wait()
        for side in range(2):
            first = 0 if side == 0 else rows - halo
            parts = [edge[side, z, first:first + halo, :] for z in range(slices)]
            sent[side] = jnp.concatenate(parts, axis=0).astype(BF)

        pl.semaphore_wait(barrier, jnp.where(tile > 0, 1, 0) + jnp.where(tile < last, 1, 0))

        @pl.when(tile > 0)
        def _():
            copy(0, tile - 1).start()

        @pl.when(tile < last)
        def _():
            copy(1, tile + 1).start()

        @pl.when(tile == 0)
        def _():
            out_ref[0] = jnp.zeros(out_ref.shape[1:], BF)

        @pl.when(tile == last)
        def _():
            out_ref[1] = jnp.zeros(out_ref.shape[1:], BF)

        @pl.when(tile > 0)
        def _():
            copy(1, tile - 1).wait_recv()

        @pl.when(tile < last)
        def _():
            copy(0, tile + 1).wait_recv()

        @pl.when(tile > 0)
        def _():
            copy(0, tile - 1).wait_send()

        @pl.when(tile < last)
        def _():
            copy(1, tile + 1).wait_send()


def halo_exchange(current, halo):
    slices, local, columns = current.shape
    return pl.pallas_call(
        functools.partial(halo_kernel, halo),
        out_shape=jax.ShapeDtypeStruct((2, slices * halo, columns), BF),
        in_specs=[pl.BlockSpec(memory_space=pl.ANY)],
        out_specs=pl.BlockSpec(memory_space=pltpu.VMEM),
        scratch_shapes=[
            pltpu.VMEM((2, slices, 8, columns), F32),
            pltpu.VMEM((2, slices * halo, columns), BF),
            pltpu.SemaphoreType.DMA((2,)),
            pltpu.SemaphoreType.DMA((2,)),
            pltpu.SemaphoreType.DMA((2,)),
        ],
        compiler_params=pltpu.CompilerParams(collective_id=2, has_side_effects=True),
        name="halo_exchange",
    )(current)


def swap_bits(me, d):
    peer, bit = me, 1
    while bit <= d:
        if d & bit:
            peer = peer + bit * (1 - 2 * ((me // bit) % 2))
        bit *= 2
    return peer


def block_copy(blocks_hbm, held, sems, i):
    at = pl.ds(i * CHUNK, min(CHUNK, held.shape[0] - i * CHUNK))
    return pltpu.make_async_copy(blocks_hbm.at[at], held.at[at], sems.at[i])


def block_step(held, picked, y, slices, transposed, u):
    row = lax.broadcasted_iota(jnp.int32, (8, LANES), 0)
    upper, even = row < 4, row % 2 == 0
    at = pl.ds(pl.multiple_of(8 * u, 8), 8)

    def turned(v):
        return pltpu.roll(v, 4, 0)

    rows = [[], []]
    for z in range(0, slices, 2):
        v, w = (picked[at, (z + i) * LANES:(z + i + 1) * LANES] for i in range(2))
        rows[0].append(jnp.where(upper, v, turned(w)))
        rows[1].append(jnp.where(upper, turned(v), w))
    outs = []
    for t in range(2):
        sides = [
            jnp.concatenate([jnp.where(row % 4 // 2 == side, v, 0.0) for v in rows[t]], axis=0) for side in range(2)
        ]
        lhs = jnp.concatenate(sides, axis=1).astype(BF)
        m = [held[8 * u + 4 * t + j] for j in range(4)]
        if transposed:
            top, bottom = jnp.concatenate([m[0], m[2]], axis=1), jnp.concatenate([m[1], m[3]], axis=1)
            dims = (((1,), (1,)), ((), ()))
        else:
            top, bottom = jnp.concatenate([m[0], m[1]], axis=1), jnp.concatenate([m[2], m[3]], axis=1)
            dims = (((1,), (0,)), ((), ()))
        rhs = jnp.concatenate([top, bottom], axis=0)
        out = lax.dot_general(lhs, rhs, dims, preferred_element_type=F32)
        outs.append(jnp.where(jnp.concatenate([even] * (slices // 2), axis=0), out[:, :LANES], out[:, LANES:]))
    for z in range(0, slices, 2):
        v, w = (o[4 * z:4 * z + 8] for o in outs)
        y[at, z * LANES:(z + 1) * LANES] = jnp.where(upper, v, turned(w))
        y[at, (z + 1) * LANES:(z + 2) * LANES] = jnp.where(upper, turned(v), w)


def block_sweep(blocks_hbm, held, sems, picked, y, slices, transposed, waiting):
    pieces = pl.cdiv(held.shape[0], CHUNK)
    for i in range(pieces):
        if waiting:
            block_copy(blocks_hbm, held, sems, i).wait()
            if i + DEPTH < pieces:
                block_copy(blocks_hbm, held, sems, i + DEPTH).start()
        for u in range(i * CHUNK // 8, min((i + 1) * CHUNK, held.shape[0]) // 8):
            block_step(held, picked, y, slices, transposed, u)


def gather_rows(hot, source):
    return jnp.dot(hot, source, preferred_element_type=F32)


def scatter_rows(hot, y):
    high = y.astype(BF)
    low = (y - high.astype(F32)).astype(BF)
    return jnp.dot(
        jnp.concatenate([hot, hot], axis=1), jnp.concatenate([high, low], axis=0), preferred_element_type=F32
    )


def join_kernel(
    plan, angle_ref, detector_ref, tile_ref, sino_ref, reflect_ref, cur_hbm, blocks_hbm, out_ref,
    held, cur, ray_hot, ray_turned, tile_hot, tile_turned, x, y, picked, total, part, got, fresh, full,
    own, pair, beside, across, onward,
    load, sems, send1, recv1, send2, recv2, ready,
    send_beside, recv_beside, send_across, recv_across, send_onward, recv_onward,
):
    agent = lax.axis_index("agent")
    me = lax.axis_index("tile")
    count, slices = plan
    chunks, height, columns = own.shape
    local = chunks * height // slices
    detectors = columns // LANES
    rays_here = fresh.shape[2]
    ray_total = count * rays_here
    tiles_here = detectors * local
    blocks_here = held.shape[0]
    order = list(range(count - 1, 0, -1))
    core = agent % 2
    neighbour = agent + 1 - 2 * core
    opposite = (agent + 2) % 4
    state = pltpu.make_async_copy(cur_hbm, cur, load.at[0])
    state.start()

    def send(source, target, s, r, k, to):
        return pltpu.make_async_remote_copy(
            src_ref=source.at[k], dst_ref=target.at[k], send_sem=s.at[k], recv_sem=r.at[k],
            device_id=(to, me), device_id_type=MESH,
        )

    def to_beside(k):
        return send(own, beside, send_beside, recv_beside, k, neighbour)

    def to_across(source, k):
        return send(source, across, send_across, recv_across, k, opposite)

    def to_onward(k):
        return send(across, onward, send_onward, recv_onward, k, neighbour)

    def rows_of(k):
        return slice(k * height, (k + 1) * height)

    width = slices // 2 * LANES

    def columns_of(h):
        return slice(h * width, (h + 1) * width)

    def part_copy(step, h, d):
        return pltpu.make_async_remote_copy(
            src_ref=part.at[step, h, swap_bits(me, d)],
            dst_ref=got.at[step, h, d],
            send_sem=send1.at[step, h, d],
            recv_sem=recv1.at[step, h, d],
            device_id=(agent, swap_bits(me, d)),
            device_id_type=MESH,
        )

    def rest_copy(step, h, d):
        return pltpu.make_async_remote_copy(
            src_ref=fresh.at[step, h],
            dst_ref=full.at[step, h, me],
            send_sem=send2.at[step, h, d],
            recv_sem=recv2.at[step, h, d],
            device_id=(agent, swap_bits(me, d)),
            device_id_type=MESH,
        )

    def exchange(step, barrier):
        for h in range(2):
            total[h] = scatter_rows(ray_hot[...], y[:, columns_of(h)])
            for slot in range(count):
                part[step, h, slot] = total[h, slot * rays_here:(slot + 1) * rays_here, :].astype(BF)
            if step == 0 and h == 0:
                pl.semaphore_wait(barrier, count - 1)
            for d in order:
                part_copy(step, h, d).start()
        for h in range(2):
            value = total[h, pl.ds(pl.multiple_of(me * rays_here, 8), rays_here), :]
            measured = [
                sino_ref[pl.ds(h * (slices // 2) + z, rays_here, stride=slices), :] for z in range(slices // 2)
            ]
            value = value - jnp.concatenate(measured, axis=1)
            for d in reversed(order):
                part_copy(step, h, d).wait_recv()
                value = value + got[step, h, d].astype(F32)
            fresh[step, h] = value.astype(BF)
            for d in order:
                rest_copy(step, h, d).start()
            full[step, h, me] = fresh[step, h]
        for h in range(2):
            for d in order:
                rest_copy(step, h, d).wait_recv()
            picked[:, columns_of(h)] = gather_rows(ray_turned[...], full[step, h].reshape(ray_total, width))

    def exchanged(step):
        for h in range(2):
            for d in order:
                part_copy(step, h, d).wait_send()
                rest_copy(step, h, d).wait_send()

    middle = chunks // 2

    def half_of(side):
        return range(side * middle, chunks if side else middle)

    def last_update(side):
        first, count_here = side * (slices // 2), slices // 2 if side == 0 else slices - slices // 2
        at = slice(first * LANES, (first + count_here) * LANES)
        moved = x[:, at] - 0.8 * scatter_rows(tile_hot[...], y[:, at])
        for z in range(count_here):
            for t in range(detectors):
                place = (slice((first + z) * local, (first + z + 1) * local), slice(t * LANES, (t + 1) * LANES))
                piece = moved[t * local:(t + 1) * local, z * LANES:(z + 1) * LANES]
                out_ref[place] = 2.0 * piece - cur[place]

    def finish(k, base, others):
        out_ref[rows_of(k), :] = 0.5 * cur[rows_of(k), :] + 0.25 * (others - base[rows_of(k), :])

    def low_part(side, base):
        mine, rest = half_of(side), half_of(1 - side)
        for part_of in (rest, mine):
            if side == 0:
                last_update(0 if part_of is mine else 1)
                for k in part_of:
                    own[k] = out_ref[rows_of(k), :].astype(BF)
                if part_of is rest:
                    pl.semaphore_wait(ready.at[0], 2)
            for k in part_of:
                to_beside(k).start()
        for k in mine:
            to_beside(k).wait_recv()
            pair[k] = (own[k].astype(F32) + beside[k].astype(F32)).astype(BF)
            to_across(pair, k).start()
        for part_of in (mine, rest):
            for k in part_of:
                if part_of is rest:
                    to_beside(k).wait_recv()
                to_across(pair, k).wait_recv()
                finish(k, base, beside[k].astype(F32) + across[k].astype(F32))
        for k in range(chunks):
            to_beside(k).wait_send()
        for k in mine:
            to_across(pair, k).wait_send()

    def high_part(side):
        mine, rest = half_of(side), half_of(1 - side)
        for k in range(chunks):
            to_beside(k).start()
        for k in range(chunks):
            to_beside(k).wait_recv()
            pair[k] = (own[k].astype(F32) + beside[k].astype(F32)).astype(BF)
            to_across(pair, k).start()
        for k in mine:
            to_across(pair, k).wait_recv()
            to_onward(k).start()
            finish(k, reflect_ref, beside[k].astype(F32) + across[k].astype(F32))
        for k in rest:
            to_onward(k).wait_recv()
            finish(k, reflect_ref, beside[k].astype(F32) + onward[k].astype(F32))
        for k in range(chunks):
            to_beside(k).wait_send()
            to_across(pair, k).wait_send()
        for k in mine:
            to_onward(k).wait_send()

    @pl.when(agent == 0)
    def _():
        barrier = pltpu.get_barrier_semaphore()
        for d in order:
            pl.semaphore_signal(barrier, inc=1, device_id=(agent, swap_bits(me, d)), device_id_type=MESH)
        for peer in (neighbour, opposite):
            pl.semaphore_signal(barrier, inc=1, device_id=(peer, me), device_id_type=MESH)
        for i in range(min(DEPTH, pl.cdiv(blocks_here, CHUNK))):
            block_copy(blocks_hbm, held, sems, i).start()

        hot_rows = lax.broadcasted_iota(jnp.int32, (ray_total, blocks_here), 0)
        ray = angle_ref[...] * detectors + detector_ref[...]
        hot = jnp.where(hot_rows == jnp.broadcast_to(ray, hot_rows.shape), 1.0, 0.0)
        ray_hot[...] = hot.astype(BF)
        ray_turned[...] = hot.T.astype(BF)
        hot_rows = lax.broadcasted_iota(jnp.int32, (tiles_here, blocks_here), 0)
        place = tile_ref[...]
        place = (place % detectors) * local + place // detectors
        hot = jnp.where(hot_rows == jnp.broadcast_to(place, hot_rows.shape), 1.0, 0.0)
        tile_hot[...] = hot.astype(BF)
        tile_turned[...] = hot.T.astype(BF)

        state.wait()
        for z in range(slices):
            for t in range(detectors):
                x[t * local:(t + 1) * local, z * LANES:(z + 1) * LANES] = cur[z * local:(z + 1) * local, t * LANES:(t + 1) * LANES]

        for step in range(DATA_STEPS):
            picked[...] = gather_rows(tile_turned[...], x[...].astype(BF))
            block_sweep(blocks_hbm, held, sems, picked, y, slices, True, step == 0)
            exchange(step, barrier)
            block_sweep(blocks_hbm, held, sems, picked, y, slices, False, False)
            exchanged(step)
            if step < DATA_STEPS - 1:
                x[...] = x[...] - 0.8 * scatter_rows(tile_hot[...], y[...])

        low_part(0, out_ref)

    @pl.when(agent != 0)
    def _():
        barrier = pltpu.get_barrier_semaphore()

        @pl.when(agent != 1)
        def _():
            pl.semaphore_signal(barrier, inc=1, device_id=(neighbour, me), device_id_type=MESH)

        @pl.when(agent != 2)
        def _():
            pl.semaphore_signal(barrier, inc=1, device_id=(opposite, me), device_id_type=MESH)

        for k in range(chunks):
            own[k] = reflect_ref[rows_of(k), :].astype(BF)
        state.wait()
        pl.semaphore_wait(barrier, 2)

        @pl.when(agent != 3)
        def _():
            pl.semaphore_signal(ready.at[0], inc=1, device_id=(0, me), device_id_type=MESH)

        @pl.when(agent == 1)
        def _():
            low_part(1, reflect_ref)

        @pl.when(agent == 2)
        def _():
            high_part(0)

        @pl.when(agent == 3)
        def _():
            high_part(1)


def idle_kernel(out_ref):
    pass


def join(angle, detector, tile, sinogram, reflect, current, blocks, count):
    slices, local, columns = current.shape
    rays_here = sinogram.shape[0]
    ray_total = rays_here * count
    tiles_here = columns // LANES * local
    blocks_here = blocks.shape[0]
    width = slices * LANES
    rows = slices * local
    chunks = max(2, rows // 32)
    chunk = (chunks, rows // chunks, columns)
    vmem = pl.BlockSpec(memory_space=pltpu.VMEM)
    anywhere = pl.BlockSpec(memory_space=pl.ANY)
    out = pl.pallas_call(
        functools.partial(join_kernel, (count, slices)),
        out_shape=pltpu.VMEM((rows, columns), F32),
        in_specs=[vmem] * 5 + [anywhere] * 2,
        out_specs=vmem,
        scratch_shapes=[
            pltpu.VMEM(blocks.shape, BF),
            pltpu.VMEM((rows, columns), F32),
            pltpu.VMEM((ray_total, blocks_here), BF),
            pltpu.VMEM((blocks_here, ray_total), BF),
            pltpu.VMEM((tiles_here, blocks_here), BF),
            pltpu.VMEM((blocks_here, tiles_here), BF),
            pltpu.VMEM((tiles_here, width), F32),
            pltpu.VMEM((blocks_here, width), F32),
            pltpu.VMEM((blocks_here, width), F32),
            pltpu.VMEM((2, ray_total, width // 2), F32),
            pltpu.VMEM((DATA_STEPS, 2, count, rays_here, width // 2), BF),
            pltpu.VMEM((DATA_STEPS, 2, count, rays_here, width // 2), BF),
            pltpu.VMEM((DATA_STEPS, 2, rays_here, width // 2), BF),
            pltpu.VMEM((DATA_STEPS, 2, count, rays_here, width // 2), BF),
        ]
        + [pltpu.VMEM(chunk, BF)] * 5
        + [pltpu.SemaphoreType.DMA((1,)), pltpu.SemaphoreType.DMA((pl.cdiv(blocks_here, CHUNK),))]
        + [pltpu.SemaphoreType.DMA((DATA_STEPS, 2, count))] * 4
        + [pltpu.SemaphoreType.REGULAR((1,))]
        + [pltpu.SemaphoreType.DMA((chunks,))] * 6,
        compiler_params=pltpu.CompilerParams(
            collective_id=0, has_side_effects=True, vmem_limit_bytes=58 * 1024 * 1024
        ),
        name="join_agents",
    )(
        angle.reshape(1, -1), detector.reshape(1, -1), tile.reshape(1, -1),
        sinogram.reshape(rays_here * slices, LANES), reflect.reshape(rows, columns),
        current.reshape(rows, columns), blocks,
    )
    return out.reshape(current.shape)


def per_device(
    states,
    sinogram,
    blocks,
    block_angle,
    block_detector,
    block_tile,
    conv_first,
    conv_hidden,
    conv_last,
):
    current = states[0]
    agent_place = lax.axis_index("agent")
    halo = conv_hidden.shape[1] + 2
    filters = (conv_first, conv_hidden, conv_last)
    edges = halo_exchange(current, halo)

    def data_only():
        return pl.pallas_call(
            idle_kernel,
            out_shape=jax.ShapeDtypeStruct(current.shape, F32),
            out_specs=pl.BlockSpec(memory_space=pl.ANY),
            name="idle",
        )()

    def axial_only():
        return axial_reflect(edges, current, *filters, halo)

    def sagittal_only():
        return plane_call(1, edges, current, *filters, halo, 1)

    def coronal_only():
        return coronal_reflect(current, *filters)

    reflect = lax.switch(agent_place, [data_only, axial_only, sagittal_only, coronal_only])
    joined = join(
        block_angle, block_detector, block_tile, sinogram, reflect, current, blocks, lax.axis_size("tile")
    )
    return joined[None]


def solution(mesh):
    placed = (
        P("agent", None, "tile", None),
        P("tile", None, None),
        P("tile", None, None),
        P("tile"),
        P("tile"),
        P("tile"),
        P(),
        P(),
        P(),
    )
    return jax.shard_map(
        per_device,
        mesh=mesh,
        in_specs=placed,
        out_specs=P("agent", None, "tile", None),
        check_vma=False,
    )
```

```python
import functools

import jax
import jax.numpy as jnp
from jax import lax
from jax.experimental import pallas as pl
from jax.experimental.pallas import tpu as pltpu
from jax.sharding import PartitionSpec as P

DATA_STEPS = 2
MESH = pl.DeviceIdType.MESH
LANES = 128
STRIPS = 16
CHUNK = 96
DEPTH = 2
BF = jnp.bfloat16
F32 = jnp.float32
NATURAL = (0, 1, 2, 3)
EVEN_ORDER = (0, 1, 2, 3)
ODD_ORDER = (1, 0, 3, 2)


def main_cells(offset):
    order = EVEN_ORDER if offset % 2 else ODD_ORDER
    return [(offset, column) for column in order]

def edge_cells(offset):
    return [(offset + 1, 4), (offset, 4), (offset, -1), (offset + 1, -1)]

def window_cells(rows):
    tiles = [main_cells(a) for a in range(rows + 2)]
    return tiles + [edge_cells(a) for a in range(0, rows + 2, 2)]

def spread_lanes(w):
    return jnp.concatenate([w] * (LANES // w.shape[-1]), axis=-1)

def lane_iota(rows):
    return lax.broadcasted_iota(jnp.int32, (rows, LANES), 1)

def slot_mix(rows, taps, column_in, order, width):
    slot = lane_iota(rows) // width
    mixed = jnp.zeros((rows, LANES), F32)
    for place, column in enumerate(order):
        tap = column_in - column + 1
        if 0 <= tap < 3:
            mixed = jnp.where(slot == place, taps[tap], mixed)
    return mixed

def build_first(w_ref, o, w1):
    for k in range(6):
        for half in range(2):
            order = ODD_ORDER if half else EVEN_ORDER
            mixes = []
            for ti in range(3):
                taps = [jnp.broadcast_to(spread_lanes(w_ref[o, ti, tj:tj+1, :].astype(F32)), (16, LANES)) for tj in range(3)]
                mixes.append(slot_mix(16, taps, k - 1, order, 32))
            row = lax.broadcasted_iota(jnp.int32, (16, LANES), 0)
            for t in range(4):
                value = jnp.zeros((16, LANES), F32)
                for ti in range(3):
                    value = jnp.where(row == 2 * t + half + ti, mixes[ti], value)
                at = t * 2 * LANES + half * LANES
                w1[k * 16:(k + 1) * 16, at:at + LANES] = value.astype(BF)

def build_hidden(w_ref, o, layer, wh):
    wide = [[spread_lanes(w_ref[o, layer, ti, tj].astype(F32)) for tj in range(3)] for ti in range(3)]
    inner = wide[0][0].shape[0]
    for n, tile in enumerate(window_cells(2)):
        for slot, (a, column) in enumerate(tile):
            at = n * LANES + slot * inner
            for half in range(2):
                ti = a - (half + 1) + 1
                if 0 <= ti < 3:
                    value = slot_mix(inner, wide[ti], column, ODD_ORDER if half else EVEN_ORDER, inner)
                else:
                    value = jnp.zeros((inner, LANES), F32)
                wh[layer, at:at + inner, half * LANES:(half + 1) * LANES] = value.astype(BF)

def column_of(row):
    inner = row.shape[1]
    r = lax.broadcasted_iota(jnp.int32, (inner, inner), 0)
    c = lax.broadcasted_iota(jnp.int32, (inner, inner), 1)
    picked = jnp.where(r == c, jnp.broadcast_to(row, (inner, inner)), 0.0)
    return jnp.broadcast_to(jnp.sum(picked, axis=1, keepdims=True), (inner, LANES))

def build_last(w_ref, o, wl):
    taps = [[column_of(w_ref[o, ti, tj:tj+1, :].astype(F32)) for tj in range(3)] for ti in range(3)]
    inner = taps[0][0].shape[0]
    lane = lane_iota(inner)
    row8 = lane % 8
    zero = jnp.zeros((inner, LANES), F32)
    rows = []
    for a in range(10):
        line = []
        for tj in range(3):
            value = zero
            for ti in range(3):
                if 0 <= a - ti < 8:
                    value = jnp.where(row8 == a - ti, taps[ti][tj], value)
            line.append(value)
        rows.append(line)
    for n, tile in enumerate(window_cells(8)):
        for slot, (a, column) in enumerate(tile):
            at = n * LANES + slot * inner
            wl[at:at + inner, :] = slot_mix(inner, rows[a], column, EVEN_ORDER, LANES // 4).astype(BF)


def axial_kernel(plan, edges_ref, cur_ref, cf_ref, ch_ref, cl_ref, out_ref, main, edge, w1, wh, wl, raw, xs, place, back, gathered_out):
    halo = plan
    slices, local, columns = cur_ref.shape
    rows = local + 2 * halo
    stored = rows + 8
    groups = columns // 4
    per = groups // STRIPS
    span = slices * groups
    layers = ch_ref.shape[1]
    tile = lax.axis_index("tile")
    at_start = tile == 0
    at_end = tile == lax.axis_size("tile") - 1
    fill_rows(raw, edges_ref, cur_ref, stored, halo)

    build_first(cf_ref, 0, w1)
    for layer in range(layers):
        build_hidden(ch_ref, 0, layer, wh)
    build_last(cl_ref, 0, wl)

    col = lax.broadcasted_iota(jnp.int32, (columns, groups), 0)
    m = lax.broadcasted_iota(jnp.int32, (columns, groups), 1)
    first_col = 4 * ((m % STRIPS) * per + m // STRIPS)
    for k in range(6):
        place[:, k * groups:(k + 1) * groups] = jnp.where(col == first_col + (k - 1), 1.0, 0.0).astype(BF)
    m = lax.broadcasted_iota(jnp.int32, (groups, columns), 0)
    col = lax.broadcasted_iota(jnp.int32, (groups, columns), 1)
    first_col = 4 * ((m % STRIPS) * per + m // STRIPS)
    for k in range(4):
        back[k * groups:(k + 1) * groups, :] = jnp.where(col == first_col + k, 1.0, 0.0).astype(BF)
    xs[...] = jnp.dot(raw[...].astype(BF), place[...], preferred_element_type=F32)

    slot = lane_iota(STRIPS) // (LANES // 4)
    even_slots = (slot == 0) | (slot == 3)
    right_slots = slot < 2
    strip = lax.broadcasted_iota(jnp.int32, (STRIPS, LANES), 0)
    zero_tile = jnp.zeros((slices, per, STRIPS, LANES), BF)

    for side in range(2):
        for r in (0, 1, 2, rows - 1, rows, rows + 1):
            main[side, r] = zero_tile
        for e in (0, 1, rows // 2 - 1, rows // 2):
            edge[side, e] = zero_tile

    def put_edge(side, e, odd_row, even_row):
        v = jnp.where(even_slots, even_row, odd_row)
        for z in range(slices):
            for i in range(per):
                if i + 1 < per:
                    right = v[z, i + 1]
                else:
                    right = jnp.where(strip == STRIPS - 1, 0.0, pltpu.roll(v[z, 0], STRIPS - 1, 0))
                if i > 0:
                    left = v[z, i - 1]
                else:
                    left = jnp.where(strip == 0, 0.0, pltpu.roll(v[z, per - 1], 1, 0))
                edge[side, e, z, i] = jnp.where(right_slots, right, left).astype(BF)

    def put_pairs(side, pair, count, y):
        before = main[side, 2 * pair].astype(F32)
        for t in range(count):
            row = 2 * (pair + t)
            v = jnp.maximum(y(t), 0.0)
            if not isinstance(row, int):
                outside = (at_start & (row < halo)) | (at_end & (row >= rows - halo))
                v = v * jnp.where(outside, 0.0, 1.0)
            elif row < halo:
                v = v * jnp.where(at_start, 0.0, 1.0)
            elif row >= rows - halo:
                v = v * jnp.where(at_end, 0.0, 1.0)
            even_row = v[:, :LANES].reshape(slices, per, STRIPS, LANES)
            odd_row = v[:, LANES:].reshape(slices, per, STRIPS, LANES)
            main[side, row + 1] = even_row.astype(BF)
            main[side, row + 2] = odd_row.astype(BF)
            put_edge(side, pair + t, before, even_row)
            before = odd_row

    def first_step(c):
        parts = []
        for z in range(slices):
            at = pl.ds(z * stored + 8 * c, 16)
            parts.append(jnp.concatenate([xs[at, k * groups:(k + 1) * groups] for k in range(6)], axis=0).astype(BF))
        x = jnp.concatenate(parts, axis=1)
        y = lax.dot_general(x, w1[...], (((0,), (0,)), ((), ())), preferred_element_type=F32)
        put_pairs(0, 4 * c, 4, lambda t: y[:, t * 2 * LANES:(t + 1) * 2 * LANES])

    for c in range(rows // 8):
        first_step(c)

    def window(side, pair, out_rows):
        parts = [main[side, 2 * pair + a].reshape(span, LANES) for a in range(out_rows + 2)]
        parts += [edge[side, pair + e].reshape(span, LANES) for e in range(out_rows // 2 + 1)]
        return jnp.concatenate(parts, axis=1)

    pairs = rows // 2 - 2
    run = max(n for n in range(1, 18) if pairs % n == 0)
    for layer in range(layers):
        source, target = layer % 2, (layer + 1) % 2

        def hidden_steps(c, carry):
            for j in range(run):
                pair = 1 + c * run + j
                y = jnp.dot(window(source, pair, 2), wh[layer], preferred_element_type=F32)
                put_pairs(target, pair, 1, lambda t: y)
            return carry

        lax.fori_loop(0, pairs // run, hidden_steps, 0)
        end = rows // 2 - 1
        put_edge(target, end, main[target, 2 * end].astype(F32), jnp.zeros((slices, per, STRIPS, LANES), F32))

    eighths = local // 8
    quad = (lane_iota(span) // 8) % 4

    four = 4 if eighths % 4 == 0 else eighths

    def last_steps(c, carry):
        value = jnp.zeros((span, LANES), F32)
        for j in range(four):
            x = window(layers % 2, halo // 2 + 4 * (c * four + j), 8)
            y = jnp.dot(x, wl[...], preferred_element_type=F32)
            value = jnp.where(quad == j, y, value)
        gathered_out[c] = value
        return carry

    lax.fori_loop(0, eighths // four, last_steps, 0)

    for big in range(gathered_out.shape[0]):
        height = min(32, local - 32 * big)
        turned = [gathered_out[big, z * groups:(z + 1) * groups, :].T for z in range(slices)]
        lines = [jnp.concatenate([turned[z][k * 32:(k + 1) * 32] for k in range(4)], axis=1) for z in range(slices)]
        values = jnp.concatenate(lines, axis=0)
        high = values.astype(BF)
        low = (values - high.astype(F32)).astype(BF)
        net = jnp.dot(high, back[...], preferred_element_type=F32) + jnp.dot(low, back[...], preferred_element_type=F32)
        for z in range(slices):
            at = pl.ds(32 * big, height)
            out_ref[z, at, :] = cur_ref[z, at, :] - 2.0 * net[z * 32:z * 32 + height]

def axial_reflect(edges, current, cf, ch, cl, halo):
    slices, local, columns = current.shape
    rows = local + 2 * halo
    groups = columns // 4
    per = groups // STRIPS
    stored = rows + 8
    whole = pl.BlockSpec(memory_space=pltpu.VMEM)
    return pl.pallas_call(
        functools.partial(axial_kernel, halo),
        out_shape=jax.ShapeDtypeStruct(current.shape, F32),
        in_specs=[whole] * 5,
        out_specs=whole,
        scratch_shapes=[
            pltpu.VMEM((2, rows + 2, slices, per, STRIPS, LANES), BF),
            pltpu.VMEM((2, rows // 2 + 1, slices, per, STRIPS, LANES), BF),
            pltpu.VMEM((96, 8 * LANES), BF),
            pltpu.VMEM((ch.shape[1], 6 * LANES, 2 * LANES), BF),
            pltpu.VMEM((15 * LANES, LANES), BF),
            pltpu.VMEM((slices * stored, columns), F32),
            pltpu.VMEM((slices * stored, 6 * groups), F32),
            pltpu.VMEM((columns, 6 * groups), BF),
            pltpu.VMEM((4 * groups, columns), BF),
            pltpu.VMEM((-(-local // 32), slices * groups, LANES), F32),
        ],
        compiler_params=pltpu.CompilerParams(vmem_limit_bytes=60 * 1024 * 1024),
        name="net_axial",
    )(edges, current, cf, ch, cl)


def fill_rows(raw, edges_ref, cur_ref, stored, halo):
    slices, local, columns = cur_ref.shape
    zero = jnp.zeros((1, columns), F32)
    tail = jnp.zeros((stored - 1 - local - 2 * halo, columns), F32)
    for z in range(slices):
        above = edges_ref[0, z * halo:(z + 1) * halo, :].astype(F32)
        below = edges_ref[1, z * halo:(z + 1) * halo, :].astype(F32)
        raw[z * stored:(z + 1) * stored, :] = jnp.concatenate([zero, above, cur_ref[z], below, tail], axis=0)


def build_first_plane(w_ref, o, w1):
    row = lax.broadcasted_iota(jnp.int32, (16, LANES), 0)
    for z in range(4):
        mixes = []
        for tj in range(3):
            taps = [jnp.broadcast_to(spread_lanes(w_ref[o, ti, tj:tj+1, :].astype(F32)), (16, LANES)) for ti in range(3)]
            mixes.append(slot_mix(16, taps, z, NATURAL, 32))
        for t in range(8):
            value = jnp.zeros((16, LANES), F32)
            for tj in range(3):
                value = jnp.where(row == t + tj, mixes[tj], value)
            w1[z * 16:(z + 1) * 16, t * LANES:(t + 1) * LANES] = value.astype(BF)

def build_hidden_plane(w_ref, o, layer, wh):
    wide = [[spread_lanes(w_ref[o, layer, ti, tj].astype(F32)) for ti in range(3)] for tj in range(3)]
    inner = wide[0][0].shape[0]
    for a in range(4):
        for z in range(4):
            at = a * LANES + z * inner
            for half in range(2):
                if 0 <= a - half < 3:
                    value = slot_mix(inner, wide[a - half], z, NATURAL, inner)
                else:
                    value = jnp.zeros((inner, LANES), F32)
                wh[layer, at:at + inner, half * LANES:(half + 1) * LANES] = value.astype(BF)

def build_last_plane(w_ref, o, wl):
    taps = [[column_of(w_ref[o, ti, tj:tj+1, :].astype(F32)) for ti in range(3)] for tj in range(3)]
    inner = taps[0][0].shape[0]
    row8 = lane_iota(inner) % 8
    zero = jnp.zeros((inner, LANES), F32)
    for a in range(10):
        line = []
        for ti in range(3):
            value = zero
            for tj in range(3):
                if 0 <= a - tj < 8:
                    value = jnp.where(row8 == a - tj, taps[tj][ti], value)
            line.append(value)
        for z in range(4):
            at = a * LANES + z * inner
            wl[at:at + inner, :] = slot_mix(inner, line, z, NATURAL, LANES // 4).astype(BF)


def plane_kernel(plan, x_ref, cur_ref, cf_ref, ch_ref, cl_ref, out_ref, main, w1, wh, wl, xs, gathered_out):
    o, halo, chunk, strips = plan
    slices, local, span = out_ref.shape
    rows = local + 2 * halo
    stored = rows + 8
    layers = ch_ref.shape[1]
    if halo:
        tile = lax.axis_index("tile")
        at_start = tile == 0
        at_end = tile == lax.axis_size("tile") - 1

    build_first_plane(cf_ref, o, w1)
    for layer in range(layers):
        build_hidden_plane(ch_ref, o, layer, wh)
    build_last_plane(cl_ref, o, wl)
    if halo:
        fill_rows(xs, x_ref, cur_ref, stored, halo)
    else:
        xs[...] = x_ref[...].astype(F32)
    for side in range(2):
        for r in (0, rows + 1):
            main[side, r] = jnp.zeros((span, LANES), BF)

    def put_pairs(side, pair, count, y):
        for t in range(count):
            row = 2 * (pair + t)
            v = jnp.maximum(y(t), 0.0)
            if halo:
                outside = (at_start & (row < halo)) | (at_end & (row >= rows - halo))
                v = v * jnp.where(outside, 0.0, 1.0)
            main[side, row + 1] = v[:, :LANES].astype(BF)
            main[side, row + 2] = v[:, LANES:].astype(BF)

    def ends(side):
        if strips > 1:
            step = span // strips
            main[side, 0, step:span] = main[side, rows, 0:span - step]
            main[side, rows + 1, 0:span - step] = main[side, 1, step:span]

    def first_step(c, carry):
        parts = [xs[pl.ds(pl.multiple_of(z * stored + 8 * c, 8), 16)] for z in range(slices)]
        x = jnp.concatenate(parts, axis=0).astype(BF)
        y = lax.dot_general(x, w1[...], (((0,), (0,)), ((), ())), preferred_element_type=F32)
        put_pairs(0, 4 * c, 4, lambda t: y[:, t * 2 * LANES:(t + 1) * 2 * LANES])
        return carry

    lax.fori_loop(0, rows // 8, first_step, 0)
    ends(0)

    for layer in range(layers):
        source, target = layer % 2, (layer + 1) % 2

        def hidden_step(c, carry):
            pair = c * chunk
            tiles = [main[source, 2 * pair + a] for a in range(2 * chunk + 2)]
            x = jnp.concatenate([jnp.concatenate(tiles[2 * t:2 * t + 4], axis=1) for t in range(chunk)], axis=0)
            y = jnp.dot(x, wh[layer], preferred_element_type=F32)
            put_pairs(target, pair, chunk, lambda t: y[t * span:(t + 1) * span])
            return carry

        lax.fori_loop(0, rows // 2 // chunk, hidden_step, 0)
        ends(target)

    quad = (lane_iota(span) // 8) % 4

    def last_step(q, carry):
        x = jnp.concatenate([main[layers % 2, halo + 8 * q + a] for a in range(10)], axis=1)
        y = jnp.dot(x, wl[...], preferred_element_type=F32)
        gathered_out[q // 4] = jnp.where(quad == q % 4, y, gathered_out[q // 4])
        return carry

    gathered_out[...] = jnp.zeros_like(gathered_out)
    lax.fori_loop(0, local // 8, last_step, 0)
    for big in range(gathered_out.shape[0]):
        height = min(32, local - 32 * big)
        net = gathered_out[big].T
        for z in range(slices):
            at = pl.ds(32 * big, height)
            out_ref[z, at, :] = cur_ref[z, at, :] - 2.0 * net[z * 32:z * 32 + height]

def plane_call(o, x, current, cf, ch, cl, halo, strips):
    slices, local, span = current.shape
    rows = local + 2 * halo
    whole = pl.BlockSpec(memory_space=pltpu.VMEM)
    return pl.pallas_call(
        functools.partial(plane_kernel, (o, halo, 4, strips)),
        out_shape=jax.ShapeDtypeStruct(current.shape, F32),
        in_specs=[whole] * 5, out_specs=whole,
        scratch_shapes=[
            pltpu.VMEM((2, rows + 2, span, LANES), BF),
            pltpu.VMEM((64, 8 * LANES), BF),
            pltpu.VMEM((ch.shape[1], 4 * LANES, 2 * LANES), BF),
            pltpu.VMEM((10 * LANES, LANES), BF),
            pltpu.VMEM((slices * (rows + 8), span), F32),
            pltpu.VMEM((-(-local // 32), span, LANES), F32),
        ],
        compiler_params=pltpu.CompilerParams(vmem_limit_bytes=60 * 1024 * 1024),
        name="net_sagittal" if halo else "net_coronal",
    )(x, current, cf, ch, cl)

def coronal_reflect(current, cf, ch, cl):
    slices, local, columns = current.shape
    strips = columns // local
    turned = jnp.transpose(current.reshape(slices, local, strips, local), (0, 3, 2, 1))
    t = turned.astype(BF)
    none = jnp.zeros((slices, 1, 1, local), BF)
    before = jnp.concatenate([none, t[:, -1:, :-1]], axis=2)
    after = jnp.concatenate([t[:, :1, 1:], none], axis=2)
    rest = jnp.zeros((slices, 6, strips, local), BF)
    x = jnp.concatenate([before, t, after, rest], axis=1)
    x = x.reshape(-1, columns)
    out = plane_call(2, x, turned.reshape(slices, local, columns), cf, ch, cl, 0, strips)
    return jnp.transpose(out.reshape(slices, local, strips, local), (0, 3, 2, 1)).reshape(current.shape)

def halo_kernel(halo, cur_hbm, out_ref, edge, sent, load, send, recv):
    agent = lax.axis_index("agent")
    tile = lax.axis_index("tile")
    last = lax.axis_size("tile") - 1
    slices, local, columns = cur_hbm.shape
    rows = edge.shape[2]
    active = (agent == 1) | (agent == 2)

    def copy(side, peer):
        return pltpu.make_async_remote_copy(
            src_ref=sent.at[side],
            dst_ref=out_ref.at[1 - side],
            send_sem=send.at[side],
            recv_sem=recv.at[1 - side],
            device_id=(agent, peer),
            device_id_type=MESH,
        )

    @pl.when(active)
    def _():
        barrier = pltpu.get_barrier_semaphore()

        @pl.when(tile > 0)
        def _():
            pl.semaphore_signal(barrier, inc=1, device_id=(agent, tile - 1), device_id_type=MESH)

        @pl.when(tile < last)
        def _():
            pl.semaphore_signal(barrier, inc=1, device_id=(agent, tile + 1), device_id_type=MESH)

        loads = [
            pltpu.make_async_copy(cur_hbm.at[:, pl.ds(0, rows)], edge.at[0], load.at[0]),
            pltpu.make_async_copy(cur_hbm.at[:, pl.ds(local - rows, rows)], edge.at[1], load.at[1]),
        ]
        for item in loads:
            item.start()
        for item in loads:
            item.wait()
        for side in range(2):
            first = 0 if side == 0 else rows - halo
            parts = [edge[side, z, first:first + halo, :] for z in range(slices)]
            sent[side] = jnp.concatenate(parts, axis=0).astype(BF)

        pl.semaphore_wait(barrier, jnp.where(tile > 0, 1, 0) + jnp.where(tile < last, 1, 0))

        @pl.when(tile > 0)
        def _():
            copy(0, tile - 1).start()

        @pl.when(tile < last)
        def _():
            copy(1, tile + 1).start()

        @pl.when(tile == 0)
        def _():
            out_ref[0] = jnp.zeros(out_ref.shape[1:], BF)

        @pl.when(tile == last)
        def _():
            out_ref[1] = jnp.zeros(out_ref.shape[1:], BF)

        @pl.when(tile > 0)
        def _():
            copy(1, tile - 1).wait_recv()

        @pl.when(tile < last)
        def _():
            copy(0, tile + 1).wait_recv()

        @pl.when(tile > 0)
        def _():
            copy(0, tile - 1).wait_send()

        @pl.when(tile < last)
        def _():
            copy(1, tile + 1).wait_send()


def halo_exchange(current, halo):
    slices, local, columns = current.shape
    return pl.pallas_call(
        functools.partial(halo_kernel, halo),
        out_shape=jax.ShapeDtypeStruct((2, slices * halo, columns), BF),
        in_specs=[pl.BlockSpec(memory_space=pl.ANY)],
        out_specs=pl.BlockSpec(memory_space=pltpu.VMEM),
        scratch_shapes=[
            pltpu.VMEM((2, slices, 8, columns), F32),
            pltpu.VMEM((2, slices * halo, columns), BF),
            pltpu.SemaphoreType.DMA((2,)),
            pltpu.SemaphoreType.DMA((2,)),
            pltpu.SemaphoreType.DMA((2,)),
        ],
        compiler_params=pltpu.CompilerParams(collective_id=2, has_side_effects=True),
        name="halo_exchange",
    )(current)


def swap_bits(me, d):
    peer, bit = me, 1
    while bit <= d:
        if d & bit:
            peer = peer + bit * (1 - 2 * ((me // bit) % 2))
        bit *= 2
    return peer


def block_copy(blocks_hbm, held, sems, i):
    at = pl.ds(i * CHUNK, min(CHUNK, held.shape[0] - i * CHUNK))
    return pltpu.make_async_copy(blocks_hbm.at[at], held.at[at], sems.at[i])


def block_step(held, picked, y, slices, transposed, u):
    row = lax.broadcasted_iota(jnp.int32, (8, LANES), 0)
    upper, even = row < 4, row % 2 == 0
    at = pl.ds(pl.multiple_of(8 * u, 8), 8)

    def turned(v):
        return pltpu.roll(v, 4, 0)

    rows = [[], []]
    for z in range(0, slices, 2):
        v, w = (picked[at, (z + i) * LANES:(z + i + 1) * LANES] for i in range(2))
        rows[0].append(jnp.where(upper, v, turned(w)))
        rows[1].append(jnp.where(upper, turned(v), w))
    outs = []
    for t in range(2):
        sides = [
            jnp.concatenate([jnp.where(row % 4 // 2 == side, v, 0.0) for v in rows[t]], axis=0) for side in range(2)
        ]
        lhs = jnp.concatenate(sides, axis=1).astype(BF)
        m = [held[8 * u + 4 * t + j] for j in range(4)]
        if transposed:
            top, bottom = jnp.concatenate([m[0], m[2]], axis=1), jnp.concatenate([m[1], m[3]], axis=1)
            dims = (((1,), (1,)), ((), ()))
        else:
            top, bottom = jnp.concatenate([m[0], m[1]], axis=1), jnp.concatenate([m[2], m[3]], axis=1)
            dims = (((1,), (0,)), ((), ()))
        rhs = jnp.concatenate([top, bottom], axis=0)
        out = lax.dot_general(lhs, rhs, dims, preferred_element_type=F32)
        outs.append(jnp.where(jnp.concatenate([even] * (slices // 2), axis=0), out[:, :LANES], out[:, LANES:]))
    for z in range(0, slices, 2):
        v, w = (o[4 * z:4 * z + 8] for o in outs)
        y[at, z * LANES:(z + 1) * LANES] = jnp.where(upper, v, turned(w))
        y[at, (z + 1) * LANES:(z + 2) * LANES] = jnp.where(upper, turned(v), w)


def block_sweep(blocks_hbm, held, sems, picked, y, slices, transposed, waiting):
    pieces = pl.cdiv(held.shape[0], CHUNK)
    for i in range(pieces):
        if waiting:
            block_copy(blocks_hbm, held, sems, i).wait()
            if i + DEPTH < pieces:
                block_copy(blocks_hbm, held, sems, i + DEPTH).start()
        for u in range(i * CHUNK // 8, min((i + 1) * CHUNK, held.shape[0]) // 8):
            block_step(held, picked, y, slices, transposed, u)


def gather_rows(hot, source):
    return jnp.dot(hot, source, preferred_element_type=F32)


def scatter_rows(hot, y):
    high = y.astype(BF)
    low = (y - high.astype(F32)).astype(BF)
    return jnp.dot(
        jnp.concatenate([hot, hot], axis=1), jnp.concatenate([high, low], axis=0), preferred_element_type=F32
    )


def join_kernel(
    plan, angle_ref, detector_ref, tile_ref, sino_ref, reflect_ref, cur_hbm, blocks_hbm, out_ref,
    held, cur, ray_hot, ray_turned, tile_hot, tile_turned, x, y, picked, total, part, got, fresh, full,
    own, pair, beside, across, onward,
    load, sems, send1, recv1, send2, recv2, ready,
    send_beside, recv_beside, send_across, recv_across, send_onward, recv_onward,
):
    agent = lax.axis_index("agent")
    me = lax.axis_index("tile")
    count, slices = plan
    chunks, height, columns = own.shape
    local = chunks * height // slices
    detectors = columns // LANES
    rays_here = fresh.shape[2]
    ray_total = count * rays_here
    tiles_here = detectors * local
    blocks_here = held.shape[0]
    order = list(range(count - 1, 0, -1))
    core = agent % 2
    neighbour = agent + 1 - 2 * core
    opposite = (agent + 2) % 4
    state = pltpu.make_async_copy(cur_hbm, cur, load.at[0])
    state.start()

    def send(source, target, s, r, k, to):
        return pltpu.make_async_remote_copy(
            src_ref=source.at[k], dst_ref=target.at[k], send_sem=s.at[k], recv_sem=r.at[k],
            device_id=(to, me), device_id_type=MESH,
        )

    def to_beside(k):
        return send(own, beside, send_beside, recv_beside, k, neighbour)

    def to_across(source, k):
        return send(source, across, send_across, recv_across, k, opposite)

    def to_onward(k):
        return send(across, onward, send_onward, recv_onward, k, neighbour)

    def rows_of(k):
        return slice(k * height, (k + 1) * height)

    width = slices // 2 * LANES

    def columns_of(h):
        return slice(h * width, (h + 1) * width)

    def part_copy(step, h, d):
        return pltpu.make_async_remote_copy(
            src_ref=part.at[step, h, swap_bits(me, d)],
            dst_ref=got.at[step, h, d],
            send_sem=send1.at[step, h, d],
            recv_sem=recv1.at[step, h, d],
            device_id=(agent, swap_bits(me, d)),
            device_id_type=MESH,
        )

    def rest_copy(step, h, d):
        return pltpu.make_async_remote_copy(
            src_ref=fresh.at[step, h],
            dst_ref=full.at[step, h, me],
            send_sem=send2.at[step, h, d],
            recv_sem=recv2.at[step, h, d],
            device_id=(agent, swap_bits(me, d)),
            device_id_type=MESH,
        )

    def exchange(step, barrier):
        for h in range(2):
            total[h] = gather_rows(ray_hot[...], y[:, columns_of(h)].astype(BF))
            for slot in range(count):
                part[step, h, slot] = total[h, slot * rays_here:(slot + 1) * rays_here, :].astype(BF)
            if step == 0 and h == 0:
                pl.semaphore_wait(barrier, count - 1)
            for d in order:
                part_copy(step, h, d).start()
        for h in range(2):
            value = total[h, pl.ds(pl.multiple_of(me * rays_here, 8), rays_here), :]
            measured = [
                sino_ref[pl.ds(h * (slices // 2) + z, rays_here, stride=slices), :] for z in range(slices // 2)
            ]
            value = value - jnp.concatenate(measured, axis=1)
            for d in reversed(order):
                part_copy(step, h, d).wait_recv()
                value = value + got[step, h, d].astype(F32)
            fresh[step, h] = value.astype(BF)
            for d in order:
                rest_copy(step, h, d).start()
            full[step, h, me] = fresh[step, h]
        for h in range(2):
            for d in order:
                rest_copy(step, h, d).wait_recv()
            picked[:, columns_of(h)] = gather_rows(ray_turned[...], full[step, h].reshape(ray_total, width))

    def exchanged(step):
        for h in range(2):
            for d in order:
                part_copy(step, h, d).wait_send()
                rest_copy(step, h, d).wait_send()

    middle = chunks // 2

    def half_of(side):
        return range(side * middle, chunks if side else middle)

    def last_update(side):
        first, count_here = side * (slices // 2), slices // 2 if side == 0 else slices - slices // 2
        at = slice(first * LANES, (first + count_here) * LANES)
        moved = x[:, at] - 0.8 * scatter_rows(tile_hot[...], y[:, at])
        for z in range(count_here):
            for t in range(detectors):
                place = (slice((first + z) * local, (first + z + 1) * local), slice(t * LANES, (t + 1) * LANES))
                piece = moved[t * local:(t + 1) * local, z * LANES:(z + 1) * LANES]
                out_ref[place] = 2.0 * piece - cur[place]

    def finish(k, base, others):
        out_ref[rows_of(k), :] = 0.5 * cur[rows_of(k), :] + 0.25 * (others - base[rows_of(k), :])

    def low_part(side, base):
        mine, rest = half_of(side), half_of(1 - side)
        for part_of in (rest, mine):
            if side == 0:
                last_update(0 if part_of is mine else 1)
                for k in part_of:
                    own[k] = out_ref[rows_of(k), :].astype(BF)
                if part_of is rest:
                    pl.semaphore_wait(ready.at[0], 2)
            for k in part_of:
                to_beside(k).start()
        for k in mine:
            to_beside(k).wait_recv()
            pair[k] = (own[k].astype(F32) + beside[k].astype(F32)).astype(BF)
            to_across(pair, k).start()
        for part_of in (mine, rest):
            for k in part_of:
                if part_of is rest:
                    to_beside(k).wait_recv()
                to_across(pair, k).wait_recv()
                finish(k, base, beside[k].astype(F32) + across[k].astype(F32))
        for k in range(chunks):
            to_beside(k).wait_send()
        for k in mine:
            to_across(pair, k).wait_send()

    def high_part(side):
        mine, rest = half_of(side), half_of(1 - side)
        for k in range(chunks):
            to_beside(k).start()
        for k in range(chunks):
            to_beside(k).wait_recv()
            pair[k] = (own[k].astype(F32) + beside[k].astype(F32)).astype(BF)
            to_across(pair, k).start()
        for k in mine:
            to_across(pair, k).wait_recv()
            to_onward(k).start()
            finish(k, reflect_ref, beside[k].astype(F32) + across[k].astype(F32))
        for k in rest:
            to_onward(k).wait_recv()
            finish(k, reflect_ref, beside[k].astype(F32) + onward[k].astype(F32))
        for k in range(chunks):
            to_beside(k).wait_send()
            to_across(pair, k).wait_send()
        for k in mine:
            to_onward(k).wait_send()

    @pl.when(agent == 0)
    def _():
        barrier = pltpu.get_barrier_semaphore()
        for d in order:
            pl.semaphore_signal(barrier, inc=1, device_id=(agent, swap_bits(me, d)), device_id_type=MESH)
        for peer in (neighbour, opposite):
            pl.semaphore_signal(barrier, inc=1, device_id=(peer, me), device_id_type=MESH)
        for i in range(min(DEPTH, pl.cdiv(blocks_here, CHUNK))):
            block_copy(blocks_hbm, held, sems, i).start()

        hot_rows = lax.broadcasted_iota(jnp.int32, (ray_total, blocks_here), 0)
        ray = angle_ref[...] * detectors + detector_ref[...]
        hot = jnp.where(hot_rows == jnp.broadcast_to(ray, hot_rows.shape), 1.0, 0.0)
        ray_hot[...] = hot.astype(BF)
        ray_turned[...] = hot.T.astype(BF)
        hot_rows = lax.broadcasted_iota(jnp.int32, (tiles_here, blocks_here), 0)
        place = tile_ref[...]
        place = (place % detectors) * local + place // detectors
        hot = jnp.where(hot_rows == jnp.broadcast_to(place, hot_rows.shape), 1.0, 0.0)
        tile_hot[...] = hot.astype(BF)
        tile_turned[...] = hot.T.astype(BF)

        state.wait()
        for z in range(slices):
            for t in range(detectors):
                x[t * local:(t + 1) * local, z * LANES:(z + 1) * LANES] = cur[z * local:(z + 1) * local, t * LANES:(t + 1) * LANES]

        for step in range(DATA_STEPS):
            picked[...] = gather_rows(tile_turned[...], x[...].astype(BF))
            block_sweep(blocks_hbm, held, sems, picked, y, slices, True, step == 0)
            exchange(step, barrier)
            block_sweep(blocks_hbm, held, sems, picked, y, slices, False, False)
            exchanged(step)
            if step < DATA_STEPS - 1:
                x[...] = x[...] - 0.8 * scatter_rows(tile_hot[...], y[...])

        low_part(0, out_ref)

    @pl.when(agent != 0)
    def _():
        barrier = pltpu.get_barrier_semaphore()

        @pl.when(agent != 1)
        def _():
            pl.semaphore_signal(barrier, inc=1, device_id=(neighbour, me), device_id_type=MESH)

        @pl.when(agent != 2)
        def _():
            pl.semaphore_signal(barrier, inc=1, device_id=(opposite, me), device_id_type=MESH)

        for k in range(chunks):
            own[k] = reflect_ref[rows_of(k), :].astype(BF)
        state.wait()
        pl.semaphore_wait(barrier, 2)

        @pl.when(agent != 3)
        def _():
            pl.semaphore_signal(ready.at[0], inc=1, device_id=(0, me), device_id_type=MESH)

        @pl.when(agent == 1)
        def _():
            low_part(1, reflect_ref)

        @pl.when(agent == 2)
        def _():
            high_part(0)

        @pl.when(agent == 3)
        def _():
            high_part(1)


def idle_kernel(out_ref):
    pass


def join(angle, detector, tile, sinogram, reflect, current, blocks, count):
    slices, local, columns = current.shape
    rays_here = sinogram.shape[0]
    ray_total = rays_here * count
    tiles_here = columns // LANES * local
    blocks_here = blocks.shape[0]
    width = slices * LANES
    rows = slices * local
    chunks = max(2, rows // 32)
    chunk = (chunks, rows // chunks, columns)
    vmem = pl.BlockSpec(memory_space=pltpu.VMEM)
    anywhere = pl.BlockSpec(memory_space=pl.ANY)
    out = pl.pallas_call(
        functools.partial(join_kernel, (count, slices)),
        out_shape=pltpu.VMEM((rows, columns), F32),
        in_specs=[vmem] * 5 + [anywhere] * 2,
        out_specs=vmem,
        scratch_shapes=[
            pltpu.VMEM(blocks.shape, BF),
            pltpu.VMEM((rows, columns), F32),
            pltpu.VMEM((ray_total, blocks_here), BF),
            pltpu.VMEM((blocks_here, ray_total), BF),
            pltpu.VMEM((tiles_here, blocks_here), BF),
            pltpu.VMEM((blocks_here, tiles_here), BF),
            pltpu.VMEM((tiles_here, width), F32),
            pltpu.VMEM((blocks_here, width), F32),
            pltpu.VMEM((blocks_here, width), F32),
            pltpu.VMEM((2, ray_total, width // 2), F32),
            pltpu.VMEM((DATA_STEPS, 2, count, rays_here, width // 2), BF),
            pltpu.VMEM((DATA_STEPS, 2, count, rays_here, width // 2), BF),
            pltpu.VMEM((DATA_STEPS, 2, rays_here, width // 2), BF),
            pltpu.VMEM((DATA_STEPS, 2, count, rays_here, width // 2), BF),
        ]
        + [pltpu.VMEM(chunk, BF)] * 5
        + [pltpu.SemaphoreType.DMA((1,)), pltpu.SemaphoreType.DMA((pl.cdiv(blocks_here, CHUNK),))]
        + [pltpu.SemaphoreType.DMA((DATA_STEPS, 2, count))] * 4
        + [pltpu.SemaphoreType.REGULAR((1,))]
        + [pltpu.SemaphoreType.DMA((chunks,))] * 6,
        compiler_params=pltpu.CompilerParams(
            collective_id=0, has_side_effects=True, vmem_limit_bytes=58 * 1024 * 1024
        ),
        name="join_agents",
    )(
        angle.reshape(1, -1), detector.reshape(1, -1), tile.reshape(1, -1),
        sinogram.reshape(rays_here * slices, LANES), reflect.reshape(rows, columns),
        current.reshape(rows, columns), blocks,
    )
    return out.reshape(current.shape)


def per_device(
    states,
    sinogram,
    blocks,
    block_angle,
    block_detector,
    block_tile,
    conv_first,
    conv_hidden,
    conv_last,
):
    current = states[0]
    agent_place = lax.axis_index("agent")
    halo = conv_hidden.shape[1] + 2
    filters = (conv_first, conv_hidden, conv_last)
    edges = halo_exchange(current, halo)

    def data_only():
        return pl.pallas_call(
            idle_kernel,
            out_shape=jax.ShapeDtypeStruct(current.shape, F32),
            out_specs=pl.BlockSpec(memory_space=pl.ANY),
            name="idle",
        )()

    def axial_only():
        return axial_reflect(edges, current, *filters, halo)

    def sagittal_only():
        return plane_call(1, edges, current, *filters, halo, 1)

    def coronal_only():
        return coronal_reflect(current, *filters)

    reflect = lax.switch(agent_place, [data_only, axial_only, sagittal_only, coronal_only])
    joined = join(
        block_angle, block_detector, block_tile, sinogram, reflect, current, blocks, lax.axis_size("tile")
    )
    return joined[None]


def solution(mesh):
    placed = (
        P("agent", None, "tile", None),
        P("tile", None, None),
        P("tile", None, None),
        P("tile"),
        P("tile"),
        P("tile"),
        P(),
        P(),
        P(),
    )
    return jax.shard_map(
        per_device,
        mesh=mesh,
        in_specs=placed,
        out_specs=P("agent", None, "tile", None),
        check_vma=False,
    )
```
